32 devices in a mesh: grp: 2 (over y), ctx: 4 (over z), hd: 4 (over x, core).
Axes of the slice: x: 2, y: 2, z: 4, core: 2. Of those that a mesh axis runs over, the one named last changes fastest.
Arguments:
- query: bfloat16 [1024, 4096], P(('grp', 'ctx'), 'hd'), parts along dimension 0, may hold values from -6 to 6
- keys: bfloat16 [1024, 1024], P(('grp', 'ctx'), 'hd'), parts along dimension 0, may hold values from -6 to 6
- values: bfloat16 [1024, 1024], P(('grp', 'ctx'), 'hd'), parts along dimension 0, may hold values from -6 to 6
- m_x: bfloat16 [1024, 8192], P(('grp', 'ctx'), 'hd'), parts along dimension 0, may hold values from -6 to 6
- m_z: bfloat16 [1024, 8192], P(('grp', 'ctx'), 'hd'), parts along dimension 0, may hold values from -6 to 6
- m_b: bfloat16 [1024, 1024], P(('grp', 'ctx'), 'hd'), parts along dimension 0, may hold values from -6 to 6
- m_c: bfloat16 [1024, 1024], P(('grp', 'ctx'), 'hd'), parts along dimension 0, may hold values from -0.5 to 0.5
- dt_raw: bfloat16 [1024, 128], P(('grp', 'ctx'), 'hd'), parts along dimension 0, may hold values from -5 to 25
- dt_bias: float32 [128], P('hd'), may hold values from -0.5 to 0.5
- a_log: float32 [128], P('hd'), may hold values from -10 to 0
- d_skip: float32 [128], P('hd'), may hold values from 0.5 to 2
- norm_gain: float32 [8192], P('hd'), may hold values from 0.5 to 1.5
Outputs:
- context: bfloat16 [1024, 4096], P(('grp', 'ctx'), 'hd'), parts along dimension 0
- mixed: bfloat16 [1024, 8192], P(('grp', 'ctx'), 'hd'), parts along dimension 0
The draws below stay inside these ranges and needn't reach their ends.
There are 2 independent parts, one for each index of `grp`. The reference program is written for one: setup_inputs(seed, part) draws one part's arguments, and reference() takes and returns one part's arrays. A program takes and returns all parts, laid end to end along the dimension named above; an argument that names none is the same for every part. Nothing has to cross between parts.
All inputs are finite; a program needn't handle non-finite values.
Results may differ from the reference program's by a relative error of at most 0.009.
Values may be sent and summed in bfloat16 or wider, within the bound.
A program may use at most 64 MiB of HBM per device.

```python
import math
import jax
import jax.numpy as jnp
from jax import lax

QUERY_HEADS = 32
KEY_VALUE_HEADS = 8
HEAD_SIZE = 128
MH = 128
MP = 64
MN = 128
MG = 8
TOK_DEV = 128
SEQUENCE_TOKENS = 512
N_CTX = 4


def spike_rows(key):
    return jax.random.randint(jax.random.fold_in(key, 101), (2,), 0, SEQUENCE_TOKENS)


def spike_level():
    return min(SEQUENCE_TOKENS // 20, 256)


def draw_keys(key, part):
    random_seed_key = jax.random.fold_in(key, 606)
    sampled = jnp.clip(jax.random.normal(random_seed_key, (SEQUENCE_TOKENS, KEY_VALUE_HEADS * HEAD_SIZE), jnp.float32), -6.0, 6.0)
    return sampled.astype(jnp.bfloat16)


def draw_query(key, part):
    random_seed_key = jax.random.fold_in(key, 707)
    sampled = jnp.clip(jax.random.normal(random_seed_key, (SEQUENCE_TOKENS, QUERY_HEADS * HEAD_SIZE), jnp.float32), -6.0, 6.0)
    return sampled.astype(jnp.bfloat16)


def draw_m_x(key, part):
    selected = spike_rows(key)
    first_key = jax.random.fold_in(jax.random.fold_in(key, 303), 0)
    sampled = jax.random.normal(first_key, (SEQUENCE_TOKENS, MH * MP), jnp.float32)
    sampled = jnp.clip(sampled, -6.0, 6.0)
    flagged = jnp.any(jnp.arange(SEQUENCE_TOKENS)[:, None] == selected[None, :], axis=1)
    sampled = jnp.where(flagged[:, None], sampled * (0.06 / spike_level()), sampled)
    return sampled.astype(jnp.bfloat16)


def draw_dt_raw(key, part):
    selected = spike_rows(key)
    first_key, other_random_key = jax.random.split(jax.random.fold_in(key, 202))
    rough = jax.random.uniform(first_key, (SEQUENCE_TOKENS, MH), jnp.float32, -1.0, 1.0) - 3.0
    offsets = jax.random.uniform(other_random_key, (SEQUENCE_TOKENS // TOK_DEV, 1), jnp.float32, -0.7, 0.7)
    sampled = rough + jnp.repeat(offsets, TOK_DEV, axis=0)
    flagged = jnp.any(jnp.arange(SEQUENCE_TOKENS)[:, None] == selected[None, :], axis=1)
    sampled = jnp.where(flagged[:, None], jnp.float32(spike_level()), sampled)
    return sampled.astype(jnp.bfloat16)


def draw_a_log(key, part):
    first_key, other_random_key, third_key = jax.random.split(jax.random.fold_in(key, 404), 3)
    quick = jax.random.bernoulli(first_key, 0.5, (MH,))
    window = jax.random.uniform(other_random_key, (MH,), jnp.float32, 20.0, 60.0)
    slack = jax.random.uniform(third_key, (MH,), jnp.float32, 0.3, 1.0)
    fast_rate = -jnp.log(0.06 * window)
    slow_rate = -jnp.log(0.06 * SEQUENCE_TOKENS) - slack
    return jnp.where(quick, fast_rate, slow_rate).astype(jnp.float32)


def block_levels(rng, shape, cuts, least, top_value):
    level = 1.0
    for position, blocks in cuts:
        steps = jax.random.uniform(jax.random.fold_in(jax.random.fold_in(rng, 6), position), (blocks,), jnp.float32, least / len(cuts), top_value / len(cuts))
        level = level * jnp.repeat(jnp.exp(steps), shape[position] // blocks).reshape((-1,) + (1,) * (len(shape) - 1 - position))
    return level


def noise(own_key, extent, scale, bound, shards=(), kind=jnp.bfloat16):
    level = block_levels(own_key, extent, shards, -0.22, 0.18) if shards else 1.0
    values = jax.random.normal(own_key, extent, jnp.float32) * scale * level
    return jnp.minimum(jnp.maximum(values, -bound), bound).astype(kind)


def setup_inputs(seed: int = 0, part: int = 0) -> dict:
    streams_of = jax.random.split(jax.random.key(seed), 13)
    part_keys = jax.random.split(jax.random.fold_in(streams_of[12], part), 13)
    return {
        "query": draw_query(jax.random.fold_in(jax.random.fold_in(streams_of[12], part), 71), part),
        "keys": draw_keys(jax.random.fold_in(jax.random.fold_in(streams_of[12], part), 71), part),
        "values": noise(part_keys[2], (SEQUENCE_TOKENS, KEY_VALUE_HEADS * HEAD_SIZE), 1.0, 6.0, ((0, 4), (1, 4))),
        "m_x": draw_m_x(jax.random.fold_in(jax.random.fold_in(streams_of[12], part), 71), part),
        "m_z": noise(part_keys[4], (SEQUENCE_TOKENS, MH * MP), 1.0, 6.0, ((0, 4), (1, 4))),
        "m_b": noise(part_keys[5], (SEQUENCE_TOKENS, MG * MN), 1.0, 6.0, ((0, 4), (1, 4))),
        "m_c": noise(part_keys[6], (SEQUENCE_TOKENS, MG * MN), MN ** -0.5, 0.5, ((0, 4), (1, 4))),
        "dt_raw": draw_dt_raw(jax.random.fold_in(jax.random.fold_in(streams_of[12], part), 71), part),
        "dt_bias": jnp.clip(jax.random.uniform(streams_of[8], (MH,), jnp.float32, -0.5, 0.5) * block_levels(streams_of[8], (MH,), ((0, 4),), -0.4, 0.0), -0.5, 0.5),
        "a_log": draw_a_log(jax.random.fold_in(streams_of[12], 71), part),
        "d_skip": jnp.clip(0.5 + 1.5 * jax.random.uniform(streams_of[10], (MH,), jnp.float32) ** block_levels(streams_of[10], (MH,), ((0, 4),), -0.2, 0.2), 0.5, 2.0),
        "norm_gain": jnp.clip(1.0 + 0.1 * jax.random.normal(streams_of[11], (MH * MP,), jnp.float32), 0.5, 1.5),
    }


highest = lax.Precision.HIGHEST
norm_eps = 1e-05

def folded_to_sequence(whole):
    half_rows = whole.shape[0] // (2 * N_CTX)
    blocks = whole.reshape((N_CTX, 2, half_rows) + whole.shape[1:])
    return jnp.concatenate([blocks[:, 0], blocks[::-1, 1]], axis=0).reshape(whole.shape)

def attention(query, keys, values):
    sequence_length = query.shape[0]
    heads_per_group = QUERY_HEADS // KEY_VALUE_HEADS
    every_query = query.astype(jnp.float32).reshape(sequence_length, KEY_VALUE_HEADS, heads_per_group, HEAD_SIZE)
    every_key = keys.astype(jnp.float32).reshape(sequence_length, KEY_VALUE_HEADS, HEAD_SIZE)
    every_value = values.astype(jnp.float32).reshape(sequence_length, KEY_VALUE_HEADS, HEAD_SIZE)
    rows_per_block = math.gcd(sequence_length, 256)
    query_block_list = every_query.reshape(sequence_length // rows_per_block, rows_per_block, KEY_VALUE_HEADS, heads_per_group, HEAD_SIZE)
    key_pos = jnp.arange(sequence_length, dtype=jnp.int32)

    def query_block(packed):
        block_query, block_index = packed
        query_pos = block_index * rows_per_block + jnp.arange(rows_per_block, dtype=jnp.int32)
        scores = jnp.einsum('qhgd,khd->hgqk', block_query, every_key, precision=highest) / math.sqrt(HEAD_SIZE)
        visible = key_pos[None, :] <= query_pos[:, None]
        scores = jnp.where(visible, scores, -jnp.inf)
        largest = lax.optimization_barrier(jnp.max(scores, axis=-1, keepdims=True))
        expons = jnp.exp(scores - largest)
        totals = lax.optimization_barrier(jnp.sum(expons, axis=-1))
        rounded = lax.optimization_barrier(expons.astype(jnp.bfloat16)).astype(jnp.float32)
        summed = jnp.einsum('hgqk,khd->qhgd', rounded, every_value, precision=highest)
        return (summed / jnp.transpose(totals, (2, 0, 1))[..., None]).reshape(rows_per_block, QUERY_HEADS * HEAD_SIZE)
    result = lax.map(query_block, (query_block_list, jnp.arange(sequence_length // rows_per_block, dtype=jnp.int32)))
    return result.reshape(sequence_length, QUERY_HEADS * HEAD_SIZE).astype(jnp.bfloat16)

def ssd_block(inputs, steps, rates, b_rows, c_rows):
    intersection = jnp.dot(c_rows, b_rows.T, preferred_element_type=jnp.float32)
    inputs = inputs.astype(jnp.float32)
    b_rows = b_rows.astype(jnp.float32)
    sequence_length = inputs.shape[0]
    running = jnp.cumsum(-steps * rates, axis=0)
    lower = jnp.arange(sequence_length)[:, None] >= jnp.arange(sequence_length)[None, :]
    spread = running[:, None, :] - running[None, :, :]
    decay = jnp.exp(jnp.where(lower[:, :, None], spread, -jnp.inf))
    weights = intersection[:, :, None] * decay * steps[None, :, :]
    inner = jnp.einsum('ijh,jhp->ihp', weights, inputs, precision=highest)
    tail_weight = jnp.exp(running[-1][None, :] - running) * steps
    state = jnp.einsum('jh,jhp,jn->hpn', tail_weight, inputs, b_rows, precision=highest)
    return (inner, state, jnp.exp(running[-1]), jnp.exp(running))

def chain_states(earlier, later):
    return (earlier[0] * later[0], earlier[1] * later[0][..., None, None] + later[1])

def ssd_sequence(inputs, steps, rates, b_rows, c_rows):
    sequence_length, head_count, width = inputs.shape
    block_len = math.gcd(sequence_length, 128)
    count = sequence_length // block_len
    c_blocks = c_rows.reshape(count, block_len, -1)
    inner, state, totals, scaled = jax.vmap(ssd_block, in_axes=(0, 0, None, 0, 0))(inputs.reshape(count, block_len, head_count, width), steps.reshape(count, block_len, head_count), rates, b_rows.reshape(count, block_len, -1), c_blocks)
    running = lax.associative_scan(chain_states, (totals, state))
    entering = jnp.concatenate([jnp.zeros_like(running[1][:1]), running[1][:-1]], axis=0)
    carried = jnp.einsum('cqn,chpn->cqhp', c_blocks.astype(jnp.float32), entering, precision=highest) * scaled[..., None]
    return (inner + carried).reshape(sequence_length, head_count, width)

def gated_norm(gated_rows, norm_scale, group_count):
    row_count = gated_rows.shape[0]
    widened = lax.optimization_barrier(gated_rows).astype(jnp.float32).reshape(row_count, group_count, -1)
    power = lax.optimization_barrier(jnp.mean(widened * widened, axis=-1, keepdims=True))
    return ((widened * lax.rsqrt(power + norm_eps)).reshape(row_count, -1) * norm_scale).astype(jnp.bfloat16)

def mamba(m_x, m_z, m_b, m_c, dt_raw, dt_bias, a_log, d_skip, norm_gain):
    sequence_length = m_x.shape[0]
    per_group = MH // MG
    x_all = m_x.reshape(sequence_length, MG, per_group, MP)
    step_all = jax.nn.softplus(dt_raw.astype(jnp.float32) + dt_bias).reshape(sequence_length, MG, per_group)
    rates = jnp.exp(a_log).reshape(MG, per_group)
    b_all = m_b.reshape(sequence_length, MG, MN)
    c_all = m_c.reshape(sequence_length, MG, MN)

    def by_group(packed):
        return ssd_sequence(packed[0], packed[1], packed[2], packed[3], packed[4])
    outputs = lax.map(by_group, (jnp.transpose(x_all, (1, 0, 2, 3)), jnp.transpose(step_all, (1, 0, 2)), rates, jnp.transpose(b_all, (1, 0, 2)), jnp.transpose(c_all, (1, 0, 2))))
    outputs = jnp.transpose(outputs, (1, 0, 2, 3)) + d_skip.reshape(MG, per_group)[None, :, :, None] * x_all.astype(jnp.float32)
    gated = (outputs.reshape(sequence_length, MH * MP) * jax.nn.silu(m_z.astype(jnp.float32))).astype(jnp.bfloat16)
    return gated_norm(gated, norm_gain, MG)

def reference(query, keys, values, m_x, m_z, m_b, m_c, dt_raw, dt_bias, a_log, d_skip, norm_gain):
    context = attention(folded_to_sequence(query), folded_to_sequence(keys), folded_to_sequence(values))
    mixed = mamba(folded_to_sequence(m_x), folded_to_sequence(m_z), folded_to_sequence(m_b), folded_to_sequence(m_c), folded_to_sequence(dt_raw), dt_bias, a_log, d_skip, norm_gain)
    return (context, mixed)
```

```python
import functools
import math

import jax
import jax.numpy as jnp
from jax import lax
from jax.experimental import pallas as pl
from jax.experimental.pallas import tpu as pltpu
from jax.sharding import PartitionSpec as P

HEAD_SIZE = 128
MP = 64
MN = 128
NORM_EPS = 1e-05
MASKED = -1e30
HIGHEST = lax.Precision.HIGHEST
F32 = jnp.float32
BF16 = jnp.bfloat16
INPUT_SPACE = pltpu.HBM
HOP_SLOTS = 2
PIECE = 256


def dot(a, b, ca=1, cb=0, precision=None):
    return lax.dot_general(
        a, b, (((ca,), (cb,)), ((), ())), preferred_element_type=F32, precision=precision
    )


def kernel(
    n, q_in, k_in, v_in, x_in, z_in, b_in, c_in, dt_in, bias_in, alog_in, skip_in,
    gain_in, ctx_out, mix_out,
    q_ref, x_ref, z_ref, b_ref, c_ref, dt_ref, bias_ref, alog_ref, skip_ref, gain_ref,
    kv_all, bias_scr, ctx_stage, arrived, gated, base_scr, er_scr, xdt_scr, hs, runt, gmask,
    buf_a, buf_b, out_a, out_b, sloc_a, sloc_b, tot_a, tot_b, log_in, log_out, wide_t,
    kv_plus, kv_minus, kv_recv, a_send, a_recv, b_send, b_recv, o_send, o_recv, c_send, c_recv,
    log_send, log_recv, load_sem,
):
    me = lax.axis_index("ctx")
    tok = q_ref.shape[0]
    half = tok // 2
    heads = dt_ref.shape[0]
    width = x_ref.shape[1]
    groups = b_ref.shape[1] // MN
    group_width = width // groups
    pieces, _, piece = buf_a.shape
    per_piece = piece // MP
    per_group = group_width // piece
    q_heads = q_ref.shape[1] // HEAD_SIZE
    kv = kv_all.shape[2] // 2
    repeat = q_ref.shape[1] // kv
    mesh_id = pl.DeviceIdType.MESH
    has_left = me > 0
    has_right = me < n - 1

    loads = [
        pltpu.make_async_copy(src, dst, load_sem.at[i])
        for i, (src, dst) in enumerate(
            (
                (dt_in, dt_ref), (bias_in, bias_ref), (alog_in, alog_ref), (skip_in, skip_ref),
                (k_in, kv_all.at[me, :, pl.ds(0, kv)]), (v_in, kv_all.at[me, :, pl.ds(kv, kv)]),
                (b_in, b_ref), (c_in, c_ref), (x_in, x_ref), (z_in, z_ref), (q_in, q_ref),
                (gain_in, gain_ref),
            )
        )
    ]
    for load in loads:
        load.start()

    barrier = pltpu.get_barrier_semaphore()

    def greet(peer):
        pl.semaphore_signal(barrier, inc=1, device_id={"ctx": peer}, device_id_type=mesh_id)

    @pl.when(has_left)
    def _():
        greet(me - 1)

    @pl.when(has_right)
    def _():
        greet(me + 1)

    def remote(src, dst, send, recv, peer):
        return pltpu.make_async_remote_copy(
            src_ref=src, dst_ref=dst, send_sem=send, recv_sem=recv,
            device_id={"ctx": peer}, device_id_type=mesh_id,
        )

    first = pl.ds(0, half)

    def kv_right(s):
        part = kv_all.at[s, first]
        return remote(part, part, kv_plus.at[s], kv_recv.at[s], jnp.minimum(me + 1, n - 1))

    def kv_left(s):
        part = kv_all.at[s]
        return remote(part, part, kv_minus.at[s], kv_recv.at[s], jnp.maximum(me - 1, 0))

    def log_copy():
        return remote(log_out, log_in, log_send, log_recv, jnp.maximum(me - 1, 0))

    row = lax.broadcasted_iota(jnp.int32, (tok, tok), 0)
    col = lax.broadcasted_iota(jnp.int32, (tok, tok), 1)
    for load in loads[:4]:
        load.wait()
    raw = dot((row == col).astype(BF16), dt_ref[...], 1, 1) + bias_ref[...]
    steps = jnp.maximum(raw, 0.0) + jnp.log1p(jnp.exp(-jnp.abs(raw)))
    decay = -steps * jnp.exp(alog_ref[...])
    lower = (col <= row) & ((row < half) == (col < half))
    tri = lower.astype(F32)
    hs[0:tok, :] = dot(tri, decay, precision=HIGHEST)
    hs[tok : 2 * tok, :] = steps
    hs[2 * tok :, :] = jnp.broadcast_to(skip_ref[...], (8, heads))
    runt[...] = dot(decay, tri, 0, 1, precision=HIGHEST)
    own_log = jnp.broadcast_to(hs[half - 1 : half, :] + hs[tok - 1 : tok, :], (8, heads))

    for load in loads[4:6]:
        load.wait()

    pl.semaphore_wait(barrier, has_left.astype(jnp.int32) + has_right.astype(jnp.int32))

    @pl.when(jnp.logical_not(has_right))
    def _():
        log_out[...] = own_log
        log_copy().start()
        kv_left(me).start()

    @pl.when(has_right)
    def _():
        kv_right(me).start()

    @pl.when(has_right & has_left)
    def _():
        kv_left(me).start()

    for load in loads[6:8]:
        load.wait()
    for g in range(groups):
        cols = slice(g * MN, (g + 1) * MN)
        gmask[g] = jnp.where(lower, dot(c_ref[:, cols], b_ref[:, cols], 1, 1), 0.0)

    @pl.when(me == 0)
    def _():
        buf_a[...] = jnp.zeros_like(buf_a)

    @pl.when(me == n - 1)
    def _():
        buf_b[...] = jnp.zeros_like(buf_b)
        wide_t[...] = jnp.ones_like(wide_t)

    lane_head = lax.broadcasted_iota(jnp.int32, (heads, piece), 1) // MP
    head_row = lax.broadcasted_iota(jnp.int32, (heads, piece), 0)
    wide_head = lax.broadcasted_iota(jnp.int32, (heads, per_piece * tok), 1) // tok
    wide_row = lax.broadcasted_iota(jnp.int32, (heads, per_piece * tok), 0)
    left = lax.broadcasted_iota(jnp.int32, (tok, 2 * MP), 1) < MP

    def block_id(which):
        return me if which == 0 else 2 * n - 1 - me

    def put(value, stage, final, rows, cols, send, recv, which):
        owner = block_id(which) // 2
        slot = lax.rem(block_id(which), 2)
        target = pl.ds(pl.multiple_of(slot * half, half), half)

        @pl.when(owner == me)
        def _():
            final[target, cols] = value

        @pl.when(owner != me)
        def _():
            stage[rows, cols] = value
            remote(
                stage.at[rows, cols], final.at[target, cols], send.at[which], recv.at[slot], owner
            ).start()

    def silu(value):
        return value / (1.0 + jnp.exp(-value))

    def prepare(k):
        cols = pl.ds(pl.multiple_of(k * piece, piece), piece)
        gcols = pl.ds(pl.multiple_of((k // per_group) * MN, MN), MN)
        pick = (head_row == k * per_piece + lane_head).astype(F32)
        spread = dot(hs[...], pick, precision=HIGHEST)
        run, step, skip = spread[0:tok], spread[tok : 2 * tok], spread[2 * tok : 2 * tok + 1]
        xs = x_ref[:, cols].astype(F32)
        xdt = xs * step
        last_a, last_b = run[half - 1 : half], run[tok - 1 : tok]
        b_rows = b_ref[:, gcols]
        sloc_a[k] = dot(b_rows[0:half], (xdt[0:half] * jnp.exp(last_a - run[0:half])).astype(BF16), 0, 0)
        sloc_b[k] = dot(b_rows[half:], (xdt[half:] * jnp.exp(last_b - run[half:])).astype(BF16), 0, 0)
        tot_a[k] = jnp.broadcast_to(jnp.exp(last_a), (8, piece))
        tot_b[k] = jnp.broadcast_to(jnp.exp(last_b), (8, piece))
        er_scr[:, cols] = jnp.exp(run)
        xdt_scr[:, cols] = xdt.astype(BF16)
        base_scr[:, cols] = skip * xs

    def within_blocks(k):
        cols = pl.ds(pl.multiple_of(k * piece, piece), piece)
        wide = dot(hs[0:tok, :], (wide_row == k * per_piece + wide_head).astype(F32), precision=HIGHEST)
        gm = gmask[k // per_group]
        inner = []
        for pair in range(per_piece // 2):
            weights = []
            for which in range(2):
                h = 2 * pair + which
                gap = wide[:, h * tok : (h + 1) * tok] - runt[pl.ds(k * per_piece + h, 1), :]
                weights.append((jnp.exp(jnp.minimum(gap, 0.0)) * gm).astype(BF16))
            at = pl.ds(pl.multiple_of(k * piece + pair * 2 * MP, 2 * MP), 2 * MP)
            part = xdt_scr[:, at]
            none = jnp.zeros_like(part)
            stacked = jnp.concatenate([jnp.where(left, part, none), jnp.where(left, none, part)], axis=0)
            inner.append(dot(jnp.concatenate(weights, axis=1), stacked))
        base_scr[:, cols] = base_scr[:, cols] + jnp.concatenate(inner, axis=1)

    def a_copy(k):
        return remote(out_a.at[k], buf_a.at[k], a_send.at[k], a_recv.at[k], jnp.minimum(me + 1, n - 1))

    def b_copy(k):
        return remote(out_b.at[k], buf_b.at[k], b_send.at[k], b_recv.at[k], jnp.maximum(me - 1, 0))

    def step_a(k):
        @pl.when(has_left)
        def _():
            a_copy(k).wait_recv()

        @pl.when(has_right)
        def _():
            out_a[k] = (buf_a[k].astype(F32) * tot_a[k][0:1] + sloc_a[k]).astype(BF16)
            a_copy(k).start()

    def step_b(k):
        cols = pl.ds(pl.multiple_of(k * piece, piece), piece)

        @pl.when(has_right)
        def _():
            b_copy(k).wait_recv()

        @pl.when(has_left)
        def _():
            mine = sloc_a[k] * wide_t[0:1, cols] + buf_b[k].astype(F32)
            out_b[k] = (mine * tot_b[k][0:1] + sloc_b[k]).astype(BF16)
            b_copy(k).start()

    def gate(k, which, state):
        cols = pl.ds(pl.multiple_of(k * piece, piece), piece)
        gcols = pl.ds(pl.multiple_of((k // per_group) * MN, MN), MN)
        rows = slice(which * half, (which + 1) * half)
        carried = dot(c_ref[rows, gcols], state) * er_scr[rows, cols]
        z = z_ref[rows, cols].astype(F32)
        value = ((base_scr[rows, cols] + carried) * silu(z)).astype(BF16)
        put(value, gated, arrived, pl.ds(which * half, half), cols, o_send.at[k], o_recv.at[k], which)

    def gate_a(k):
        gate(k, 0, buf_a[k])

    def gate_b(k):
        cols = pl.ds(pl.multiple_of(k * piece, piece), piece)
        after = buf_a[k].astype(F32) * tot_a[k][0:1] + sloc_a[k]
        entering = after * wide_t[0:1, cols] + buf_b[k].astype(F32)
        gate(k, 1, entering.astype(BF16))

    def take_log():
        @pl.when(has_right)
        def _():
            log_copy().wait_recv()
            later = log_in[...]
            at_head = lax.broadcasted_iota(jnp.int32, (heads, width), 1) // MP
            pick = (lax.broadcasted_iota(jnp.int32, (heads, width), 0) == at_head).astype(F32)

            @pl.when(has_left)
            def _():
                log_out[...] = later + own_log
                log_copy().start()

            wide_t[...] = jnp.exp(dot(later, pick, precision=HIGHEST))

    def relay(h):
        @pl.when(me - h >= 0)
        def _():
            kv_right(jnp.maximum(me - h, 0)).wait_recv()

            @pl.when(has_right)
            def _():
                kv_right(jnp.maximum(me - h, 0)).start()

        @pl.when(me + h < n)
        def _():
            kv_left(jnp.minimum(me + h, n - 1)).wait_recv()

            @pl.when(has_left)
            def _():
                kv_left(jnp.minimum(me + h, n - 1)).start()

    def attention_mask():
        def clear(s, _):
            @pl.when(s < me)
            def _():
                kv_all[s, half:, :] = jnp.zeros((half, 2 * kv), BF16)

            return 0

        lax.fori_loop(0, n, clear, 0)
        key = lax.broadcasted_iota(jnp.int32, (tok, n * tok), 1)
        source = key // tok
        within = key - source * tok
        key_pos = jnp.where(
            within < half, source * half + within, (2 * n - 2 - source) * half + within
        )
        query = lax.broadcasted_iota(jnp.int32, (tok, n * tok), 0)
        query_pos = jnp.where(query < half, me * half + query, (2 * n - 2 - me) * half + query)
        bias_scr[...] = jnp.where(key_pos <= query_pos, 0.0, MASKED)

    scale = 1.0 / math.sqrt(HEAD_SIZE)

    def one_head(h):
        hcols = pl.ds(pl.multiple_of(h * HEAD_SIZE, HEAD_SIZE), HEAD_SIZE)
        kcols = pl.ds(pl.multiple_of((h // repeat) * HEAD_SIZE, HEAD_SIZE), HEAD_SIZE)
        vcols = pl.ds(pl.multiple_of(kv + (h // repeat) * HEAD_SIZE, HEAD_SIZE), HEAD_SIZE)
        keys = kv_all[:, :, kcols].reshape(n * tok, HEAD_SIZE)
        values = kv_all[:, :, vcols].reshape(n * tok, HEAD_SIZE)
        scores = dot(q_ref[:, hcols], keys, 1, 1) * scale + bias_scr[...]
        expo = jnp.exp(scores - jnp.max(scores, axis=-1, keepdims=True))
        total = jnp.sum(expo, axis=-1, keepdims=True)
        value = (dot(expo.astype(BF16), values) / total).astype(BF16)
        for which in range(2):
            rows = slice(which * half, (which + 1) * half)
            put(value[rows], ctx_stage, ctx_out, pl.ds(which * half, half), hcols, c_send.at[h], c_recv.at[h], which)

    for load in loads[8:11]:
        load.wait()
    attention_mask()
    lag_a = me * HOP_SLOTS
    lag_b = (n - 1 - me) * HOP_SLOTS
    lag = jnp.maximum(lag_a, lag_b)
    attend = (n - 1) * HOP_SLOTS
    last = (n - 1) * HOP_SLOTS + max(pieces, q_heads)

    def slot_step(t, _):
        @pl.when(t < pieces)
        def _():
            prepare(t)

        @pl.when((t >= lag_a) & (t < lag_a + pieces))
        def _():
            step_a(t - lag_a)

        @pl.when(t == lag_b)
        def _():
            take_log()

        @pl.when((t >= lag_b) & (t < lag_b + pieces))
        def _():
            step_b(t - lag_b)

        @pl.when((t > 0) & (lax.rem(t, HOP_SLOTS) == 0) & (t <= (n - 1) * HOP_SLOTS))
        def _():
            relay(t // HOP_SLOTS)

        @pl.when(t < pieces)
        def _():
            within_blocks(t)

        @pl.when((t >= lag_a) & (t < lag_a + pieces))
        def _():
            gate_a(t - lag_a)

        @pl.when((t >= lag) & (t < lag + pieces))
        def _():
            gate_b(t - lag)

        @pl.when((t >= attend) & (t < attend + q_heads))
        def _():
            one_head(t - attend)

        return 0

    lax.fori_loop(0, last, slot_step, 0)

    def drain(k, _):
        @pl.when(has_right)
        def _():
            a_copy(k).wait_send()

        @pl.when(has_left)
        def _():
            b_copy(k).wait_send()

        return 0

    lax.fori_loop(0, pieces, drain, 0)

    @pl.when(has_left)
    def _():
        log_copy().wait_send()

    def drain_kv(s, _):
        @pl.when((s <= me) & has_right)
        def _():
            kv_right(s).wait_send()

        @pl.when((s >= me) & has_left)
        def _():
            kv_left(s).wait_send()

        return 0

    lax.fori_loop(0, n, drain_kv, 0)

    def settle(stage, final, cols, send, recv):
        for which in range(2):
            rows = pl.ds(which * half, half)
            copy = remote(stage.at[rows, cols], final.at[rows, cols], send.at[which], recv.at[which], me)

            @pl.when(block_id(which) // 2 != me)
            def _():
                copy.wait_send()

        for slot in range(2):
            source = jnp.where(2 * me + slot < n, 2 * me + slot, 2 * n - 1 - 2 * me - slot)
            rows = pl.ds(slot * half, half)
            copy = remote(stage.at[rows, cols], final.at[rows, cols], send.at[slot], recv.at[slot], me)

            @pl.when(source != me)
            def _():
                copy.wait_recv()

    for h in range(q_heads):
        settle(ctx_stage, ctx_out, pl.ds(h * HEAD_SIZE, HEAD_SIZE), c_send.at[h], c_recv.at[h])
    loads[11].wait()
    for g in range(groups):
        gcols = slice(g * group_width, (g + 1) * group_width)
        for k in range(g * per_group, (g + 1) * per_group):
            settle(gated, arrived, pl.ds(k * piece, piece), o_send.at[k], o_recv.at[k])
        for which in range(2):
            rows = pl.ds(which * half, half)
            value = arrived[rows, gcols].astype(F32)
            power = jnp.mean(value * value, axis=-1, keepdims=True)
            mix_out[rows, gcols] = (value * lax.rsqrt(power + NORM_EPS) * gain_ref[:, gcols]).astype(BF16)


def body(n, query, keys, values, m_x, m_z, m_b, m_c, dt_raw, dt_bias, a_log, d_skip, norm_gain):
    tok, width = m_x.shape
    half = tok // 2
    heads = dt_raw.shape[1]
    anywhere = pl.BlockSpec(memory_space=INPUT_SPACE)
    groups = m_b.shape[1] // MN
    piece = math.gcd(width // groups, PIECE)
    pieces = width // piece
    kv = keys.shape[1]
    q_heads = query.shape[1] // HEAD_SIZE
    dma = pltpu.SemaphoreType.DMA
    vmem = pltpu.VMEM
    state = (pieces, MN, piece)
    spec = pl.BlockSpec(memory_space=pltpu.VMEM)
    return pl.pallas_call(
        functools.partial(kernel, n),
        out_shape=(
            jax.ShapeDtypeStruct(query.shape, BF16),
            jax.ShapeDtypeStruct(m_x.shape, BF16),
        ),
        in_specs=[anywhere] * 12,
        out_specs=(spec, spec),
        scratch_shapes=[
            vmem(query.shape, BF16),
            vmem(m_x.shape, BF16),
            vmem(m_x.shape, BF16),
            vmem(m_b.shape, BF16),
            vmem(m_b.shape, BF16),
            vmem((heads, tok), BF16),
            vmem((1, heads), F32),
            vmem((1, heads), F32),
            vmem((1, heads), F32),
            vmem((1, width), F32),
            vmem((n, tok, 2 * kv), BF16),
            vmem((tok, n * tok), F32),
            vmem(query.shape, BF16),
            vmem(m_x.shape, BF16),
            vmem(m_x.shape, BF16),
            vmem((tok, width), F32),
            vmem((tok, width), F32),
            vmem((tok, width), BF16),
            vmem((2 * tok + 8, heads), F32),
            vmem((heads, tok), F32),
            vmem((groups, tok, tok), F32),
            vmem(state, BF16),
            vmem(state, BF16),
            vmem(state, BF16),
            vmem(state, BF16),
            vmem(state, F32),
            vmem(state, F32),
            vmem((pieces, 8, piece), F32),
            vmem((pieces, 8, piece), F32),
            vmem((8, heads), F32),
            vmem((8, heads), F32),
            vmem((8, width), F32),
            dma((n,)),
            dma((n,)),
            dma((n,)),
            dma((pieces,)),
            dma((pieces,)),
            dma((pieces,)),
            dma((pieces,)),
            dma((pieces, 2)),
            dma((pieces, 2)),
            dma((q_heads, 2)),
            dma((q_heads, 2)),
            dma(()),
            dma(()),
            dma((12,)),
        ],
        compiler_params=pltpu.CompilerParams(
            collective_id=0, has_side_effects=True, vmem_limit_bytes=67043328
        ),
    )(
        query, keys, values, m_x, m_z, m_b, m_c, dt_raw.T,
        dt_bias.reshape(1, -1), a_log.reshape(1, -1), d_skip.reshape(1, -1), norm_gain.reshape(1, -1),
    )


def solution(mesh):
    rows = P(("grp", "ctx"), "hd")
    in_specs = (rows,) * 8 + (P("hd"),) * 4
    return jax.shard_map(
        functools.partial(body, mesh.shape["ctx"]),
        mesh=mesh, in_specs=in_specs, out_specs=(rows, rows), check_vma=False,
    )
```

```python
import functools
import math

import jax
import jax.numpy as jnp
from jax import lax
from jax.experimental import pallas as pl
from jax.experimental.pallas import tpu as pltpu
from jax.sharding import PartitionSpec as P

HEAD_SIZE = 128
MP = 64
MN = 128
NORM_EPS = 1e-05
MASKED = -1e30
HIGHEST = lax.Precision.HIGHEST
F32 = jnp.float32
BF16 = jnp.bfloat16
INPUT_SPACE = pltpu.HBM
PIECE = 256


def dot(a, b, ca=1, cb=0, precision=None):
    return lax.dot_general(
        a, b, (((ca,), (cb,)), ((), ())), preferred_element_type=F32, precision=precision
    )


def split(value):
    high = value.astype(BF16)
    rest = value - high.astype(F32)
    mid = rest.astype(BF16)
    return high, mid, (rest - mid.astype(F32)).astype(BF16)


def kernel(
    n, wide_hd, q_in, k_in, v_in, x_in, z_in, b_in, c_in, dt_in, bias_in, alog_in, skip_in,
    gain_in, ctx_out, mix_out,
    q_ref, x_ref, z_ref, b_ref, c_ref, dt_ref, bias_ref, alog_ref, skip_ref, gain_ref,
    kv_all, bias_scr, ctx_stage, arrived, gated, base_scr, er_scr, xdt_scr, hs, run_split, gmask,
    buf_a, buf_b, out_a, out_b, sloc_a, sloc_b, tot_a, tot_b, log_in, log_out, wide_t,
    kv_plus, kv_minus, kv_recv, a_send, a_recv, b_send, b_recv, o_send, o_recv, c_send, c_recv,
    log_send, log_recv, plus_sem, minus_sem, pair_plus, pair_minus, load_sem,
):
    me = lax.axis_index("ctx")
    tok = q_ref.shape[0]
    half = tok // 2
    heads = dt_ref.shape[0]
    width = x_ref.shape[1]
    groups = b_ref.shape[1] // MN
    group_width = width // groups
    pieces, _, piece = buf_a.shape
    per_piece = piece // MP
    per_group = group_width // piece
    q_heads = q_ref.shape[1] // HEAD_SIZE
    kv = kv_all.shape[2] // 2
    repeat = q_ref.shape[1] // kv
    mesh_id = pl.DeviceIdType.MESH
    core = lax.axis_index("hd")
    paired = wide_hd % 2 == 0
    partner = core + 1 - 2 * lax.rem(core, 2)
    has_left = me > 0
    has_right = me < n - 1

    loads = [
        pltpu.make_async_copy(src, dst, load_sem.at[i])
        for i, (src, dst) in enumerate(
            (
                (dt_in, dt_ref), (bias_in, bias_ref), (alog_in, alog_ref), (skip_in, skip_ref),
                (k_in, kv_all.at[me, :, pl.ds(0, kv)]), (v_in, kv_all.at[me, :, pl.ds(kv, kv)]),
                (b_in, b_ref), (c_in, c_ref), (x_in, x_ref), (z_in, z_ref), (q_in, q_ref),
                (gain_in, gain_ref),
            )
        )
    ]
    for load in loads:
        load.start()

    barrier = pltpu.get_barrier_semaphore()

    def greet(peer):
        pl.semaphore_signal(barrier, inc=1, device_id={"ctx": peer}, device_id_type=mesh_id)

    @pl.when(has_left)
    def _():
        greet(me - 1)

    @pl.when(has_right)
    def _():
        greet(me + 1)

    if paired:
        pl.semaphore_signal(barrier, inc=1, device_id={"hd": partner}, device_id_type=mesh_id)

    def remote(src, dst, send, recv, peer):
        return pltpu.make_async_remote_copy(
            src_ref=src, dst_ref=dst, send_sem=send, recv_sem=recv,
            device_id={"ctx": peer}, device_id_type=mesh_id,
        )

    first = pl.ds(0, half)

    def kv_right(s):
        part = kv_all.at[s, first]
        return remote(part, part, kv_plus.at[s], kv_recv.at[s, 0], jnp.minimum(me + 1, n - 1))

    def kv_left(s):
        copies = []
        for i in range(2):
            part = kv_all.at[s, pl.ds(i * half, half)]
            copies.append(
                remote(part, part, kv_minus.at[s, i], kv_recv.at[s, i], jnp.maximum(me - 1, 0))
            )
        return copies

    def log_copy():
        return remote(log_out, log_in, log_send, log_recv, jnp.maximum(me - 1, 0))

    row = lax.broadcasted_iota(jnp.int32, (tok, tok), 0)
    col = lax.broadcasted_iota(jnp.int32, (tok, tok), 1)
    for load in loads[:4]:
        load.wait()
    raw = dot((row == col).astype(BF16), dt_ref[...], 1, 1) + bias_ref[...]
    steps = jnp.maximum(raw, 0.0) + jnp.log1p(jnp.exp(-jnp.abs(raw)))
    decay = -steps * jnp.exp(alog_ref[...])
    lower = (col <= row) & ((row < half) == (col < half))
    tri = lower.astype(BF16)
    high, mid, low = split(decay)
    run = dot(tri, high) + dot(tri, mid) + dot(tri, low)
    ends = jnp.where(
        lax.broadcasted_iota(jnp.int32, (tok, heads), 0) < half, run[half - 1 : half], run[tok - 1 : tok]
    )

    def keep_split(ref, start, value):
        for i, part in enumerate(split(value)):
            ref[start : start + value.shape[0], i * heads : (i + 1) * heads] = part

    keep_split(run_split, 0, run)
    keep_split(hs, 0, jnp.exp(run))
    keep_split(hs, tok, jnp.exp(ends - run) * steps)
    keep_split(hs, 2 * tok, steps)
    keep_split(hs, 3 * tok, jnp.broadcast_to(skip_ref[...], (16, heads)))
    own_log = jnp.broadcast_to(run[half - 1 : half] + run[tok - 1 : tok], (8, heads))

    for load in loads[4:6]:
        load.wait()

    pl.semaphore_wait(barrier, has_left.astype(jnp.int32) + has_right.astype(jnp.int32) + int(paired))

    @pl.when(jnp.logical_not(has_right))
    def _():
        log_out[...] = own_log
        log_copy().start()

    @pl.when(has_right & has_left)
    def _():
        kv_right(me).start()
        for copy in kv_left(me):
            copy.start()

    for load in loads[6:8]:
        load.wait()
    lanes = per_piece * half
    lane = lax.broadcasted_iota(jnp.int32, (half, lanes), 1)
    source = lane - lane // half * half
    target = lax.broadcasted_iota(jnp.int32, (half, lanes), 0)
    causal = source <= target
    diagonal = source == target
    for g in range(groups):
        cols = slice(g * MN, (g + 1) * MN)
        for which in range(2):
            rows = slice(which * half, (which + 1) * half)
            repeated = jnp.concatenate([b_ref[rows, cols]] * per_piece, axis=0)
            gmask[g, rows, :] = jnp.where(causal, dot(c_ref[rows, cols], repeated, 1, 1), 0.0)

    @pl.when(me == 0)
    def _():
        buf_a[...] = jnp.zeros_like(buf_a)

    @pl.when(me == n - 1)
    def _():
        buf_b[...] = jnp.zeros_like(buf_b)
        wide_t[...] = jnp.ones_like(wide_t)

    split_head = lax.rem(lax.broadcasted_iota(jnp.int32, (3 * heads, piece), 0), heads)
    lane_head = lax.broadcasted_iota(jnp.int32, (3 * heads, piece), 1) // MP
    wide_head = lax.rem(lax.broadcasted_iota(jnp.int32, (3 * heads, lanes), 0), heads)
    wide_lane = lax.broadcasted_iota(jnp.int32, (3 * heads, lanes), 1) // half
    part_head = lax.broadcasted_iota(jnp.int32, (half, piece), 1) // MP

    def block_id(which):
        return me if which == 0 else 2 * n - 1 - me

    def send(stage, final, cols, send_sem, recv_sem, which):
        owner = block_id(which) // 2
        slot = lax.rem(block_id(which), 2)
        rows = pl.ds(which * half, half)
        target = pl.ds(pl.multiple_of(slot * half, half), half)

        @pl.when(owner == me)
        def _():
            final[target, cols] = stage[rows, cols]

        @pl.when(owner != me)
        def _():
            remote(
                stage.at[rows, cols], final.at[target, cols], send_sem.at[which], recv_sem.at[slot], owner
            ).start()

    def silu(value):
        return value / (1.0 + jnp.exp(-value))

    def prepare(k):
        cols = pl.ds(pl.multiple_of(k * piece, piece), piece)
        gcols = pl.ds(pl.multiple_of((k // per_group) * MN, MN), MN)
        spread = dot(hs[...], (split_head == k * per_piece + lane_head).astype(BF16))
        xs = x_ref[:, cols].astype(F32)
        weighted = (xs * spread[tok : 2 * tok]).astype(BF16)
        b_rows = b_ref[:, gcols]
        sloc_a[k] = dot(b_rows[0:half], weighted[0:half], 0, 0)
        sloc_b[k] = dot(b_rows[half:], weighted[half:], 0, 0)
        tot_a[k] = jnp.broadcast_to(spread[half - 1 : half], (8, piece))
        tot_b[k] = jnp.broadcast_to(spread[tok - 1 : tok], (8, piece))
        er_scr[:, cols] = spread[0:tok]
        xdt_scr[:, cols] = (xs * spread[2 * tok : 3 * tok]).astype(BF16)
        base_scr[:, cols] = spread[3 * tok : 3 * tok + 1] * xs

    def within_blocks(k):
        cols = pl.ds(pl.multiple_of(k * piece, piece), piece)
        wide = dot(run_split[...], (wide_head == k * per_piece + wide_lane).astype(BF16))
        for which in range(2):
            rows = slice(which * half, (which + 1) * half)
            mine = wide[rows]
            gap = mine - jnp.sum(jnp.where(diagonal, mine, 0.0), axis=0, keepdims=True)
            weights = (jnp.exp(jnp.minimum(gap, 0.0)) * gmask[k // per_group, rows, :]).astype(BF16)
            part = xdt_scr[rows, cols]
            none = jnp.zeros_like(part)
            stacked = jnp.concatenate(
                [jnp.where(part_head == h, part, none) for h in range(per_piece)], axis=0
            )
            base_scr[rows, cols] = base_scr[rows, cols] + dot(weights, stacked)

    def a_copy(k):
        return remote(out_a.at[k], buf_a.at[k], a_send.at[k], a_recv.at[k], jnp.minimum(me + 1, n - 1))

    def b_copy(k):
        return remote(out_b.at[k], buf_b.at[k], b_send.at[k], b_recv.at[k], jnp.maximum(me - 1, 0))

    def step_a(k):
        @pl.when(has_left)
        def _():
            a_copy(k).wait_recv()

        @pl.when(has_right)
        def _():
            out_a[k] = (buf_a[k].astype(F32) * tot_a[k][0:1] + sloc_a[k]).astype(BF16)
            a_copy(k).start()

    def step_b(k):
        cols = pl.ds(pl.multiple_of(k * piece, piece), piece)

        @pl.when(has_right)
        def _():
            b_copy(k).wait_recv()

        @pl.when(has_left)
        def _():
            mine = sloc_a[k] * wide_t[0:1, cols] + buf_b[k].astype(F32)
            out_b[k] = (mine * tot_b[k][0:1] + sloc_b[k]).astype(BF16)
            b_copy(k).start()

    def gate(k, which, state):
        cols = pl.ds(pl.multiple_of(k * piece, piece), piece)
        gcols = pl.ds(pl.multiple_of((k // per_group) * MN, MN), MN)
        rows = slice(which * half, (which + 1) * half)
        carried = dot(c_ref[rows, gcols], state) * er_scr[rows, cols]
        z = z_ref[rows, cols].astype(F32)
        value = ((base_scr[rows, cols] + carried) * silu(z)).astype(BF16)
        gated[rows, cols] = value

    def send_gated(k):
        cols = pl.ds(pl.multiple_of(k * piece, piece), piece)
        for which in range(2):
            send(gated, arrived, cols, o_send.at[k], o_recv.at[k], which)

    def gate_a(k):
        gate(k, 0, buf_a[k])

    def gate_b(k):
        cols = pl.ds(pl.multiple_of(k * piece, piece), piece)
        after = buf_a[k].astype(F32) * tot_a[k][0:1] + sloc_a[k]
        entering = after * wide_t[0:1, cols] + buf_b[k].astype(F32)
        gate(k, 1, entering.astype(BF16))

    def take_log():
        @pl.when(has_right)
        def _():
            log_copy().wait_recv()
            later = log_in[...]
            @pl.when(has_left)
            def _():
                log_out[...] = later + own_log
                log_copy().start()

            shape = (heads, width)
            pick = lax.broadcasted_iota(jnp.int32, shape, 0) == lax.broadcasted_iota(jnp.int32, shape, 1) // MP
            high, mid, low = split(jnp.exp(later))
            pick = pick.astype(BF16)
            wide_t[...] = dot(high, pick) + dot(mid, pick) + dot(low, pick)

    def relay_right(h):
        source = jnp.maximum(me - h, 0)

        @pl.when(source != me)
        def _():
            kv_right(source).wait_recv()

        @pl.when(has_right)
        def _():
            kv_right(source).start()

    def relay_left(h):
        source = jnp.minimum(me + h, n - 1)
        for copy in kv_left(source):
            @pl.when(source != me)
            def _(copy=copy):
                copy.wait_recv()

            @pl.when(has_left)
            def _(copy=copy):
                copy.start()

    def attention_mask():
        def clear(s, _):
            @pl.when(s < me)
            def _():
                kv_all[s, half:, :] = jnp.zeros((half, 2 * kv), BF16)

            return 0

        lax.fori_loop(0, n, clear, 0)
        key = lax.broadcasted_iota(jnp.int32, (tok, n * tok), 1)
        source = key // tok
        within = key - source * tok
        key_pos = jnp.where(
            within < half, source * half + within, (2 * n - 2 - source) * half + within
        )
        query = lax.broadcasted_iota(jnp.int32, (tok, n * tok), 0)
        query_pos = jnp.where(query < half, me * half + query, (2 * n - 2 - me) * half + query)
        bias_scr[...] = jnp.where(key_pos <= query_pos, 0.0, MASKED)

    scale = 1.0 / math.sqrt(HEAD_SIZE)

    def one_head(h):
        hcols = pl.ds(pl.multiple_of(h * HEAD_SIZE, HEAD_SIZE), HEAD_SIZE)
        kcols = pl.ds(pl.multiple_of((h // repeat) * HEAD_SIZE, HEAD_SIZE), HEAD_SIZE)
        vcols = pl.ds(pl.multiple_of(kv + (h // repeat) * HEAD_SIZE, HEAD_SIZE), HEAD_SIZE)
        keys = kv_all[:, :, kcols].reshape(n * tok, HEAD_SIZE)
        values = kv_all[:, :, vcols].reshape(n * tok, HEAD_SIZE)
        scores = dot(q_ref[:, hcols], keys, 1, 1) * scale + bias_scr[...]
        expo = jnp.exp(scores - jnp.max(scores, axis=-1, keepdims=True))
        total = jnp.sum(expo, axis=-1, keepdims=True)
        ctx_stage[:, hcols] = (dot(expo.astype(BF16), values) / total).astype(BF16)

    def send_ctx():
        for which in range(2):
            send(ctx_stage, ctx_out, slice(None), c_send, c_recv, which)

    for load in loads[8:11]:
        load.wait()
    attention_mask()
    hops = n - 1 - me
    middle = pieces // 2

    def first_step(k, _):
        prepare(k)

        @pl.when((k == middle) & (me == 0))
        def _():
            relay_right(0)

        @pl.when((k == middle) & (me == n - 1))
        def _():
            relay_left(0)

        @pl.when(me == 0)
        def _():
            step_a(k)

        @pl.when(me == n - 1)
        def _():
            step_b(k)

        return 0

    lax.fori_loop(0, pieces, first_step, 0)

    def base(distance):
        return (9 * jnp.maximum(distance - 1, 0)) // 4

    lag_a = base(me)
    lag_b = base(hops)
    block_b = 2 * n - 1 - me
    hold_plus = block_b // 2 - 1 > me
    hold_minus = me // 2 + 1 < me
    gap = jnp.where(hops > 1, 2, 1)
    attend = 1 + jnp.maximum(
        jnp.where(has_left, lag_a + middle, 0), jnp.where(has_right, lag_b + middle + gap, 0)
    )
    gates = jnp.maximum(lag_a + middle + 1, lag_b + middle + gap + 1)
    gates = gates + jnp.where(2 * me < n, jnp.where(has_left, 2, 1), jnp.where(has_right, 3, 1))
    gates = jnp.maximum(gates, jnp.where(hold_plus, lag_a + pieces + 1, 0))
    gates = jnp.maximum(gates, jnp.where(hold_minus, lag_b + pieces + gap + 1, 0))
    place_ctx = jnp.maximum(attend + q_heads // 2 - 1, gates)
    last = functools.reduce(jnp.maximum, [
        lag_a + pieces + 2, lag_b + pieces + gap + 2, attend + q_heads // 2, place_ctx + 1,
        gates + middle, 3 * n,
    ])

    def passed(pair_sem, sem, peers, wait):
        any_peer = functools.reduce(jnp.logical_or, [ok for _, ok in peers])

        @pl.when(any_peer)
        def _():
            if paired and not wait:
                pl.semaphore_signal(pair_sem, inc=1, device_id={"hd": partner}, device_id_type=mesh_id)
            elif paired:
                pl.semaphore_wait(pair_sem, 1)

        if wait:
            for peer, ok in peers:
                @pl.when(ok)
                def _(peer=peer):
                    pl.semaphore_signal(sem, inc=1, device_id={"ctx": peer}, device_id_type=mesh_id)

    plus_peers = [(p, (p >= 0) & (p < me)) for p in (2 * n - 3 - 2 * me, 2 * n - 4 - 2 * me)]
    minus_peers = [(p, (p > me) & (p < n)) for p in (2 * me - 2, 2 * me - 1)]
    plus_peers = [(p, ok & has_right) for p, ok in plus_peers]
    minus_peers = [(p, ok & has_left) for p, ok in minus_peers]

    def chain_a(t):
        at = t - lag_a

        @pl.when((at == middle) & has_left)
        def _():
            relay_right(me)

        k = jnp.where(at < middle, at, at - 1)

        @pl.when((at >= 0) & (at <= pieces) & (at != middle) & has_left)
        def _():
            step_a(k)

        @pl.when((at == pieces) & has_left)
        def _():
            passed(pair_plus, plus_sem, plus_peers, False)

        @pl.when((at == pieces + 1) & has_left)
        def _():
            passed(pair_plus, plus_sem, plus_peers, True)

    def chain_b(t):
        at = t - lag_b

        @pl.when((at == 0) & has_right)
        def _():
            take_log()

        @pl.when((at == middle + gap) & has_right)
        def _():
            relay_left(hops)

        k = jnp.where(at < middle, at, at - gap - 1)

        @pl.when(((at >= 0) & (at < middle) | (at > middle + gap) & (at <= pieces + gap)) & has_right)
        def _():
            step_b(k)

        @pl.when((at == pieces + gap) & has_right)
        def _():
            passed(pair_minus, minus_sem, minus_peers, False)

        @pl.when((at == pieces + gap + 1) & has_right)
        def _():
            passed(pair_minus, minus_sem, minus_peers, True)

    def slot_step(t, _):
        @pl.when(2 * me >= n)
        def _():
            chain_b(t)

        chain_a(t)

        @pl.when(2 * me < n)
        def _():
            chain_b(t)

        for h in range(1, n - 1):
            @pl.when((t == 2 * h - 2) & (h < me))
            def _(h=h):
                relay_right(h)

            @pl.when((t == 3 * h - 2) & (h < hops))
            def _(h=h):
                relay_left(h)

        @pl.when(t < pieces)
        def _():
            within_blocks(t)

        @pl.when((t >= attend) & (t < attend + q_heads // 2))
        def _():
            one_head(2 * (t - attend))
            one_head(2 * (t - attend) + 1)

        @pl.when((t == gates) & hold_plus)
        def _():
            pl.semaphore_wait(plus_sem, 1)

        @pl.when((t == gates) & hold_minus)
        def _():
            pl.semaphore_wait(minus_sem, 1)

        @pl.when(t == place_ctx)
        def _():
            send_ctx()

        @pl.when((t >= gates) & (t < gates + middle))
        def _():
            for i in range(2):
                gate_a(2 * (t - gates) + i)
                gate_b(2 * (t - gates) + i)
            for i in range(2):
                send_gated(2 * (t - gates) + i)

        return 0

    lax.fori_loop(0, last, slot_step, 0)

    def drain(k, _):
        @pl.when(has_right)
        def _():
            a_copy(k).wait_send()

        @pl.when(has_left)
        def _():
            b_copy(k).wait_send()

        return 0

    lax.fori_loop(0, pieces, drain, 0)

    @pl.when(has_left)
    def _():
        log_copy().wait_send()

    def drain_kv(s, _):
        @pl.when((s <= me) & has_right)
        def _():
            kv_right(s).wait_send()

        @pl.when((s >= me) & has_left)
        def _():
            for copy in kv_left(s):
                copy.wait_send()

        return 0

    lax.fori_loop(0, n, drain_kv, 0)

    def settle(stage, final, cols, send_sem, recv_sem):
        for which in range(2):
            rows = pl.ds(which * half, half)
            copy = remote(stage.at[rows, cols], final.at[rows, cols], send_sem.at[which], recv_sem.at[which], me)

            @pl.when(block_id(which) // 2 != me)
            def _():
                copy.wait_send()

        for slot in range(2):
            source = jnp.where(2 * me + slot < n, 2 * me + slot, 2 * n - 1 - 2 * me - slot)
            rows = pl.ds(slot * half, half)
            copy = remote(stage.at[rows, cols], final.at[rows, cols], send_sem.at[slot], recv_sem.at[slot], me)

            @pl.when(source != me)
            def _():
                copy.wait_recv()

    settle(ctx_stage, ctx_out, slice(None), c_send, c_recv)
    loads[11].wait()
    for g in range(groups):
        gcols = slice(g * group_width, (g + 1) * group_width)
        for k in range(g * per_group, (g + 1) * per_group):
            settle(gated, arrived, pl.ds(k * piece, piece), o_send.at[k], o_recv.at[k])
        for which in range(2):
            rows = pl.ds(which * half, half)
            value = arrived[rows, gcols].astype(F32)
            power = jnp.mean(value * value, axis=-1, keepdims=True)
            mix_out[rows, gcols] = (value * lax.rsqrt(power + NORM_EPS) * gain_ref[:, gcols]).astype(BF16)


def body(n, wide_hd, query, keys, values, m_x, m_z, m_b, m_c, dt_raw, dt_bias, a_log, d_skip, norm_gain):
    tok, width = m_x.shape
    half = tok // 2
    heads = dt_raw.shape[1]
    anywhere = pl.BlockSpec(memory_space=INPUT_SPACE)
    groups = m_b.shape[1] // MN
    piece = math.gcd(width // groups, PIECE)
    pieces = width // piece
    kv = keys.shape[1]
    q_heads = query.shape[1] // HEAD_SIZE
    dma = pltpu.SemaphoreType.DMA
    vmem = pltpu.VMEM
    state = (pieces, MN, piece)
    spec = pl.BlockSpec(memory_space=pltpu.VMEM)
    return pl.pallas_call(
        functools.partial(kernel, n, wide_hd),
        out_shape=(
            jax.ShapeDtypeStruct(query.shape, BF16),
            jax.ShapeDtypeStruct(m_x.shape, BF16),
        ),
        in_specs=[anywhere] * 12,
        out_specs=(spec, spec),
        scratch_shapes=[
            vmem(query.shape, BF16),
            vmem(m_x.shape, BF16),
            vmem(m_x.shape, BF16),
            vmem(m_b.shape, BF16),
            vmem(m_b.shape, BF16),
            vmem((heads, tok), BF16),
            vmem((1, heads), F32),
            vmem((1, heads), F32),
            vmem((1, heads), F32),
            vmem((1, width), F32),
            vmem((n, tok, 2 * kv), BF16),
            vmem((tok, n * tok), F32),
            vmem(query.shape, BF16),
            vmem(m_x.shape, BF16),
            vmem(m_x.shape, BF16),
            vmem((tok, width), F32),
            vmem((tok, width), F32),
            vmem((tok, width), BF16),
            vmem((3 * tok + 16, 3 * heads), BF16),
            vmem((tok, 3 * heads), BF16),
            vmem((groups, tok, piece // MP * (tok // 2)), F32),
            vmem(state, BF16),
            vmem(state, BF16),
            vmem(state, BF16),
            vmem(state, BF16),
            vmem(state, F32),
            vmem(state, F32),
            vmem((pieces, 8, piece), F32),
            vmem((pieces, 8, piece), F32),
            vmem((8, heads), F32),
            vmem((8, heads), F32),
            vmem((8, width), F32),
            dma((n,)),
            dma((n, 2)),
            dma((n, 2)),
            dma((pieces,)),
            dma((pieces,)),
            dma((pieces,)),
            dma((pieces,)),
            dma((pieces, 2)),
            dma((pieces, 2)),
            dma((2,)),
            dma((2,)),
            dma(()),
            dma(()),
            pltpu.SemaphoreType.REGULAR,
            pltpu.SemaphoreType.REGULAR,
            pltpu.SemaphoreType.REGULAR,
            pltpu.SemaphoreType.REGULAR,
            dma((12,)),
        ],
        compiler_params=pltpu.CompilerParams(
            collective_id=0, has_side_effects=True, vmem_limit_bytes=67043328
        ),
    )(
        query, keys, values, m_x, m_z, m_b, m_c, dt_raw.T,
        dt_bias.reshape(1, -1), a_log.reshape(1, -1), d_skip.reshape(1, -1), norm_gain.reshape(1, -1),
    )


def solution(mesh):
    rows = P(("grp", "ctx"), "hd")
    in_specs = (rows,) * 8 + (P("hd"),) * 4
    return jax.shard_map(
        functools.partial(body, mesh.shape["ctx"], mesh.shape["hd"]),
        mesh=mesh, in_specs=in_specs, out_specs=(rows, rows), check_vma=False,
    )
```

```python
import functools
import math

import jax
import jax.numpy as jnp
from jax import lax
from jax.experimental import pallas as pl
from jax.experimental.pallas import tpu as pltpu
from jax.sharding import PartitionSpec as P

HEAD_SIZE = 128
MP = 64
MN = 128
NORM_EPS = 1e-05
MASKED = -1e30
HIGHEST = lax.Precision.HIGHEST
F32 = jnp.float32
BF16 = jnp.bfloat16
INPUT_SPACE = pltpu.HBM
PIECE = 256
VMEM_BYTES = 67043328


def dot(a, b, ca=1, cb=0, precision=None):
    return lax.dot_general(
        a, b, (((ca,), (cb,)), ((), ())), preferred_element_type=F32, precision=precision
    )


def split(value):
    high = value.astype(BF16)
    rest = value - high.astype(F32)
    mid = rest.astype(BF16)
    return high, mid, (rest - mid.astype(F32)).astype(BF16)


def kernel(
    n, wide_hd, q_in, k_in, v_in, x_in, z_in, b_in, c_in, dt_in, bias_in, alog_in, skip_in,
    gain_in, ctx_out, arrived, gain_ref,
    q_ref, x_ref, z_ref, b_ref, c_ref, dt_ref, bias_ref, alog_ref, skip_ref,
    kv_all, bias_scr, ctx_stage, gated, base_scr, er_scr, xdt_scr, hs, run_split, gmask,
    buf_a, buf_b, out_a, out_b, sloc_a, sloc_b, tot_a, tot_b, log_in, log_out, wide_t,
    kv_plus, kv_minus, kv_recv, a_send, a_recv, b_send, b_recv, o_send, o_recv, c_send, c_recv,
    log_send, log_recv, plus_sem, minus_sem, pair_plus, pair_minus, load_sem,
):
    me = lax.axis_index("ctx")
    tok = q_ref.shape[0]
    half = tok // 2
    heads = dt_ref.shape[0]
    width = x_ref.shape[1]
    groups = b_ref.shape[1] // MN
    group_width = width // groups
    pieces, _, piece = buf_a.shape
    per_piece = piece // MP
    per_group = group_width // piece
    q_heads = q_ref.shape[1] // HEAD_SIZE
    kv = kv_all.shape[2] // 2
    repeat = q_ref.shape[1] // kv
    mesh_id = pl.DeviceIdType.MESH
    core = lax.axis_index("hd")
    paired = wide_hd % 2 == 0
    partner = core + 1 - 2 * lax.rem(core, 2)
    has_left = me > 0
    has_right = me < n - 1

    loads = [
        pltpu.make_async_copy(src, dst, load_sem.at[i])
        for i, (src, dst) in enumerate(
            (
                (dt_in, dt_ref), (bias_in, bias_ref), (alog_in, alog_ref), (skip_in, skip_ref),
                (k_in, kv_all.at[me, :, pl.ds(0, kv)]), (v_in, kv_all.at[me, :, pl.ds(kv, kv)]),
                (b_in, b_ref), (c_in, c_ref), (x_in, x_ref), (z_in, z_ref), (q_in, q_ref),
                (gain_in, gain_ref),
            )
        )
    ]
    for load in loads:
        load.start()

    barrier = pltpu.get_barrier_semaphore()

    def greet(peer):
        pl.semaphore_signal(barrier, inc=1, device_id={"ctx": peer}, device_id_type=mesh_id)

    @pl.when(has_left)
    def _():
        greet(me - 1)

    @pl.when(has_right)
    def _():
        greet(me + 1)

    if paired:
        pl.semaphore_signal(barrier, inc=1, device_id={"hd": partner}, device_id_type=mesh_id)

    def remote(src, dst, send, recv, peer):
        return pltpu.make_async_remote_copy(
            src_ref=src, dst_ref=dst, send_sem=send, recv_sem=recv,
            device_id={"ctx": peer}, device_id_type=mesh_id,
        )

    first = pl.ds(0, half)

    def kv_right(s):
        part = kv_all.at[s, first]
        return remote(part, part, kv_plus.at[s], kv_recv.at[s, 0], jnp.minimum(me + 1, n - 1))

    def kv_left(s):
        copies = []
        for i in range(2):
            part = kv_all.at[s, pl.ds(i * half, half)]
            copies.append(
                remote(part, part, kv_minus.at[s, i], kv_recv.at[s, i], jnp.maximum(me - 1, 0))
            )
        return copies

    def log_copy():
        return remote(log_out, log_in, log_send, log_recv, jnp.maximum(me - 1, 0))

    row = lax.broadcasted_iota(jnp.int32, (tok, tok), 0)
    col = lax.broadcasted_iota(jnp.int32, (tok, tok), 1)
    for load in loads[:4]:
        load.wait()
    raw = dot((row == col).astype(BF16), dt_ref[...], 1, 1) + bias_ref[...]
    steps = jnp.maximum(raw, 0.0) + jnp.log1p(jnp.exp(-jnp.abs(raw)))
    decay = -steps * jnp.exp(alog_ref[...])
    lower = (col <= row) & ((row < half) == (col < half))
    tri = lower.astype(BF16)
    high, mid, low = split(decay)
    run = dot(tri, high) + dot(tri, mid) + dot(tri, low)
    ends = jnp.where(
        lax.broadcasted_iota(jnp.int32, (tok, heads), 0) < half, run[half - 1 : half], run[tok - 1 : tok]
    )

    def keep_split(ref, start, value):
        for i, part in enumerate(split(value)):
            ref[start : start + value.shape[0], i * heads : (i + 1) * heads] = part

    keep_split(run_split, 0, run)
    keep_split(hs, 0, jnp.exp(run))
    keep_split(hs, tok, jnp.exp(ends - run) * steps)
    keep_split(hs, 2 * tok, steps)
    keep_split(hs, 3 * tok, jnp.broadcast_to(skip_ref[...], (16, heads)))
    own_log = jnp.broadcast_to(run[half - 1 : half] + run[tok - 1 : tok], (8, heads))

    for load in loads[4:6]:
        load.wait()

    pl.semaphore_wait(barrier, has_left.astype(jnp.int32) + has_right.astype(jnp.int32) + int(paired))

    @pl.when(jnp.logical_not(has_right))
    def _():
        log_out[...] = own_log
        log_copy().start()

    @pl.when(has_right & has_left)
    def _():
        kv_right(me).start()
        for copy in kv_left(me):
            copy.start()

    for load in loads[6:8]:
        load.wait()
    lanes = per_piece * half
    lane = lax.broadcasted_iota(jnp.int32, (half, lanes), 1)
    source = lane - lane // half * half
    target = lax.broadcasted_iota(jnp.int32, (half, lanes), 0)
    causal = source <= target
    diagonal = source == target
    for g in range(groups):
        cols = slice(g * MN, (g + 1) * MN)
        for which in range(2):
            rows = slice(which * half, (which + 1) * half)
            repeated = jnp.concatenate([b_ref[rows, cols]] * per_piece, axis=0)
            gmask[g, rows, :] = jnp.where(causal, dot(c_ref[rows, cols], repeated, 1, 1), 0.0)

    @pl.when(me == 0)
    def _():
        buf_a[...] = jnp.zeros_like(buf_a)

    @pl.when(me == n - 1)
    def _():
        buf_b[...] = jnp.zeros_like(buf_b)
        wide_t[...] = jnp.ones_like(wide_t)

    split_head = lax.rem(lax.broadcasted_iota(jnp.int32, (3 * heads, piece), 0), heads)
    lane_head = lax.broadcasted_iota(jnp.int32, (3 * heads, piece), 1) // MP
    wide_head = lax.rem(lax.broadcasted_iota(jnp.int32, (3 * heads, lanes), 0), heads)
    wide_lane = lax.broadcasted_iota(jnp.int32, (3 * heads, lanes), 1) // half
    part_head = lax.broadcasted_iota(jnp.int32, (half, piece), 1) // MP

    def block_id(which):
        return me if which == 0 else 2 * n - 1 - me

    def send(stage, final, cols, send_sem, recv_sem, which):
        owner = block_id(which) // 2
        slot = lax.rem(block_id(which), 2)
        rows = pl.ds(which * half, half)
        target = pl.ds(pl.multiple_of(slot * half, half), half)

        @pl.when(owner == me)
        def _():
            final[target, cols] = stage[rows, cols]

        @pl.when(owner != me)
        def _():
            remote(
                stage.at[rows, cols], final.at[target, cols], send_sem.at[which], recv_sem.at[slot], owner
            ).start()

    def silu(value):
        return value / (1.0 + jnp.exp(-value))

    def prepare(k):
        cols = pl.ds(pl.multiple_of(k * piece, piece), piece)
        gcols = pl.ds(pl.multiple_of((k // per_group) * MN, MN), MN)
        spread = dot(hs[...], (split_head == k * per_piece + lane_head).astype(BF16))
        xs = x_ref[:, cols].astype(F32)
        weighted = (xs * spread[tok : 2 * tok]).astype(BF16)
        b_rows = b_ref[:, gcols]
        sloc_a[k] = dot(b_rows[0:half], weighted[0:half], 0, 0)
        sloc_b[k] = dot(b_rows[half:], weighted[half:], 0, 0)
        tot_a[k] = jnp.broadcast_to(spread[half - 1 : half], (8, piece))
        tot_b[k] = jnp.broadcast_to(spread[tok - 1 : tok], (8, piece))
        er_scr[:, cols] = spread[0:tok]
        xdt_scr[:, cols] = (xs * spread[2 * tok : 3 * tok]).astype(BF16)
        base_scr[:, cols] = spread[3 * tok : 3 * tok + 1] * xs

    def within_blocks(k):
        cols = pl.ds(pl.multiple_of(k * piece, piece), piece)
        wide = dot(run_split[...], (wide_head == k * per_piece + wide_lane).astype(BF16))
        for which in range(2):
            rows = slice(which * half, (which + 1) * half)
            mine = wide[rows]
            gap = mine - jnp.sum(jnp.where(diagonal, mine, 0.0), axis=0, keepdims=True)
            weights = (jnp.exp(jnp.minimum(gap, 0.0)) * gmask[k // per_group, rows, :]).astype(BF16)
            part = xdt_scr[rows, cols]
            none = jnp.zeros_like(part)
            stacked = jnp.concatenate(
                [jnp.where(part_head == h, part, none) for h in range(per_piece)], axis=0
            )
            base_scr[rows, cols] = base_scr[rows, cols] + dot(weights, stacked)

    def a_copy(k):
        return remote(out_a.at[k], buf_a.at[k], a_send.at[k], a_recv.at[k], jnp.minimum(me + 1, n - 1))

    def b_copy(k):
        return remote(out_b.at[k], buf_b.at[k], b_send.at[k], b_recv.at[k], jnp.maximum(me - 1, 0))

    def step_a(k):
        @pl.when(has_left)
        def _():
            a_copy(k).wait_recv()

        @pl.when(has_right)
        def _():
            out_a[k] = (buf_a[k].astype(F32) * tot_a[k][0:1] + sloc_a[k]).astype(BF16)
            a_copy(k).start()

    def step_b(k):
        cols = pl.ds(pl.multiple_of(k * piece, piece), piece)

        @pl.when(has_right)
        def _():
            b_copy(k).wait_recv()

        @pl.when(has_left)
        def _():
            mine = sloc_a[k] * wide_t[0:1, cols] + buf_b[k].astype(F32)
            out_b[k] = (mine * tot_b[k][0:1] + sloc_b[k]).astype(BF16)
            b_copy(k).start()

    def gate(k, which, state):
        cols = pl.ds(pl.multiple_of(k * piece, piece), piece)
        gcols = pl.ds(pl.multiple_of((k // per_group) * MN, MN), MN)
        rows = slice(which * half, (which + 1) * half)
        carried = dot(c_ref[rows, gcols], state) * er_scr[rows, cols]
        z = z_ref[rows, cols].astype(F32)
        value = ((base_scr[rows, cols] + carried) * silu(z)).astype(BF16)
        gated[rows, cols] = value

    def send_gated(k):
        cols = pl.ds(pl.multiple_of(k * piece, piece), piece)
        for which in range(2):
            send(gated, arrived, cols, o_send.at[k], o_recv.at[k], which)

    def gate_a(k):
        gate(k, 0, buf_a[k])

    def gate_b(k):
        cols = pl.ds(pl.multiple_of(k * piece, piece), piece)
        after = buf_a[k].astype(F32) * tot_a[k][0:1] + sloc_a[k]
        entering = after * wide_t[0:1, cols] + buf_b[k].astype(F32)
        gate(k, 1, entering.astype(BF16))

    def take_log():
        @pl.when(has_right)
        def _():
            log_copy().wait_recv()
            later = log_in[...]
            @pl.when(has_left)
            def _():
                log_out[...] = later + own_log
                log_copy().start()

            shape = (heads, width)
            pick = lax.broadcasted_iota(jnp.int32, shape, 0) == lax.broadcasted_iota(jnp.int32, shape, 1) // MP
            high, mid, low = split(jnp.exp(later))
            pick = pick.astype(BF16)
            wide_t[...] = dot(high, pick) + dot(mid, pick) + dot(low, pick)

    def relay_right(h):
        source = jnp.maximum(me - h, 0)

        @pl.when(source != me)
        def _():
            kv_right(source).wait_recv()

        @pl.when(has_right)
        def _():
            kv_right(source).start()

    def relay_left(h):
        source = jnp.minimum(me + h, n - 1)
        for copy in kv_left(source):
            @pl.when(source != me)
            def _(copy=copy):
                copy.wait_recv()

            @pl.when(has_left)
            def _(copy=copy):
                copy.start()

    def attention_mask():
        def clear(s, _):
            @pl.when(s < me)
            def _():
                kv_all[s, half:, :] = jnp.zeros((half, 2 * kv), BF16)

            return 0

        lax.fori_loop(0, n, clear, 0)
        key = lax.broadcasted_iota(jnp.int32, (tok, n * tok), 1)
        source = key // tok
        within = key - source * tok
        key_pos = jnp.where(
            within < half, source * half + within, (2 * n - 2 - source) * half + within
        )
        query = lax.broadcasted_iota(jnp.int32, (tok, n * tok), 0)
        query_pos = jnp.where(query < half, me * half + query, (2 * n - 2 - me) * half + query)
        bias_scr[...] = jnp.where(key_pos <= query_pos, 0.0, MASKED)

    scale = 1.0 / math.sqrt(HEAD_SIZE)

    def one_head(h):
        hcols = pl.ds(pl.multiple_of(h * HEAD_SIZE, HEAD_SIZE), HEAD_SIZE)
        kcols = pl.ds(pl.multiple_of((h // repeat) * HEAD_SIZE, HEAD_SIZE), HEAD_SIZE)
        vcols = pl.ds(pl.multiple_of(kv + (h // repeat) * HEAD_SIZE, HEAD_SIZE), HEAD_SIZE)
        keys = kv_all[:, :, kcols].reshape(n * tok, HEAD_SIZE)
        values = kv_all[:, :, vcols].reshape(n * tok, HEAD_SIZE)
        scores = dot(q_ref[:, hcols], keys, 1, 1) * scale + bias_scr[...]
        expo = jnp.exp(scores - jnp.max(scores, axis=-1, keepdims=True))
        total = jnp.sum(expo, axis=-1, keepdims=True)
        ctx_stage[:, hcols] = (dot(expo.astype(BF16), values) / total).astype(BF16)

    def send_ctx():
        for which in range(2):
            send(ctx_stage, ctx_out, slice(None), c_send, c_recv, which)

    for load in loads[8:11]:
        load.wait()
    attention_mask()
    hops = n - 1 - me
    middle = pieces // 2

    def first_step(k, _):
        prepare(k)

        @pl.when((k == middle) & (me == 0))
        def _():
            relay_right(0)

        @pl.when((k == middle) & (me == n - 1))
        def _():
            relay_left(0)

        @pl.when(me == 0)
        def _():
            step_a(k)

        @pl.when(me == n - 1)
        def _():
            step_b(k)

        return 0

    lax.fori_loop(0, pieces, first_step, 0)

    def base(distance):
        return (9 * jnp.maximum(distance - 1, 0)) // 4

    lag_a = base(me)
    lag_b = base(hops)
    block_b = 2 * n - 1 - me
    hold_plus = block_b // 2 - 1 > me
    hold_minus = me // 2 + 1 < me
    gap = jnp.where(hops > 1, 2, 1)
    attend = 1 + jnp.maximum(
        jnp.where(has_left, lag_a + middle, 0), jnp.where(has_right, lag_b + middle + gap, 0)
    )
    gates = jnp.maximum(lag_a + middle + 1, lag_b + middle + gap + 1)
    gates = gates + jnp.where(2 * me < n, jnp.where(has_left, 2, 1), jnp.where(has_right, 3, 1))
    gates = jnp.maximum(gates, jnp.where(hold_plus, lag_a + pieces + 1, 0))
    gates = jnp.maximum(gates, jnp.where(hold_minus, lag_b + pieces + gap + 1, 0))
    place_ctx = jnp.maximum(attend + q_heads // 2 - 1, gates)
    last = functools.reduce(jnp.maximum, [
        lag_a + pieces + 2, lag_b + pieces + gap + 2, attend + q_heads // 2, place_ctx + 1,
        gates + middle, 3 * n,
    ])

    def passed(pair_sem, sem, peers, wait):
        any_peer = functools.reduce(jnp.logical_or, [ok for _, ok in peers])

        @pl.when(any_peer)
        def _():
            if paired and not wait:
                pl.semaphore_signal(pair_sem, inc=1, device_id={"hd": partner}, device_id_type=mesh_id)
            elif paired:
                pl.semaphore_wait(pair_sem, 1)

        if wait:
            for peer, ok in peers:
                @pl.when(ok)
                def _(peer=peer):
                    pl.semaphore_signal(sem, inc=1, device_id={"ctx": peer}, device_id_type=mesh_id)

    plus_peers = [(p, (p >= 0) & (p < me)) for p in (2 * n - 3 - 2 * me, 2 * n - 4 - 2 * me)]
    minus_peers = [(p, (p > me) & (p < n)) for p in (2 * me - 2, 2 * me - 1)]
    plus_peers = [(p, ok & has_right) for p, ok in plus_peers]
    minus_peers = [(p, ok & has_left) for p, ok in minus_peers]

    def chain_a(t):
        at = t - lag_a

        @pl.when((at == middle) & has_left)
        def _():
            relay_right(me)

        k = jnp.where(at < middle, at, at - 1)

        @pl.when((at >= 0) & (at <= pieces) & (at != middle) & has_left)
        def _():
            step_a(k)

        @pl.when((at == pieces) & has_left)
        def _():
            passed(pair_plus, plus_sem, plus_peers, False)

        @pl.when((at == pieces + 1) & has_left)
        def _():
            passed(pair_plus, plus_sem, plus_peers, True)

    def chain_b(t):
        at = t - lag_b

        @pl.when((at == 0) & has_right)
        def _():
            take_log()

        @pl.when((at == middle + gap) & has_right)
        def _():
            relay_left(hops)

        k = jnp.where(at < middle, at, at - gap - 1)

        @pl.when(((at >= 0) & (at < middle) | (at > middle + gap) & (at <= pieces + gap)) & has_right)
        def _():
            step_b(k)

        @pl.when((at == pieces + gap) & has_right)
        def _():
            passed(pair_minus, minus_sem, minus_peers, False)

        @pl.when((at == pieces + gap + 1) & has_right)
        def _():
            passed(pair_minus, minus_sem, minus_peers, True)

    def slot_step(t, _):
        @pl.when(2 * me >= n)
        def _():
            chain_b(t)

        chain_a(t)

        @pl.when(2 * me < n)
        def _():
            chain_b(t)

        for h in range(1, n - 1):
            @pl.when((t == 2 * h - 2) & (h < me))
            def _(h=h):
                relay_right(h)

            @pl.when((t == 3 * h - 2) & (h < hops))
            def _(h=h):
                relay_left(h)

        @pl.when(t < pieces)
        def _():
            within_blocks(t)

        @pl.when((t >= attend) & (t < attend + q_heads // 2))
        def _():
            one_head(2 * (t - attend))
            one_head(2 * (t - attend) + 1)

        @pl.when((t == gates) & hold_plus)
        def _():
            pl.semaphore_wait(plus_sem, 1)

        @pl.when((t == gates) & hold_minus)
        def _():
            pl.semaphore_wait(minus_sem, 1)

        @pl.when(t == place_ctx)
        def _():
            send_ctx()

        @pl.when((t >= gates) & (t < gates + middle))
        def _():
            for i in range(2):
                gate_a(2 * (t - gates) + i)
                gate_b(2 * (t - gates) + i)
            for i in range(2):
                send_gated(2 * (t - gates) + i)

        return 0

    lax.fori_loop(0, last, slot_step, 0)

    def drain(k, _):
        @pl.when(has_right)
        def _():
            a_copy(k).wait_send()

        @pl.when(has_left)
        def _():
            b_copy(k).wait_send()

        return 0

    lax.fori_loop(0, pieces, drain, 0)

    @pl.when(has_left)
    def _():
        log_copy().wait_send()

    def drain_kv(s, _):
        @pl.when((s <= me) & has_right)
        def _():
            kv_right(s).wait_send()

        @pl.when((s >= me) & has_left)
        def _():
            for copy in kv_left(s):
                copy.wait_send()

        return 0

    lax.fori_loop(0, n, drain_kv, 0)

    def settle(stage, final, cols, send_sem, recv_sem):
        for which in range(2):
            rows = pl.ds(which * half, half)
            copy = remote(stage.at[rows, cols], final.at[rows, cols], send_sem.at[which], recv_sem.at[which], me)

            @pl.when(block_id(which) // 2 != me)
            def _():
                copy.wait_send()

        for slot in range(2):
            source = jnp.where(2 * me + slot < n, 2 * me + slot, 2 * n - 1 - 2 * me - slot)
            rows = pl.ds(slot * half, half)
            copy = remote(stage.at[rows, cols], final.at[rows, cols], send_sem.at[slot], recv_sem.at[slot], me)

            @pl.when(source != me)
            def _():
                copy.wait_recv()

    settle(ctx_stage, ctx_out, slice(None), c_send, c_recv)
    loads[11].wait()
    for k in range(pieces):
        settle(gated, arrived, pl.ds(k * piece, piece), o_send.at[k], o_recv.at[k])


def finish(groups, ctx_ref, gated_ref, gain_ref, ctx_out, mix_out, mixed, sems):
    tok, width = gated_ref.shape
    group_width = width // groups
    half = tok // 2
    copies = [pltpu.make_async_copy(ctx_ref, ctx_out, sems.at[0])]
    copies[0].start()
    for g in range(groups):
        for which in range(2):
            rows, cols = pl.ds(which * half, half), pl.ds(g * group_width, group_width)
            value = gated_ref[rows, cols].astype(F32)
            power = jnp.mean(value * value, axis=-1, keepdims=True)
            mixed[rows, cols] = (value * lax.rsqrt(power + NORM_EPS) * gain_ref[:, cols]).astype(BF16)
            copies.append(
                pltpu.make_async_copy(
                    mixed.at[rows, cols], mix_out.at[rows, cols], sems.at[1 + 2 * g + which]
                )
            )
            copies[-1].start()
    for copy in copies:
        copy.wait()


def body(n, wide_hd, query, keys, values, m_x, m_z, m_b, m_c, dt_raw, dt_bias, a_log, d_skip, norm_gain):
    tok, width = m_x.shape
    half = tok // 2
    heads = dt_raw.shape[1]
    anywhere = pl.BlockSpec(memory_space=INPUT_SPACE)
    groups = m_b.shape[1] // MN
    piece = math.gcd(width // groups, PIECE)
    pieces = width // piece
    kv = keys.shape[1]
    q_heads = query.shape[1] // HEAD_SIZE
    dma = pltpu.SemaphoreType.DMA
    vmem = pltpu.VMEM
    state = (pieces, MN, piece)
    spec = pl.BlockSpec(memory_space=pltpu.VMEM)
    spare = 2 * (query.size + m_x.size) + 4 * width + 49152
    context, gated, gain = pl.pallas_call(
        functools.partial(kernel, n, wide_hd),
        out_shape=(
            vmem(query.shape, BF16),
            vmem(m_x.shape, BF16),
            vmem((1, width), F32),
        ),
        in_specs=[anywhere] * 12,
        out_specs=(spec, spec, spec),
        scratch_shapes=[
            vmem(query.shape, BF16),
            vmem(m_x.shape, BF16),
            vmem(m_x.shape, BF16),
            vmem(m_b.shape, BF16),
            vmem(m_b.shape, BF16),
            vmem((heads, tok), BF16),
            vmem((1, heads), F32),
            vmem((1, heads), F32),
            vmem((1, heads), F32),
            vmem((n, tok, 2 * kv), BF16),
            vmem((tok, n * tok), F32),
            vmem(query.shape, BF16),
            vmem(m_x.shape, BF16),
            vmem((tok, width), F32),
            vmem((tok, width), F32),
            vmem((tok, width), BF16),
            vmem((3 * tok + 16, 3 * heads), BF16),
            vmem((tok, 3 * heads), BF16),
            vmem((groups, tok, piece // MP * (tok // 2)), F32),
            vmem(state, BF16),
            vmem(state, BF16),
            vmem(state, BF16),
            vmem(state, BF16),
            vmem(state, F32),
            vmem(state, F32),
            vmem((pieces, 8, piece), F32),
            vmem((pieces, 8, piece), F32),
            vmem((8, heads), F32),
            vmem((8, heads), F32),
            vmem((8, width), F32),
            dma((n,)),
            dma((n, 2)),
            dma((n, 2)),
            dma((pieces,)),
            dma((pieces,)),
            dma((pieces,)),
            dma((pieces,)),
            dma((pieces, 2)),
            dma((pieces, 2)),
            dma((2,)),
            dma((2,)),
            dma(()),
            dma(()),
            pltpu.SemaphoreType.REGULAR,
            pltpu.SemaphoreType.REGULAR,
            pltpu.SemaphoreType.REGULAR,
            pltpu.SemaphoreType.REGULAR,
            dma((12,)),
        ],
        compiler_params=pltpu.CompilerParams(
            collective_id=0, has_side_effects=True, vmem_limit_bytes=VMEM_BYTES - spare
        ),
    )(
        query, keys, values, m_x, m_z, m_b, m_c, dt_raw.T,
        dt_bias.reshape(1, -1), a_log.reshape(1, -1), d_skip.reshape(1, -1), norm_gain.reshape(1, -1),
    )
    return pl.pallas_call(
        functools.partial(finish, groups),
        out_shape=(
            jax.ShapeDtypeStruct(query.shape, BF16),
            jax.ShapeDtypeStruct(m_x.shape, BF16),
        ),
        in_specs=[spec] * 3,
        out_specs=(anywhere, anywhere),
        scratch_shapes=[vmem(m_x.shape, BF16), dma((1 + 2 * groups,))],
        compiler_params=pltpu.CompilerParams(vmem_limit_bytes=4 << 20),
    )(context, gated, gain)


def solution(mesh):
    rows = P(("grp", "ctx"), "hd")
    in_specs = (rows,) * 8 + (P("hd"),) * 4
    return jax.shard_map(
        functools.partial(body, mesh.shape["ctx"], mesh.shape["hd"]),
        mesh=mesh, in_specs=in_specs, out_specs=(rows, rows), check_vma=False,
    )
```

```python
import functools
import math

import jax
import jax.numpy as jnp
from jax import lax
from jax.experimental import pallas as pl
from jax.experimental.pallas import tpu as pltpu
from jax.sharding import PartitionSpec as P

HEAD_SIZE = 128
MP = 64
MN = 128
NORM_EPS = 1e-05
MASKED = -1e30
HIGHEST = lax.Precision.HIGHEST
F32 = jnp.float32
BF16 = jnp.bfloat16
INPUT_SPACE = pltpu.HBM
PIECE = 128
UNIT = 256
VMEM_BYTES = 67043328


def dot(a, b, ca=1, cb=0, precision=None):
    return lax.dot_general(
        a, b, (((ca,), (cb,)), ((), ())), preferred_element_type=F32, precision=precision
    )


def split(value):
    high = value.astype(BF16)
    rest = value - high.astype(F32)
    mid = rest.astype(BF16)
    return high, mid, (rest - mid.astype(F32)).astype(BF16)


def kernel(
    n, wide_hd, q_in, k_in, v_in, x_in, z_in, b_in, c_in, dt_in, bias_in, alog_in, skip_in,
    gain_in, ctx_out, arrived, gain_ref,
    q_ref, x_ref, z_ref, b_ref, c_ref, dt_ref, bias_ref, alog_ref, skip_ref,
    kv_all, bias_scr, ctx_stage, gated, base_scr, er_scr, xdt_scr, hs, run_split, gmask,
    buf_a, buf_b, out_a, out_b, sloc_a, sloc_b, tot_a, tot_b, log_in, log_out, wide_t,
    kv_plus, kv_minus, kv_recv, a_send, a_recv, b_send, b_recv, o_send, o_recv, c_send, c_recv,
    log_send, log_recv, plus_sem, minus_sem, pair_plus, pair_minus, load_sem,
):
    me = lax.axis_index("ctx")
    tok = q_ref.shape[0]
    half = tok // 2
    heads = dt_ref.shape[0]
    width = x_ref.shape[1]
    groups = b_ref.shape[1] // MN
    group_width = width // groups
    pieces, _, piece = buf_a.shape
    units = o_send.shape[0]
    unit = width // units
    per_unit = unit // MP
    per_group = group_width // unit
    span = unit // piece
    q_heads = q_ref.shape[1] // HEAD_SIZE
    kv = kv_all.shape[2] // 2
    repeat = q_ref.shape[1] // kv
    mesh_id = pl.DeviceIdType.MESH
    core = lax.axis_index("hd")
    paired = wide_hd % 2 == 0
    partner = core + 1 - 2 * lax.rem(core, 2)
    has_left = me > 0
    has_right = me < n - 1

    loads = [
        pltpu.make_async_copy(src, dst, load_sem.at[i])
        for i, (src, dst) in enumerate(
            (
                (dt_in, dt_ref), (bias_in, bias_ref), (alog_in, alog_ref), (skip_in, skip_ref),
                (k_in, kv_all.at[me, :, pl.ds(0, kv)]), (v_in, kv_all.at[me, :, pl.ds(kv, kv)]),
                (b_in, b_ref), (c_in, c_ref), (x_in, x_ref), (z_in, z_ref), (q_in, q_ref),
                (gain_in, gain_ref),
            )
        )
    ]
    barrier = pltpu.get_barrier_semaphore()

    def greet(peer):
        pl.semaphore_signal(barrier, inc=1, device_id={"ctx": peer}, device_id_type=mesh_id)

    @pl.when(has_left)
    def _():
        greet(me - 1)

    @pl.when(has_right)
    def _():
        greet(me + 1)

    if paired:
        pl.semaphore_signal(barrier, inc=1, device_id={"hd": partner}, device_id_type=mesh_id)

    for load in loads:
        load.start()

    def remote(src, dst, send, recv, peer):
        return pltpu.make_async_remote_copy(
            src_ref=src, dst_ref=dst, send_sem=send, recv_sem=recv,
            device_id={"ctx": peer}, device_id_type=mesh_id,
        )

    first = pl.ds(0, half)

    def kv_right(s):
        part = kv_all.at[s, first]
        return remote(part, part, kv_plus.at[s], kv_recv.at[s, 0], jnp.minimum(me + 1, n - 1))

    def kv_left(s):
        copies = []
        for i in range(2):
            part = kv_all.at[s, pl.ds(i * half, half)]
            copies.append(
                remote(part, part, kv_minus.at[s, i], kv_recv.at[s, i], jnp.maximum(me - 1, 0))
            )
        return copies

    def log_copy():
        return remote(log_out, log_in, log_send, log_recv, jnp.maximum(me - 1, 0))

    row = lax.broadcasted_iota(jnp.int32, (tok, tok), 0)
    col = lax.broadcasted_iota(jnp.int32, (tok, tok), 1)
    for load in loads[:4]:
        load.wait()
    raw = dot((row == col).astype(BF16), dt_ref[...], 1, 1) + bias_ref[...]
    steps = jnp.maximum(raw, 0.0) + jnp.log1p(jnp.exp(-jnp.abs(raw)))
    decay = -steps * jnp.exp(alog_ref[...])
    lower = (col <= row) & ((row < half) == (col < half))
    tri = lower.astype(BF16)
    high, mid, low = split(decay)
    run = dot(tri, high) + dot(tri, mid) + dot(tri, low)
    ends = jnp.where(
        lax.broadcasted_iota(jnp.int32, (tok, heads), 0) < half, run[half - 1 : half], run[tok - 1 : tok]
    )

    def keep_split(ref, start, value):
        for i, part in enumerate(split(value)):
            ref[start : start + value.shape[0], i * heads : (i + 1) * heads] = part

    keep_split(run_split, 0, run)
    keep_split(hs, 0, jnp.exp(run))
    keep_split(hs, tok, jnp.exp(ends - run) * steps)
    keep_split(hs, 2 * tok, steps)
    keep_split(hs, 3 * tok, jnp.broadcast_to(skip_ref[...], (16, heads)))
    own_log = jnp.broadcast_to(run[half - 1 : half] + run[tok - 1 : tok], (8, heads))

    for load in loads[4:6]:
        load.wait()

    for load in loads[6:8]:
        load.wait()
    lanes = per_unit * half
    lane = lax.broadcasted_iota(jnp.int32, (half, lanes), 1)
    source = lane - lane // half * half
    target = lax.broadcasted_iota(jnp.int32, (half, lanes), 0)
    causal = source <= target
    diagonal = source == target
    for g in range(groups):
        cols = slice(g * MN, (g + 1) * MN)
        for which in range(2):
            rows = slice(which * half, (which + 1) * half)
            repeated = jnp.concatenate([b_ref[rows, cols]] * per_unit, axis=0)
            gmask[g, rows, :] = jnp.where(causal, dot(c_ref[rows, cols], repeated, 1, 1), 0.0)

    @pl.when(me == 0)
    def _():
        buf_a[...] = jnp.zeros_like(buf_a)

    @pl.when(me == n - 1)
    def _():
        buf_b[...] = jnp.zeros_like(buf_b)
        wide_t[...] = jnp.ones_like(wide_t)

    split_head = lax.rem(lax.broadcasted_iota(jnp.int32, (3 * heads, unit), 0), heads)
    lane_head = lax.broadcasted_iota(jnp.int32, (3 * heads, unit), 1) // MP
    wide_head = lax.rem(lax.broadcasted_iota(jnp.int32, (3 * heads, lanes), 0), heads)
    wide_lane = lax.broadcasted_iota(jnp.int32, (3 * heads, lanes), 1) // half
    part_head = lax.broadcasted_iota(jnp.int32, (half, unit), 1) // MP

    def block_id(which):
        return me if which == 0 else 2 * n - 1 - me

    def send(stage, final, cols, send_sem, recv_sem, which):
        owner = block_id(which) // 2
        slot = lax.rem(block_id(which), 2)
        rows = pl.ds(which * half, half)
        target = pl.ds(pl.multiple_of(slot * half, half), half)

        @pl.when(owner == me)
        def _():
            final[target, cols] = stage[rows, cols]

        @pl.when(owner != me)
        def _():
            remote(
                stage.at[rows, cols], final.at[target, cols], send_sem.at[which], recv_sem.at[slot], owner
            ).start()

    def silu(value):
        return value / (1.0 + jnp.exp(-value))

    def prepare(k):
        cols = pl.ds(pl.multiple_of(k * unit, unit), unit)
        gcols = pl.ds(pl.multiple_of((k // per_group) * MN, MN), MN)
        spread = dot(hs[...], (split_head == k * per_unit + lane_head).astype(BF16))
        xs = x_ref[:, cols].astype(F32)
        weighted = (xs * spread[tok : 2 * tok]).astype(BF16)
        b_rows = b_ref[:, gcols]
        local_a = dot(b_rows[0:half], weighted[0:half], 0, 0)
        local_b = dot(b_rows[half:], weighted[half:], 0, 0)
        for i in range(span):
            part = slice(i * piece, (i + 1) * piece)
            sloc_a[span * k + i] = local_a[:, part]
            sloc_b[span * k + i] = local_b[:, part]
            tot_a[span * k + i] = jnp.broadcast_to(spread[half - 1 : half, part], (8, piece))
            tot_b[span * k + i] = jnp.broadcast_to(spread[tok - 1 : tok, part], (8, piece))
        er_scr[:, cols] = spread[0:tok]
        xdt_scr[:, cols] = (xs * spread[2 * tok : 3 * tok]).astype(BF16)
        base_scr[:, cols] = spread[3 * tok : 3 * tok + 1] * xs

    def within_blocks(k):
        cols = pl.ds(pl.multiple_of(k * unit, unit), unit)
        wide = dot(run_split[...], (wide_head == k * per_unit + wide_lane).astype(BF16))
        for which in range(2):
            rows = slice(which * half, (which + 1) * half)
            mine = wide[rows]
            gap = mine - jnp.sum(jnp.where(diagonal, mine, 0.0), axis=0, keepdims=True)
            weights = (jnp.exp(jnp.minimum(gap, 0.0)) * gmask[k // per_group, rows, :]).astype(BF16)
            part = xdt_scr[rows, cols]
            none = jnp.zeros_like(part)
            stacked = jnp.concatenate(
                [jnp.where(part_head == h, part, none) for h in range(per_unit)], axis=0
            )
            base_scr[rows, cols] = base_scr[rows, cols] + dot(weights, stacked)

    def a_copy(k):
        return remote(out_a.at[k], buf_a.at[k], a_send.at[k], a_recv.at[k], jnp.minimum(me + 1, n - 1))

    def b_copy(k):
        return remote(out_b.at[k], buf_b.at[k], b_send.at[k], b_recv.at[k], jnp.maximum(me - 1, 0))

    def step_a(k):
        @pl.when(has_left)
        def _():
            a_copy(k).wait_recv()

        @pl.when(has_right)
        def _():
            out_a[k] = (buf_a[k].astype(F32) * tot_a[k][0:1] + sloc_a[k]).astype(BF16)
            a_copy(k).start()

    def step_b(k):
        cols = pl.ds(pl.multiple_of(k * piece, piece), piece)

        @pl.when(has_right)
        def _():
            b_copy(k).wait_recv()

        @pl.when(has_left)
        def _():
            mine = sloc_a[k] * wide_t[0:1, cols] + buf_b[k].astype(F32)
            out_b[k] = (mine * tot_b[k][0:1] + sloc_b[k]).astype(BF16)
            b_copy(k).start()

    def gate(k, which, state):
        cols = pl.ds(pl.multiple_of(k * unit, unit), unit)
        gcols = pl.ds(pl.multiple_of((k // per_group) * MN, MN), MN)
        rows = slice(which * half, (which + 1) * half)
        carried = dot(c_ref[rows, gcols], state) * er_scr[rows, cols]
        z = z_ref[rows, cols].astype(F32)
        gated[rows, cols] = ((base_scr[rows, cols] + carried) * silu(z)).astype(BF16)

    def send_gated(k, which):
        cols = pl.ds(pl.multiple_of(k * unit, unit), unit)
        send(gated, arrived, cols, o_send.at[k], o_recv.at[k], which)

    def gate_a(k):
        gate(k, 0, jnp.concatenate([buf_a[span * k + i] for i in range(span)], axis=1))

    def gate_b(k):
        entering = []
        for i in range(span):
            j = span * k + i
            cols = pl.ds(pl.multiple_of(j * piece, piece), piece)
            after = buf_a[j].astype(F32) * tot_a[j][0:1] + sloc_a[j]
            entering.append((after * wide_t[0:1, cols] + buf_b[j].astype(F32)).astype(BF16))
        gate(k, 1, jnp.concatenate(entering, axis=1))

    def take_log():
        @pl.when(has_right)
        def _():
            log_copy().wait_recv()
            later = log_in[...]
            @pl.when(has_left)
            def _():
                log_out[...] = later + own_log
                log_copy().start()

            shape = (heads, width)
            pick = lax.broadcasted_iota(jnp.int32, shape, 0) == lax.broadcasted_iota(jnp.int32, shape, 1) // MP
            high, mid, low = split(jnp.exp(later))
            pick = pick.astype(BF16)
            wide_t[...] = dot(high, pick) + dot(mid, pick) + dot(low, pick)

    def relay_right(h):
        source = jnp.maximum(me - h, 0)

        @pl.when(source != me)
        def _():
            kv_right(source).wait_recv()

        @pl.when(has_right)
        def _():
            kv_right(source).start()

    def relay_left(h):
        source = jnp.minimum(me + h, n - 1)
        for copy in kv_left(source):
            @pl.when(source != me)
            def _(copy=copy):
                copy.wait_recv()

            @pl.when(has_left)
            def _(copy=copy):
                copy.start()

    def attention_mask():
        def clear(s, _):
            @pl.when(s < me)
            def _():
                kv_all[s, half:, :] = jnp.zeros((half, 2 * kv), BF16)

            return 0

        lax.fori_loop(0, n, clear, 0)
        key = lax.broadcasted_iota(jnp.int32, (tok, n * tok), 1)
        source = key // tok
        within = key - source * tok
        key_pos = jnp.where(
            within < half, source * half + within, (2 * n - 2 - source) * half + within
        )
        query = lax.broadcasted_iota(jnp.int32, (tok, n * tok), 0)
        query_pos = jnp.where(query < half, me * half + query, (2 * n - 2 - me) * half + query)
        bias_scr[...] = jnp.where(key_pos <= query_pos, 0.0, MASKED)

    scale = 1.0 / math.sqrt(HEAD_SIZE)

    def one_head(h):
        hcols = pl.ds(pl.multiple_of(h * HEAD_SIZE, HEAD_SIZE), HEAD_SIZE)
        kcols = pl.ds(pl.multiple_of((h // repeat) * HEAD_SIZE, HEAD_SIZE), HEAD_SIZE)
        vcols = pl.ds(pl.multiple_of(kv + (h // repeat) * HEAD_SIZE, HEAD_SIZE), HEAD_SIZE)
        keys = kv_all[:, :, kcols].reshape(n * tok, HEAD_SIZE)
        values = kv_all[:, :, vcols].reshape(n * tok, HEAD_SIZE)
        scores = dot(q_ref[:, hcols], keys, 1, 1) * scale + bias_scr[...]
        expo = jnp.exp(scores - jnp.max(scores, axis=-1, keepdims=True))
        total = jnp.sum(expo, axis=-1, keepdims=True)
        ctx_stage[:, hcols] = (dot(expo.astype(BF16), values) / total).astype(BF16)

    def send_ctx():
        for which in range(2):
            send(ctx_stage, ctx_out, slice(None), c_send, c_recv, which)

    loads[8].wait()
    hops = n - 1 - me
    middle = pieces // 2

    peers = has_left.astype(jnp.int32) + has_right.astype(jnp.int32) + int(paired)

    @pl.when(has_left)
    def _():
        pl.semaphore_wait(barrier, peers)

    @pl.when(jnp.logical_not(has_right))
    def _():
        log_out[...] = own_log
        log_copy().start()

    @pl.when(has_right & has_left)
    def _():
        kv_right(me).start()
        for copy in kv_left(me):
            copy.start()

    prepare(0)

    @pl.when(jnp.logical_not(has_left))
    def _():
        pl.semaphore_wait(barrier, peers)

    def first_step(k, _):
        @pl.when(k > 0)
        def _():
            prepare(k)

        @pl.when((k == units // 2) & (me == 0))
        def _():
            relay_right(0)

        @pl.when((k == units // 2) & (me == n - 1))
        def _():
            relay_left(0)

        for i in range(span):
            @pl.when(me == 0)
            def _(i=i):
                step_a(span * k + i)

            @pl.when(me == n - 1)
            def _(i=i):
                step_b(span * k + i)

        return 0

    lax.fori_loop(0, units, first_step, 0)
    for load in loads[9:11]:
        load.wait()
    attention_mask()

    def base(distance):
        return (14 * jnp.maximum(distance - 1, 0)) // 3

    lag_a = base(me)
    lag_b = base(hops)
    block_b = 2 * n - 1 - me
    hold_plus = block_b // 2 - 1 > me
    hold_minus = me // 2 + 1 < me
    gap = jnp.where(hops > 1, 6, 2)
    free = jnp.maximum(lag_a + pieces + 1, lag_b + pieces + gap + 1)
    gates = jnp.maximum(lag_a, lag_b + gap) + pieces - units + 3
    gates = gates + jnp.where(2 * me < n, jnp.where(has_left, 3, 0), jnp.where(has_right, 7, 1))
    gates = jnp.maximum(gates, jnp.where(hold_plus, lag_a + pieces + 2, 0))
    gates = jnp.maximum(gates, jnp.where(hold_minus, lag_b + pieces + gap + 2, 0))
    quick = gates >= jnp.maximum(lag_a + pieces + 2, lag_b + pieces + gap + 2)
    ending = has_left & jnp.logical_not(has_right)
    first_out = jnp.where((2 * me < n) | jnp.logical_not(has_right), 1, 0)
    early = lag_b + middle + 1
    fills = has_left & has_right & (2 * me >= n) & (lag_a + 2 * span <= early)
    last = functools.reduce(jnp.maximum, [
        lag_a + pieces + 2, lag_b + pieces + gap + 2, gates + jnp.where(quick, middle // 2, middle),
        6 * n - 10, 2 * units,
    ])

    def greet_pair(pair_sem, peers):
        if paired:
            @pl.when(functools.reduce(jnp.logical_or, [ok for _, ok in peers]))
            def _():
                pl.semaphore_signal(pair_sem, inc=1, device_id={"hd": partner}, device_id_type=mesh_id)

    def release(pair_sem, sem, peers):
        if paired:
            @pl.when(functools.reduce(jnp.logical_or, [ok for _, ok in peers]))
            def _():
                pl.semaphore_wait(pair_sem, 1)

        for peer, ok in peers:
            @pl.when(ok)
            def _(peer=peer):
                pl.semaphore_signal(sem, inc=1, device_id={"ctx": peer}, device_id_type=mesh_id)

    plus_peers = [(p, (p >= 0) & (p < me)) for p in (2 * n - 3 - 2 * me, 2 * n - 4 - 2 * me)]
    minus_peers = [(p, (p > me) & (p < n)) for p in (2 * me - 2, 2 * me - 1)]
    plus_peers = [(p, ok & has_right) for p, ok in plus_peers]
    minus_peers = [(p, ok & has_left) for p, ok in minus_peers]

    def chain_a(t):
        at = t - lag_a

        @pl.when((at == middle) & has_left)
        def _():
            relay_right(me)

        k = jnp.where(at < middle, at, at - 2)

        @pl.when(((at >= 0) & (at < middle) | (at > middle + 1) & (at < pieces + 2)) & has_left)
        def _():
            step_a(k)

        @pl.when((at == pieces + 1) & has_left)
        def _():
            greet_pair(pair_plus, plus_peers)

    def chain_b(t):
        at = t - lag_b

        @pl.when((at == 0) & has_right)
        def _():
            take_log()

        @pl.when((at == middle + gap) & has_right)
        def _():
            relay_left(hops)

        k = jnp.where(at < middle, at, at - gap - 2)

        @pl.when(((at >= 0) & (at < middle) | (at > middle + gap + 1) & (at <= pieces + gap + 1)) & has_right)
        def _():
            step_b(k)

        @pl.when((at == pieces + gap + 1) & has_right)
        def _():
            greet_pair(pair_minus, minus_peers)

    def slot_step(t, _):
        @pl.when(2 * me >= n)
        def _():
            chain_b(t)

        chain_a(t)

        @pl.when(2 * me < n)
        def _():
            chain_b(t)

        @pl.when(t == free)
        def _():
            release(pair_minus, minus_sem, minus_peers)
            release(pair_plus, plus_sem, plus_peers)

        for h in range(1, n - 1):
            @pl.when((t == 4 * h - 4) & (h < me))
            def _(h=h):
                relay_right(h)

            @pl.when((t == 6 * h - 4) & (h < hops))
            def _(h=h):
                relay_left(h)

        @pl.when((t < 2 * units) & (lax.rem(t, 2) == 0))
        def _():
            within_blocks(t // 2)

        @pl.when((t == gates) & hold_plus)
        def _():
            pl.semaphore_wait(plus_sem, 1)

        @pl.when((t == gates) & hold_minus)
        def _():
            pl.semaphore_wait(minus_sem, 1)

        @pl.when((t == early) & fills)
        def _():
            for i in range(2):
                gate_a(i)
            for i in range(2):
                send_gated(i, 0)

        @pl.when((t == lag_a + middle - 1) & ending)
        def _():
            def gate_early(i, _):
                for j in range(2):
                    gate_a(2 * i + j)
                    gate_b(2 * i + j)
                for j in range(2):
                    send_gated(2 * i + j, 1)
                return 0

            lax.fori_loop(0, units // 4, gate_early, 0)

        at = jnp.where(quick, 2, 1) * (t - gates)
        on = (at >= jnp.where(ending, units // 4 * 2, 0)) & (at < units) & (lax.rem(at, 2) == 0)
        done_a = fills & (at == 0)

        @pl.when(on & jnp.logical_not(done_a))
        def _():
            for i in range(2):
                gate_a(at + i)
                gate_b(at + i)
            for which in range(2):
                @pl.when(first_out == which)
                def _(which=which):
                    for i in range(2):
                        send_gated(at + i, which)

        @pl.when(on & done_a)
        def _():
            for i in range(2):
                gate_b(at + i)

        return 0

    lax.fori_loop(0, last, slot_step, 0)

    for which in range(2):
        @pl.when(first_out != which)
        def _(which=which):
            def send_rest(k, _):
                send_gated(k, which)
                return 0

            lax.fori_loop(0, units, send_rest, 0)

    def two_heads(i, _):
        one_head(2 * i)
        one_head(2 * i + 1)
        return 0

    lax.fori_loop(0, q_heads // 2, two_heads, 0)
    send_ctx()

    def drain(k, _):
        @pl.when(has_right)
        def _():
            a_copy(k).wait_send()

        @pl.when(has_left)
        def _():
            b_copy(k).wait_send()

        return 0

    lax.fori_loop(0, pieces, drain, 0)

    @pl.when(has_left)
    def _():
        log_copy().wait_send()

    def drain_kv(s, _):
        @pl.when((s <= me) & has_right)
        def _():
            kv_right(s).wait_send()

        @pl.when((s >= me) & has_left)
        def _():
            for copy in kv_left(s):
                copy.wait_send()

        return 0

    lax.fori_loop(0, n, drain_kv, 0)

    def settle(stage, final, cols, send_sem, recv_sem):
        for which in range(2):
            rows = pl.ds(which * half, half)
            copy = remote(stage.at[rows, cols], final.at[rows, cols], send_sem.at[which], recv_sem.at[which], me)

            @pl.when(block_id(which) // 2 != me)
            def _():
                copy.wait_send()

        for slot in range(2):
            source = jnp.where(2 * me + slot < n, 2 * me + slot, 2 * n - 1 - 2 * me - slot)
            rows = pl.ds(slot * half, half)
            copy = remote(stage.at[rows, cols], final.at[rows, cols], send_sem.at[slot], recv_sem.at[slot], me)

            @pl.when(source != me)
            def _():
                copy.wait_recv()

    settle(ctx_stage, ctx_out, slice(None), c_send, c_recv)
    loads[11].wait()
    for k in range(units):
        settle(gated, arrived, pl.ds(k * unit, unit), o_send.at[k], o_recv.at[k])


def finish(groups, ctx_ref, gated_ref, gain_ref, ctx_out, mix_out, mixed, sems):
    tok, width = gated_ref.shape
    group_width = width // groups
    half = tok // 2
    copies = [pltpu.make_async_copy(ctx_ref, ctx_out, sems.at[0])]
    copies[0].start()
    for g in range(groups):
        for which in range(2):
            rows, cols = pl.ds(which * half, half), pl.ds(g * group_width, group_width)
            value = gated_ref[rows, cols].astype(F32)
            power = jnp.mean(value * value, axis=-1, keepdims=True)
            mixed[rows, cols] = (value * lax.rsqrt(power + NORM_EPS) * gain_ref[:, cols]).astype(BF16)
            copies.append(
                pltpu.make_async_copy(
                    mixed.at[rows, cols], mix_out.at[rows, cols], sems.at[1 + 2 * g + which]
                )
            )
            copies[-1].start()
    for copy in copies:
        copy.wait()


def body(n, wide_hd, query, keys, values, m_x, m_z, m_b, m_c, dt_raw, dt_bias, a_log, d_skip, norm_gain):
    tok, width = m_x.shape
    half = tok // 2
    heads = dt_raw.shape[1]
    anywhere = pl.BlockSpec(memory_space=INPUT_SPACE)
    groups = m_b.shape[1] // MN
    piece = math.gcd(width // groups, PIECE)
    pieces = width // piece
    unit = math.gcd(width // groups, UNIT)
    units = width // unit
    kv = keys.shape[1]
    q_heads = query.shape[1] // HEAD_SIZE
    dma = pltpu.SemaphoreType.DMA
    vmem = pltpu.VMEM
    state = (pieces, MN, piece)
    spec = pl.BlockSpec(memory_space=pltpu.VMEM)
    spare = 2 * (query.size + m_x.size) + 4 * width + 49152
    context, gated, gain = pl.pallas_call(
        functools.partial(kernel, n, wide_hd),
        out_shape=(
            vmem(query.shape, BF16),
            vmem(m_x.shape, BF16),
            vmem((1, width), F32),
        ),
        in_specs=[anywhere] * 12,
        out_specs=(spec, spec, spec),
        scratch_shapes=[
            vmem(query.shape, BF16),
            vmem(m_x.shape, BF16),
            vmem(m_x.shape, BF16),
            vmem(m_b.shape, BF16),
            vmem(m_b.shape, BF16),
            vmem((heads, tok), BF16),
            vmem((1, heads), F32),
            vmem((1, heads), F32),
            vmem((1, heads), F32),
            vmem((n, tok, 2 * kv), BF16),
            vmem((tok, n * tok), F32),
            vmem(query.shape, BF16),
            vmem(m_x.shape, BF16),
            vmem((tok, width), F32),
            vmem((tok, width), F32),
            vmem((tok, width), BF16),
            vmem((3 * tok + 16, 3 * heads), BF16),
            vmem((tok, 3 * heads), BF16),
            vmem((groups, tok, unit // MP * (tok // 2)), F32),
            vmem(state, BF16),
            vmem(state, BF16),
            vmem(state, BF16),
            vmem(state, BF16),
            vmem(state, F32),
            vmem(state, F32),
            vmem((pieces, 8, piece), F32),
            vmem((pieces, 8, piece), F32),
            vmem((8, heads), F32),
            vmem((8, heads), F32),
            vmem((8, width), F32),
            dma((n,)),
            dma((n, 2)),
            dma((n, 2)),
            dma((pieces,)),
            dma((pieces,)),
            dma((pieces,)),
            dma((pieces,)),
            dma((units, 2)),
            dma((units, 2)),
            dma((2,)),
            dma((2,)),
            dma(()),
            dma(()),
            pltpu.SemaphoreType.REGULAR,
            pltpu.SemaphoreType.REGULAR,
            pltpu.SemaphoreType.REGULAR,
            pltpu.SemaphoreType.REGULAR,
            dma((12,)),
        ],
        compiler_params=pltpu.CompilerParams(
            collective_id=0, has_side_effects=True, vmem_limit_bytes=VMEM_BYTES - spare
        ),
    )(
        query, keys, values, m_x, m_z, m_b, m_c, dt_raw.T,
        dt_bias.reshape(1, -1), a_log.reshape(1, -1), d_skip.reshape(1, -1), norm_gain.reshape(1, -1),
    )
    return pl.pallas_call(
        functools.partial(finish, groups),
        out_shape=(
            jax.ShapeDtypeStruct(query.shape, BF16),
            jax.ShapeDtypeStruct(m_x.shape, BF16),
        ),
        in_specs=[spec] * 3,
        out_specs=(anywhere, anywhere),
        scratch_shapes=[vmem(m_x.shape, BF16), dma((1 + 2 * groups,))],
        compiler_params=pltpu.CompilerParams(vmem_limit_bytes=4 << 20),
    )(context, gated, gain)


def solution(mesh):
    rows = P(("grp", "ctx"), "hd")
    in_specs = (rows,) * 8 + (P("hd"),) * 4
    return jax.shard_map(
        functools.partial(body, mesh.shape["ctx"], mesh.shape["hd"]),
        mesh=mesh, in_specs=in_specs, out_specs=(rows, rows), check_vma=False,
    )
```

```python
import functools
import math

import jax
import jax.numpy as jnp
from jax import lax
from jax.experimental import pallas as pl
from jax.experimental.pallas import tpu as pltpu
from jax.sharding import PartitionSpec as P

HEAD_SIZE = 128
MP = 64
MN = 128
NORM_EPS = 1e-05
MASKED = -1e30
HIGHEST = lax.Precision.HIGHEST
F32 = jnp.float32
BF16 = jnp.bfloat16
INPUT_SPACE = pltpu.HBM
PIECE = 128
UNIT = 256
VMEM_BYTES = 67043328


def dot(a, b, ca=1, cb=0, precision=None):
    return lax.dot_general(
        a, b, (((ca,), (cb,)), ((), ())), preferred_element_type=F32, precision=precision
    )


def split(value):
    high = value.astype(BF16)
    rest = value - high.astype(F32)
    mid = rest.astype(BF16)
    return high, mid, (rest - mid.astype(F32)).astype(BF16)


def kernel(
    n, wide_hd, q_in, k_in, v_in, x_in, z_in, b_in, c_in, dt_in, bias_in, alog_in, skip_in,
    gain_in, ctx_out, arrived, gain_ref,
    q_ref, x_ref, z_ref, bc_ref, dt_ref, small_ref,
    kv_all, bias_scr, ctx_stage, gated, base_scr, er_scr, xdt_scr, hs, run_split, gmask,
    buf_a, buf_b, out_a, out_b, sloc_a, sloc_b, tot_a, tot_b, log_in, log_out, wide_t,
    kv_plus, kv_minus, kv_recv, a_send, a_recv, b_send, b_recv, o_send, o_recv, c_send, c_recv,
    log_send, log_recv, plus_sem, minus_sem, pair_plus, pair_minus, load_sem,
):
    me = lax.axis_index("ctx")
    tok = q_ref.shape[0]
    half = tok // 2
    heads = dt_ref.shape[0]
    width = x_ref.shape[1]
    groups = bc_ref.shape[2] // MN
    group_width = width // groups
    pieces, _, piece = buf_a.shape
    unit = math.gcd(group_width, UNIT)
    units = width // unit
    per_unit = unit // MP
    per_group = group_width // unit
    span = unit // piece
    q_heads = q_ref.shape[1] // HEAD_SIZE
    kv = kv_all.shape[2] // 2
    repeat = q_ref.shape[1] // kv
    mesh_id = pl.DeviceIdType.MESH
    core = lax.axis_index("hd")
    paired = wide_hd % 2 == 0
    partner = core + 1 - 2 * lax.rem(core, 2)
    has_left = me > 0
    has_right = me < n - 1

    b_ref, c_ref = bc_ref.at[0], bc_ref.at[1]
    bias_ref, alog_ref, skip_ref = (small_ref.at[i] for i in range(3))
    parts = (
        ((dt_in, dt_ref),),
        ((bias_in, bias_ref), (alog_in, alog_ref), (skip_in, skip_ref)),
        ((k_in, kv_all.at[me, :, pl.ds(0, kv)]), (v_in, kv_all.at[me, :, pl.ds(kv, kv)])),
        ((b_in, b_ref), (c_in, c_ref)), ((x_in, x_ref),), ((z_in, z_ref),), ((q_in, q_ref),),
        ((gain_in, gain_ref),),
    )
    wholes = (dt_ref, small_ref, kv_all.at[me], bc_ref, x_ref, z_ref, q_ref, gain_ref)
    loads = [
        pltpu.make_async_copy(whole, whole, load_sem.at[i]) for i, whole in enumerate(wholes)
    ]

    barrier = pltpu.get_barrier_semaphore()

    def greet(peer):
        pl.semaphore_signal(barrier, inc=1, device_id={"ctx": peer}, device_id_type=mesh_id)

    @pl.when(has_left)
    def _():
        greet(me - 1)

    @pl.when(has_right)
    def _():
        greet(me + 1)

    if paired:
        pl.semaphore_signal(barrier, inc=1, device_id={"hd": partner}, device_id_type=mesh_id)

    for i, pairs in enumerate(parts):
        for src, dst in pairs:
            pltpu.make_async_copy(src, dst, load_sem.at[i]).start()

    def remote(src, dst, send, recv, peer):
        return pltpu.make_async_remote_copy(
            src_ref=src, dst_ref=dst, send_sem=send, recv_sem=recv,
            device_id={"ctx": peer}, device_id_type=mesh_id,
        )

    first = pl.ds(0, half)

    def kv_right(s):
        part = kv_all.at[s, first]
        return remote(part, part, kv_plus, kv_recv.at[s, 0], jnp.minimum(me + 1, n - 1))

    def kv_left(s):
        copies = []
        for i in range(2):
            part = kv_all.at[s, pl.ds(i * half, half)]
            copies.append(
                remote(part, part, kv_minus, kv_recv.at[s, i], jnp.maximum(me - 1, 0))
            )
        return copies

    def log_copy():
        return remote(log_out, log_in, log_send, log_recv, jnp.maximum(me - 1, 0))

    row = lax.broadcasted_iota(jnp.int32, (tok, tok), 0)
    col = lax.broadcasted_iota(jnp.int32, (tok, tok), 1)
    for load in loads[:2]:
        load.wait()
    raw = dot((row == col).astype(BF16), dt_ref[...], 1, 1) + bias_ref[...]
    steps = jnp.maximum(raw, 0.0) + jnp.log1p(jnp.exp(-jnp.abs(raw)))
    decay = -steps * jnp.exp(alog_ref[...])
    lower = (col <= row) & ((row < half) == (col < half))
    tri = lower.astype(BF16)
    high, mid, low = split(decay)
    run = dot(tri, high) + dot(tri, mid) + dot(tri, low)
    ends = jnp.where(
        lax.broadcasted_iota(jnp.int32, (tok, heads), 0) < half, run[half - 1 : half], run[tok - 1 : tok]
    )

    def keep_split(ref, start, value):
        for i, part in enumerate(split(value)):
            ref[start : start + value.shape[0], i * heads : (i + 1) * heads] = part

    keep_split(run_split, 0, run)
    keep_split(hs, 0, jnp.exp(run))
    keep_split(hs, tok, jnp.exp(ends - run) * steps)
    keep_split(hs, 2 * tok, steps)
    keep_split(hs, 3 * tok, jnp.broadcast_to(skip_ref[...], (16, heads)))
    own_log = jnp.broadcast_to(run[half - 1 : half] + run[tok - 1 : tok], (8, heads))

    for load in loads[2:4]:
        load.wait()
    lanes = per_unit * half
    lane = lax.broadcasted_iota(jnp.int32, (half, lanes), 1)
    source = lane - lane // half * half
    target = lax.broadcasted_iota(jnp.int32, (half, lanes), 0)
    causal = source <= target
    diagonal = source == target
    for g in range(groups):
        cols = slice(g * MN, (g + 1) * MN)
        for which in range(2):
            rows = slice(which * half, (which + 1) * half)
            repeated = jnp.concatenate([b_ref[rows, cols]] * per_unit, axis=0)
            gmask[g, rows, :] = jnp.where(causal, dot(c_ref[rows, cols], repeated, 1, 1), 0.0)

    @pl.when(me == 0)
    def _():
        buf_a[...] = jnp.zeros_like(buf_a)

    @pl.when(me == n - 1)
    def _():
        buf_b[...] = jnp.zeros_like(buf_b)
        wide_t[...] = jnp.ones_like(wide_t)

    split_head = lax.rem(lax.broadcasted_iota(jnp.int32, (3 * heads, unit), 0), heads)
    lane_head = lax.broadcasted_iota(jnp.int32, (3 * heads, unit), 1) // MP
    wide_head = lax.rem(lax.broadcasted_iota(jnp.int32, (3 * heads, lanes), 0), heads)
    wide_lane = lax.broadcasted_iota(jnp.int32, (3 * heads, lanes), 1) // half
    part_head = lax.broadcasted_iota(jnp.int32, (half, unit), 1) // MP

    def block_id(which):
        return me if which == 0 else 2 * n - 1 - me

    def send(stage, final, cols, send_sem, recv_sem, which):
        owner = block_id(which) // 2
        slot = lax.rem(block_id(which), 2)
        rows = pl.ds(which * half, half)
        target = pl.ds(pl.multiple_of(slot * half, half), half)

        @pl.when(owner == me)
        def _():
            final[target, cols] = stage[rows, cols]

        @pl.when(owner != me)
        def _():
            remote(
                stage.at[rows, cols], final.at[target, cols], send_sem, recv_sem, owner
            ).start()

    def silu(value):
        return value / (1.0 + jnp.exp(-value))

    def prepare(k):
        cols = pl.ds(pl.multiple_of(k * unit, unit), unit)
        gcols = pl.ds(pl.multiple_of((k // per_group) * MN, MN), MN)
        spread = dot(hs[...], (split_head == k * per_unit + lane_head).astype(BF16))
        xs = x_ref[:, cols].astype(F32)
        weighted = (xs * spread[tok : 2 * tok]).astype(BF16)
        b_rows = b_ref[:, gcols]
        local_a = dot(b_rows[0:half], weighted[0:half], 0, 0)
        local_b = dot(b_rows[half:], weighted[half:], 0, 0)
        for i in range(span):
            part = slice(i * piece, (i + 1) * piece)
            sloc_a[span * k + i] = local_a[:, part]
            sloc_b[span * k + i] = local_b[:, part]
            tot_a[span * k + i] = jnp.broadcast_to(spread[half - 1 : half, part], (8, piece))
            tot_b[span * k + i] = jnp.broadcast_to(spread[tok - 1 : tok, part], (8, piece))
        er_scr[:, cols] = spread[0:tok]
        xdt_scr[:, cols] = (xs * spread[2 * tok : 3 * tok]).astype(BF16)
        base_scr[:, cols] = spread[3 * tok : 3 * tok + 1] * xs

    def within_blocks(k):
        cols = pl.ds(pl.multiple_of(k * unit, unit), unit)
        wide = dot(run_split[...], (wide_head == k * per_unit + wide_lane).astype(BF16))
        for which in range(2):
            rows = slice(which * half, (which + 1) * half)
            mine = wide[rows]
            gap = mine - jnp.sum(jnp.where(diagonal, mine, 0.0), axis=0, keepdims=True)
            weights = (jnp.exp(jnp.minimum(gap, 0.0)) * gmask[k // per_group, rows, :]).astype(BF16)
            part = xdt_scr[rows, cols]
            none = jnp.zeros_like(part)
            stacked = jnp.concatenate(
                [jnp.where(part_head == h, part, none) for h in range(per_unit)], axis=0
            )
            base_scr[rows, cols] = base_scr[rows, cols] + dot(weights, stacked)

    def a_copy(k):
        return remote(out_a.at[k], buf_a.at[k], a_send, a_recv.at[k], jnp.minimum(me + 1, n - 1))

    def b_copy(k):
        return remote(out_b.at[k], buf_b.at[k], b_send, b_recv.at[k], jnp.maximum(me - 1, 0))

    def step_a(k):
        @pl.when(has_left)
        def _():
            a_copy(k).wait_recv()

        @pl.when(has_right)
        def _():
            out_a[k] = (buf_a[k].astype(F32) * tot_a[k][0:1] + sloc_a[k]).astype(BF16)
            a_copy(k).start()

    def step_b(k):
        cols = pl.ds(pl.multiple_of(k * piece, piece), piece)

        @pl.when(has_right)
        def _():
            b_copy(k).wait_recv()

        @pl.when(has_left)
        def _():
            mine = sloc_a[k] * wide_t[0:1, cols] + buf_b[k].astype(F32)
            out_b[k] = (mine * tot_b[k][0:1] + sloc_b[k]).astype(BF16)
            b_copy(k).start()

    def gate(k, which, state):
        cols = pl.ds(pl.multiple_of(k * unit, unit), unit)
        gcols = pl.ds(pl.multiple_of((k // per_group) * MN, MN), MN)
        rows = slice(which * half, (which + 1) * half)
        carried = dot(c_ref[rows, gcols], state) * er_scr[rows, cols]
        z = z_ref[rows, cols].astype(F32)
        gated[rows, cols] = ((base_scr[rows, cols] + carried) * silu(z)).astype(BF16)

    def send_gated(k, which):
        cols = pl.ds(pl.multiple_of(k * unit, unit), unit)
        send(gated, arrived, cols, o_send, o_recv, which)

    def gate_a(k):
        gate(k, 0, jnp.concatenate([buf_a[span * k + i] for i in range(span)], axis=1))

    def gate_b(k):
        entering = []
        for i in range(span):
            j = span * k + i
            cols = pl.ds(pl.multiple_of(j * piece, piece), piece)
            after = buf_a[j].astype(F32) * tot_a[j][0:1] + sloc_a[j]
            entering.append((after * wide_t[0:1, cols] + buf_b[j].astype(F32)).astype(BF16))
        gate(k, 1, jnp.concatenate(entering, axis=1))

    def take_log():
        @pl.when(has_right)
        def _():
            log_copy().wait_recv()
            later = log_in[...]
            @pl.when(has_left)
            def _():
                log_out[...] = later + own_log
                log_copy().start()

            shape = (heads, width)
            pick = lax.broadcasted_iota(jnp.int32, shape, 0) == lax.broadcasted_iota(jnp.int32, shape, 1) // MP
            high, mid, low = split(jnp.exp(later))
            pick = pick.astype(BF16)
            wide_t[...] = dot(high, pick) + dot(mid, pick) + dot(low, pick)

    def relay_right(h):
        source = jnp.maximum(me - h, 0)

        @pl.when(source != me)
        def _():
            kv_right(source).wait_recv()

        @pl.when(has_right)
        def _():
            kv_right(source).start()

    def relay_left(h):
        source = jnp.minimum(me + h, n - 1)
        for copy in kv_left(source):
            @pl.when(source != me)
            def _(copy=copy):
                copy.wait_recv()

            @pl.when(has_left)
            def _(copy=copy):
                copy.start()

    def attention_mask():
        def clear(s, _):
            @pl.when(s < me)
            def _():
                kv_all[s, half:, :] = jnp.zeros((half, 2 * kv), BF16)

            return 0

        lax.fori_loop(0, n, clear, 0)
        key = lax.broadcasted_iota(jnp.int32, (tok, n * tok), 1)
        source = key // tok
        within = key - source * tok
        key_pos = jnp.where(
            within < half, source * half + within, (2 * n - 2 - source) * half + within
        )
        query = lax.broadcasted_iota(jnp.int32, (tok, n * tok), 0)
        query_pos = jnp.where(query < half, me * half + query, (2 * n - 2 - me) * half + query)
        bias_scr[...] = jnp.where(key_pos <= query_pos, 0.0, MASKED)

    scale = 1.0 / math.sqrt(HEAD_SIZE)

    def one_head(h):
        hcols = pl.ds(pl.multiple_of(h * HEAD_SIZE, HEAD_SIZE), HEAD_SIZE)
        kcols = pl.ds(pl.multiple_of((h // repeat) * HEAD_SIZE, HEAD_SIZE), HEAD_SIZE)
        vcols = pl.ds(pl.multiple_of(kv + (h // repeat) * HEAD_SIZE, HEAD_SIZE), HEAD_SIZE)
        keys = kv_all[:, :, kcols].reshape(n * tok, HEAD_SIZE)
        values = kv_all[:, :, vcols].reshape(n * tok, HEAD_SIZE)
        scores = dot(q_ref[:, hcols], keys, 1, 1) * scale + bias_scr[...]
        expo = jnp.exp(scores - jnp.max(scores, axis=-1, keepdims=True))
        total = jnp.sum(expo, axis=-1, keepdims=True)
        ctx_stage[:, hcols] = (dot(expo.astype(BF16), values) / total).astype(BF16)

    def send_ctx():
        for which in range(2):
            send(ctx_stage, ctx_out, slice(None), c_send, c_recv, which)

    loads[4].wait()
    hops = n - 1 - me
    middle = pieces // 2

    peers = has_left.astype(jnp.int32) + has_right.astype(jnp.int32) + int(paired)

    @pl.when(has_left)
    def _():
        pl.semaphore_wait(barrier, peers)

    @pl.when(jnp.logical_not(has_right))
    def _():
        log_out[...] = own_log
        log_copy().start()

    @pl.when(has_right & has_left)
    def _():
        kv_right(me).start()
        for copy in kv_left(me):
            copy.start()

    prepare(0)

    @pl.when(jnp.logical_not(has_left))
    def _():
        pl.semaphore_wait(barrier, peers)

    def first_step(k, _):
        @pl.when(k > 0)
        def _():
            prepare(k)

        @pl.when((k == units // 2) & (me == 0))
        def _():
            relay_right(0)

        @pl.when((k == units // 2) & (me == n - 1))
        def _():
            relay_left(0)

        for i in range(span):
            @pl.when(me == 0)
            def _(i=i):
                step_a(span * k + i)

            @pl.when(me == n - 1)
            def _(i=i):
                step_b(span * k + i)

        return 0

    lax.fori_loop(0, units, first_step, 0)
    for load in loads[5:7]:
        load.wait()
    attention_mask()

    def base(distance):
        return (14 * jnp.maximum(distance - 1, 0)) // 3

    lag_a = base(me)
    lag_b = base(hops)
    block_b = 2 * n - 1 - me
    hold_plus = block_b // 2 - 1 > me
    hold_minus = me // 2 + 1 < me
    gap = jnp.where(hops > 1, 6, 2)
    free = jnp.maximum(lag_a + pieces + 1, lag_b + pieces + gap + 1)
    gates = jnp.maximum(lag_a, lag_b + gap) + pieces - units + 3
    gates = gates + jnp.where(2 * me < n, jnp.where(has_left, 3, 0), jnp.where(has_right, 7, 1))
    gates = jnp.maximum(gates, jnp.where(hold_plus, lag_a + pieces + 2, 0))
    gates = jnp.maximum(gates, jnp.where(hold_minus, lag_b + pieces + gap + 2, 0))
    quick = gates >= jnp.maximum(lag_a + pieces + 2, lag_b + pieces + gap + 2)
    ending = has_left & jnp.logical_not(has_right)
    first_out = jnp.where((2 * me < n) | jnp.logical_not(has_right), 1, 0)
    early = lag_b + middle + 1
    fills = has_left & has_right & (2 * me >= n) & (lag_a + 2 * span <= early)
    last = functools.reduce(jnp.maximum, [
        lag_a + pieces + 2, lag_b + pieces + gap + 2, gates + jnp.where(quick, middle // 2, middle),
        6 * n - 10, 2 * units,
    ])

    def greet_pair(pair_sem, peers):
        if paired:
            @pl.when(functools.reduce(jnp.logical_or, [ok for _, ok in peers]))
            def _():
                pl.semaphore_signal(pair_sem, inc=1, device_id={"hd": partner}, device_id_type=mesh_id)

    def release(pair_sem, sem, peers):
        if paired:
            @pl.when(functools.reduce(jnp.logical_or, [ok for _, ok in peers]))
            def _():
                pl.semaphore_wait(pair_sem, 1)

        for peer, ok in peers:
            @pl.when(ok)
            def _(peer=peer):
                pl.semaphore_signal(sem, inc=1, device_id={"ctx": peer}, device_id_type=mesh_id)

    plus_peers = [(p, (p >= 0) & (p < me)) for p in (2 * n - 3 - 2 * me, 2 * n - 4 - 2 * me)]
    minus_peers = [(p, (p > me) & (p < n)) for p in (2 * me - 2, 2 * me - 1)]
    plus_peers = [(p, ok & has_right) for p, ok in plus_peers]
    minus_peers = [(p, ok & has_left) for p, ok in minus_peers]

    def chain_a(t):
        at = t - lag_a

        @pl.when((at == middle) & has_left)
        def _():
            relay_right(me)

        k = jnp.where(at < middle, at, at - 2)

        @pl.when(((at >= 0) & (at < middle) | (at > middle + 1) & (at < pieces + 2)) & has_left)
        def _():
            step_a(k)

        @pl.when((at == pieces + 1) & has_left)
        def _():
            greet_pair(pair_plus, plus_peers)

    def chain_b(t):
        at = t - lag_b

        @pl.when((at == 0) & has_right)
        def _():
            take_log()

        @pl.when((at == middle + gap) & has_right)
        def _():
            relay_left(hops)

        k = jnp.where(at < middle, at, at - gap - 2)

        @pl.when(((at >= 0) & (at < middle) | (at > middle + gap + 1) & (at <= pieces + gap + 1)) & has_right)
        def _():
            step_b(k)

        @pl.when((at == pieces + gap + 1) & has_right)
        def _():
            greet_pair(pair_minus, minus_peers)

    def slot_step(t, _):
        @pl.when(2 * me >= n)
        def _():
            chain_b(t)

        chain_a(t)

        @pl.when(2 * me < n)
        def _():
            chain_b(t)

        @pl.when(t == free)
        def _():
            release(pair_minus, minus_sem, minus_peers)
            release(pair_plus, plus_sem, plus_peers)

        for h in range(1, n - 1):
            @pl.when((t == 4 * h - 4) & (h < me))
            def _(h=h):
                relay_right(h)

            @pl.when((t == 6 * h - 4) & (h < hops))
            def _(h=h):
                relay_left(h)

        @pl.when((t < 2 * units) & (lax.rem(t, 2) == 0))
        def _():
            within_blocks(t // 2)

        @pl.when((t == gates) & hold_plus)
        def _():
            pl.semaphore_wait(plus_sem, 1)

        @pl.when((t == gates) & hold_minus)
        def _():
            pl.semaphore_wait(minus_sem, 1)

        @pl.when((t == early) & fills)
        def _():
            for i in range(2):
                gate_a(i)
            for i in range(2):
                send_gated(i, 0)

        @pl.when((t == lag_a + middle - 1) & ending)
        def _():
            def gate_early(i, _):
                for j in range(2):
                    gate_a(2 * i + j)
                    gate_b(2 * i + j)
                for j in range(2):
                    send_gated(2 * i + j, 1)
                return 0

            lax.fori_loop(0, units // 4, gate_early, 0)

        at = jnp.where(quick, 2, 1) * (t - gates)
        on = (at >= jnp.where(ending, units // 4 * 2, 0)) & (at < units) & (lax.rem(at, 2) == 0)
        done_a = fills & (at == 0)

        @pl.when(on & jnp.logical_not(done_a))
        def _():
            for i in range(2):
                gate_a(at + i)
                gate_b(at + i)
            for which in range(2):
                @pl.when(first_out == which)
                def _(which=which):
                    for i in range(2):
                        send_gated(at + i, which)

        @pl.when(on & done_a)
        def _():
            for i in range(2):
                gate_b(at + i)

        return 0

    lax.fori_loop(0, last, slot_step, 0)

    for which in range(2):
        @pl.when(first_out != which)
        def _(which=which):
            def send_rest(k, _):
                send_gated(k, which)
                return 0

            lax.fori_loop(0, units, send_rest, 0)

    def two_heads(i, _):
        one_head(2 * i)
        one_head(2 * i + 1)
        return 0

    lax.fori_loop(0, q_heads // 2, two_heads, 0)
    send_ctx()

    @pl.when(has_right)
    def _():
        remote(out_a, buf_a, a_send, a_recv.at[0], me).wait_send()

    @pl.when(has_left)
    def _():
        remote(out_b, buf_b, b_send, b_recv.at[0], me).wait_send()

    @pl.when(has_left)
    def _():
        log_copy().wait_send()

    for i in range(n):
        @pl.when((me == i) & has_right)
        def _(i=i):
            part = kv_all.at[pl.ds(0, i + 1), first]
            remote(part, part, kv_plus, kv_recv.at[0, 0], me).wait_send()

        @pl.when((me == i) & has_left)
        def _(i=i):
            part = kv_all.at[pl.ds(i, n - i)]
            remote(part, part, kv_minus, kv_recv.at[0, 0], me).wait_send()

    def settle(stage, final, send_sem, recv_sem):
        def whole(rows):
            return remote(stage.at[pl.ds(0, rows)], final.at[pl.ds(0, rows)], send_sem, recv_sem, me)

        kept = (block_id(0) // 2 == me) | (block_id(1) // 2 == me)
        for rows, here in ((tok, jnp.logical_not(kept)), (half, kept)):
            @pl.when(here)
            def _(rows=rows):
                whole(rows).wait_send()

            @pl.when(here)
            def _(rows=rows):
                whole(rows).wait_recv()

    settle(ctx_stage, ctx_out, c_send, c_recv)
    loads[7].wait()
    settle(gated, arrived, o_send, o_recv)


def finish(groups, ctx_ref, gated_ref, gain_ref, ctx_out, mix_out, mixed, sems):
    tok, width = gated_ref.shape
    group_width = width // groups
    half = tok // 2
    copies = [pltpu.make_async_copy(ctx_ref, ctx_out, sems.at[0])]
    copies[0].start()
    for g in range(groups):
        for which in range(2):
            rows, cols = pl.ds(which * half, half), pl.ds(g * group_width, group_width)
            value = gated_ref[rows, cols].astype(F32)
            power = jnp.mean(value * value, axis=-1, keepdims=True)
            mixed[rows, cols] = (value * lax.rsqrt(power + NORM_EPS) * gain_ref[:, cols]).astype(BF16)
            copies.append(
                pltpu.make_async_copy(
                    mixed.at[rows, cols], mix_out.at[rows, cols], sems.at[1 + 2 * g + which]
                )
            )
            copies[-1].start()
    for copy in copies:
        copy.wait()


def body(n, wide_hd, query, keys, values, m_x, m_z, m_b, m_c, dt_raw, dt_bias, a_log, d_skip, norm_gain):
    tok, width = m_x.shape
    half = tok // 2
    heads = dt_raw.shape[1]
    anywhere = pl.BlockSpec(memory_space=INPUT_SPACE)
    groups = m_b.shape[1] // MN
    piece = math.gcd(width // groups, PIECE)
    pieces = width // piece
    unit = math.gcd(width // groups, UNIT)
    units = width // unit
    kv = keys.shape[1]
    q_heads = query.shape[1] // HEAD_SIZE
    dma = pltpu.SemaphoreType.DMA
    vmem = pltpu.VMEM
    state = (pieces, MN, piece)
    spec = pl.BlockSpec(memory_space=pltpu.VMEM)
    spare = 2 * (query.size + m_x.size) + 4 * width + 49152
    context, gated, gain = pl.pallas_call(
        functools.partial(kernel, n, wide_hd),
        out_shape=(
            vmem(query.shape, BF16),
            vmem(m_x.shape, BF16),
            vmem((1, width), F32),
        ),
        in_specs=[anywhere] * 12,
        out_specs=(spec, spec, spec),
        scratch_shapes=[
            vmem(query.shape, BF16),
            vmem(m_x.shape, BF16),
            vmem(m_x.shape, BF16),
            vmem((2,) + m_b.shape, BF16),
            vmem((heads, tok), BF16),
            vmem((3, 1, heads), F32),
            vmem((n, tok, 2 * kv), BF16),
            vmem((tok, n * tok), F32),
            vmem(query.shape, BF16),
            vmem(m_x.shape, BF16),
            vmem((tok, width), F32),
            vmem((tok, width), F32),
            vmem((tok, width), BF16),
            vmem((3 * tok + 16, 3 * heads), BF16),
            vmem((tok, 3 * heads), BF16),
            vmem((groups, tok, unit // MP * (tok // 2)), F32),
            vmem(state, BF16),
            vmem(state, BF16),
            vmem(state, BF16),
            vmem(state, BF16),
            vmem(state, F32),
            vmem(state, F32),
            vmem((pieces, 8, piece), F32),
            vmem((pieces, 8, piece), F32),
            vmem((8, heads), F32),
            vmem((8, heads), F32),
            vmem((8, width), F32),
            dma(()),
            dma(()),
            dma((n, 2)),
            dma(()),
            dma((pieces,)),
            dma(()),
            dma((pieces,)),
            dma(()),
            dma(()),
            dma(()),
            dma(()),
            dma(()),
            dma(()),
            pltpu.SemaphoreType.REGULAR,
            pltpu.SemaphoreType.REGULAR,
            pltpu.SemaphoreType.REGULAR,
            pltpu.SemaphoreType.REGULAR,
            dma((8,)),
        ],
        compiler_params=pltpu.CompilerParams(
            collective_id=0, has_side_effects=True, vmem_limit_bytes=VMEM_BYTES - spare
        ),
    )(
        query, keys, values, m_x, m_z, m_b, m_c, dt_raw.T,
        dt_bias.reshape(1, -1), a_log.reshape(1, -1), d_skip.reshape(1, -1), norm_gain.reshape(1, -1),
    )
    return pl.pallas_call(
        functools.partial(finish, groups),
        out_shape=(
            jax.ShapeDtypeStruct(query.shape, BF16),
            jax.ShapeDtypeStruct(m_x.shape, BF16),
        ),
        in_specs=[spec] * 3,
        out_specs=(anywhere, anywhere),
        scratch_shapes=[vmem(m_x.shape, BF16), dma((1 + 2 * groups,))],
        compiler_params=pltpu.CompilerParams(vmem_limit_bytes=4 << 20),
    )(context, gated, gain)


def solution(mesh):
    rows = P(("grp", "ctx"), "hd")
    in_specs = (rows,) * 8 + (P("hd"),) * 4
    return jax.shard_map(
        functools.partial(body, mesh.shape["ctx"], mesh.shape["hd"]),
        mesh=mesh, in_specs=in_specs, out_specs=(rows, rows), check_vma=False,
    )
```

```python
import functools
import math

import jax
import jax.numpy as jnp
from jax import lax
from jax.experimental import pallas as pl
from jax.experimental.pallas import tpu as pltpu
from jax.sharding import PartitionSpec as P

HEAD_SIZE = 128
MP = 64
MN = 128
NORM_EPS = 1e-05
MASKED = -1e30
HIGHEST = lax.Precision.HIGHEST
F32 = jnp.float32
BF16 = jnp.bfloat16
INPUT_SPACE = pltpu.HBM
PIECE = 128
UNIT = 256
VMEM_BYTES = 67043328


def dot(a, b, ca=1, cb=0, precision=None):
    return lax.dot_general(
        a, b, (((ca,), (cb,)), ((), ())), preferred_element_type=F32, precision=precision
    )


def split(value):
    high = value.astype(BF16)
    rest = value - high.astype(F32)
    mid = rest.astype(BF16)
    return high, mid, (rest - mid.astype(F32)).astype(BF16)


def kernel(
    n, wide_hd, q_in, k_in, v_in, x_in, z_in, b_in, c_in, dt_in, bias_in, alog_in, skip_in,
    gain_in, ctx_out, arrived, gain_ref,
    q_ref, x_ref, z_ref, bc_ref, dt_ref, small_ref,
    kv_all, bias_scr, ctx_stage, gated, base_scr, er_scr, xdt_scr, hs, run_split, gmask,
    buf_a, buf_b, out_a, out_b, sloc_a, sloc_b, tot_a, tot_b, log_in, log_out, wide_t,
    kv_plus, kv_minus, kv_recv, a_send, a_recv, b_send, b_recv, o_send, o_recv, c_send, c_recv,
    log_send, log_recv, q_more, ctx_more, q_send, q_recv, m_send, plus_sem, minus_sem, pair_plus, pair_minus, load_sem,
):
    me = lax.axis_index("ctx")
    tok = q_ref.shape[0]
    half = tok // 2
    heads = dt_ref.shape[0]
    width = x_ref.shape[1]
    groups = bc_ref.shape[2] // MN
    group_width = width // groups
    pieces, _, piece = buf_a.shape
    unit = math.gcd(group_width, UNIT)
    units = width // unit
    per_unit = unit // MP
    per_group = group_width // unit
    span = unit // piece
    q_heads = q_ref.shape[1] // HEAD_SIZE
    kv = kv_all.shape[2] // 2
    repeat = q_ref.shape[1] // kv
    mesh_id = pl.DeviceIdType.MESH
    core = lax.axis_index("hd")
    paired = wide_hd % 2 == 0
    partner = core + 1 - 2 * lax.rem(core, 2)
    has_left = me > 0
    has_right = me < n - 1
    helped = (me == n - 1) & (n > 1)
    helper = (me == n - 2) & (n > 1)
    kv_right_on = me < n - 2

    b_ref, c_ref = bc_ref.at[0], bc_ref.at[1]
    bias_ref, alog_ref, skip_ref = (small_ref.at[i] for i in range(3))
    parts = (
        ((dt_in, dt_ref),),
        ((bias_in, bias_ref), (alog_in, alog_ref), (skip_in, skip_ref)),
        ((k_in, kv_all.at[me, :, pl.ds(0, kv)]), (v_in, kv_all.at[me, :, pl.ds(kv, kv)])),
        ((b_in, b_ref), (c_in, c_ref)), ((x_in, x_ref),), ((z_in, z_ref),), ((q_in, q_ref),),
        ((gain_in, gain_ref),),
    )
    wholes = (dt_ref, small_ref, kv_all.at[me], bc_ref, x_ref, z_ref, q_ref, gain_ref)
    loads = [
        pltpu.make_async_copy(whole, whole, load_sem.at[i]) for i, whole in enumerate(wholes)
    ]

    barrier = pltpu.get_barrier_semaphore()

    def greet(peer):
        pl.semaphore_signal(barrier, inc=1, device_id={"ctx": peer}, device_id_type=mesh_id)

    @pl.when(has_left)
    def _():
        greet(me - 1)

    @pl.when(has_right)
    def _():
        greet(me + 1)

    if paired:
        pl.semaphore_signal(barrier, inc=1, device_id={"hd": partner}, device_id_type=mesh_id)

    for i, pairs in enumerate(parts):
        for src, dst in pairs:
            pltpu.make_async_copy(src, dst, load_sem.at[i]).start()

    def remote(src, dst, send, recv, peer):
        return pltpu.make_async_remote_copy(
            src_ref=src, dst_ref=dst, send_sem=send, recv_sem=recv,
            device_id={"ctx": peer}, device_id_type=mesh_id,
        )

    first = pl.ds(0, half)

    def kv_right(s):
        part = kv_all.at[s, first]
        return remote(part, part, kv_plus, kv_recv.at[s, 0], jnp.minimum(me + 1, n - 1))

    def kv_left(s):
        copies = []
        for i in range(2):
            part = kv_all.at[s, pl.ds(i * half, half)]
            copies.append(
                remote(part, part, kv_minus, kv_recv.at[s, i], jnp.maximum(me - 1, 0))
            )
        return copies

    def log_copy():
        return remote(log_out, log_in, log_send, log_recv, jnp.maximum(me - 1, 0))

    row = lax.broadcasted_iota(jnp.int32, (tok, tok), 0)
    col = lax.broadcasted_iota(jnp.int32, (tok, tok), 1)
    for load in loads[:2]:
        load.wait()
    raw = dot((row == col).astype(BF16), dt_ref[...], 1, 1) + bias_ref[...]
    steps = jnp.maximum(raw, 0.0) + jnp.log1p(jnp.exp(-jnp.abs(raw)))
    decay = -steps * jnp.exp(alog_ref[...])
    lower = (col <= row) & ((row < half) == (col < half))
    tri = lower.astype(BF16)
    high, mid, low = split(decay)
    run = dot(tri, high) + dot(tri, mid) + dot(tri, low)
    ends = jnp.where(
        lax.broadcasted_iota(jnp.int32, (tok, heads), 0) < half, run[half - 1 : half], run[tok - 1 : tok]
    )

    def keep_split(ref, start, value):
        for i, part in enumerate(split(value)):
            ref[start : start + value.shape[0], i * heads : (i + 1) * heads] = part

    keep_split(run_split, 0, run)
    keep_split(hs, 0, jnp.exp(run))
    keep_split(hs, tok, jnp.exp(ends - run) * steps)
    keep_split(hs, 2 * tok, steps)
    keep_split(hs, 3 * tok, jnp.broadcast_to(skip_ref[...], (16, heads)))
    own_log = jnp.broadcast_to(run[half - 1 : half] + run[tok - 1 : tok], (8, heads))

    for load in loads[2:4]:
        load.wait()
    lanes = per_unit * half
    lane = lax.broadcasted_iota(jnp.int32, (half, lanes), 1)
    source = lane - lane // half * half
    target = lax.broadcasted_iota(jnp.int32, (half, lanes), 0)
    causal = source <= target
    diagonal = source == target

    def causal_products():
        for g in range(groups):
            cols = slice(g * MN, (g + 1) * MN)
            for which in range(2):
                rows = slice(which * half, (which + 1) * half)
                repeated = jnp.concatenate([b_ref[rows, cols]] * per_unit, axis=0)
                gmask[g, rows, :] = jnp.where(causal, dot(c_ref[rows, cols], repeated, 1, 1), 0.0)

    @pl.when(me == 0)
    def _():
        buf_a[...] = jnp.zeros_like(buf_a)

    @pl.when(me == n - 1)
    def _():
        buf_b[...] = jnp.zeros_like(buf_b)
        wide_t[...] = jnp.ones_like(wide_t)

    split_head = lax.rem(lax.broadcasted_iota(jnp.int32, (3 * heads, unit), 0), heads)
    lane_head = lax.broadcasted_iota(jnp.int32, (3 * heads, unit), 1) // MP
    wide_head = lax.rem(lax.broadcasted_iota(jnp.int32, (3 * heads, lanes), 0), heads)
    wide_lane = lax.broadcasted_iota(jnp.int32, (3 * heads, lanes), 1) // half
    part_head = lax.broadcasted_iota(jnp.int32, (half, unit), 1) // MP

    def block_id(which):
        return me if which == 0 else 2 * n - 1 - me

    def send(stage, final, cols, send_sem, recv_sem, which, block=None):
        block = block_id(which) if block is None else block
        owner = block // 2
        slot = lax.rem(block, 2)
        rows = pl.ds(which * half, half)
        target = pl.ds(pl.multiple_of(slot * half, half), half)

        @pl.when(owner == me)
        def _():
            final[target, cols] = stage[rows, cols]

        @pl.when(owner != me)
        def _():
            remote(
                stage.at[rows, cols], final.at[target, cols], send_sem, recv_sem, owner
            ).start()

    def silu(value):
        return value / (1.0 + jnp.exp(-value))

    def prepare(k):
        cols = pl.ds(pl.multiple_of(k * unit, unit), unit)
        gcols = pl.ds(pl.multiple_of((k // per_group) * MN, MN), MN)
        spread = dot(hs[...], (split_head == k * per_unit + lane_head).astype(BF16))
        xs = x_ref[:, cols].astype(F32)
        weighted = (xs * spread[tok : 2 * tok]).astype(BF16)
        b_rows = b_ref[:, gcols]
        local_a = dot(b_rows[0:half], weighted[0:half], 0, 0)
        local_b = dot(b_rows[half:], weighted[half:], 0, 0)
        for i in range(span):
            part = slice(i * piece, (i + 1) * piece)
            sloc_a[span * k + i] = local_a[:, part]
            sloc_b[span * k + i] = local_b[:, part]
            tot_a[span * k + i] = jnp.broadcast_to(spread[half - 1 : half, part], (8, piece))
            tot_b[span * k + i] = jnp.broadcast_to(spread[tok - 1 : tok, part], (8, piece))
        er_scr[:, cols] = spread[0:tok]
        xdt_scr[:, cols] = (xs * spread[2 * tok : 3 * tok]).astype(BF16)
        base_scr[:, cols] = spread[3 * tok : 3 * tok + 1] * xs

    def within_blocks(k):
        cols = pl.ds(pl.multiple_of(k * unit, unit), unit)
        wide = dot(run_split[...], (wide_head == k * per_unit + wide_lane).astype(BF16))
        for which in range(2):
            rows = slice(which * half, (which + 1) * half)
            mine = wide[rows]
            gap = mine - jnp.sum(jnp.where(diagonal, mine, 0.0), axis=0, keepdims=True)
            weights = (jnp.exp(jnp.minimum(gap, 0.0)) * gmask[k // per_group, rows, :]).astype(BF16)
            part = xdt_scr[rows, cols]
            none = jnp.zeros_like(part)
            stacked = jnp.concatenate(
                [jnp.where(part_head == h, part, none) for h in range(per_unit)], axis=0
            )
            base_scr[rows, cols] = base_scr[rows, cols] + dot(weights, stacked)

    def a_copy(k):
        return remote(out_a.at[k], buf_a.at[k], a_send, a_recv.at[k], jnp.minimum(me + 1, n - 1))

    def b_copy(k):
        return remote(out_b.at[k], buf_b.at[k], b_send, b_recv.at[k], jnp.maximum(me - 1, 0))

    def step_a(k):
        @pl.when(has_left)
        def _():
            a_copy(k).wait_recv()

        @pl.when(has_right)
        def _():
            out_a[k] = (buf_a[k].astype(F32) * tot_a[k][0:1] + sloc_a[k]).astype(BF16)
            a_copy(k).start()

    def step_b(k):
        cols = pl.ds(pl.multiple_of(k * piece, piece), piece)

        @pl.when(has_right)
        def _():
            b_copy(k).wait_recv()

        @pl.when(has_left)
        def _():
            mine = sloc_a[k] * wide_t[0:1, cols] + buf_b[k].astype(F32)
            out_b[k] = (mine * tot_b[k][0:1] + sloc_b[k]).astype(BF16)
            b_copy(k).start()

    def gate(k, which, state):
        cols = pl.ds(pl.multiple_of(k * unit, unit), unit)
        gcols = pl.ds(pl.multiple_of((k // per_group) * MN, MN), MN)
        rows = slice(which * half, (which + 1) * half)
        carried = dot(c_ref[rows, gcols], state) * er_scr[rows, cols]
        z = z_ref[rows, cols].astype(F32)
        gated[rows, cols] = ((base_scr[rows, cols] + carried) * silu(z)).astype(BF16)

    def send_gated(k, which):
        cols = pl.ds(pl.multiple_of(k * unit, unit), unit)
        send(gated, arrived, cols, o_send, o_recv, which)

    def gate_a(k):
        gate(k, 0, jnp.concatenate([buf_a[span * k + i] for i in range(span)], axis=1))

    def gate_b(k):
        entering = []
        for i in range(span):
            j = span * k + i
            cols = pl.ds(pl.multiple_of(j * piece, piece), piece)
            after = buf_a[j].astype(F32) * tot_a[j][0:1] + sloc_a[j]
            entering.append((after * wide_t[0:1, cols] + buf_b[j].astype(F32)).astype(BF16))
        gate(k, 1, jnp.concatenate(entering, axis=1))

    def take_log():
        @pl.when(has_right)
        def _():
            log_copy().wait_recv()
            later = log_in[...]
            @pl.when(has_left)
            def _():
                log_out[...] = later + own_log
                log_copy().start()

            shape = (heads, width)
            pick = lax.broadcasted_iota(jnp.int32, shape, 0) == lax.broadcasted_iota(jnp.int32, shape, 1) // MP
            high, mid, low = split(jnp.exp(later))
            pick = pick.astype(BF16)
            wide_t[...] = dot(high, pick) + dot(mid, pick) + dot(low, pick)

    def relay_right(h):
        source = jnp.maximum(me - h, 0)

        @pl.when(source != me)
        def _():
            kv_right(source).wait_recv()

        @pl.when(kv_right_on)
        def _():
            kv_right(source).start()

    def q_copy():
        return remote(q_ref, q_more, q_send, q_recv, jnp.maximum(me - 1, 0))

    def relay_left(h):
        source = jnp.minimum(me + h, n - 1)
        for copy in kv_left(source):
            @pl.when(source != me)
            def _(copy=copy):
                copy.wait_recv()

            @pl.when(has_left)
            def _(copy=copy):
                copy.start()

    def attention_mask(who):
        def clear(s, _):
            @pl.when(s < me)
            def _():
                kv_all[s, half:, :] = jnp.zeros((half, 2 * kv), BF16)

            return 0

        lax.fori_loop(0, n, clear, 0)
        key = lax.broadcasted_iota(jnp.int32, (tok, n * tok), 1)
        source = key // tok
        within = key - source * tok
        key_pos = jnp.where(
            within < half, source * half + within, (2 * n - 2 - source) * half + within
        )
        query = lax.broadcasted_iota(jnp.int32, (tok, n * tok), 0)
        query_pos = jnp.where(query < half, who * half + query, (2 * n - 2 - who) * half + query)
        bias_scr[...] = jnp.where(key_pos <= query_pos, 0.0, MASKED)

    scale = 1.0 / math.sqrt(HEAD_SIZE)

    def one_head(h, queries, stage):
        hcols = pl.ds(pl.multiple_of(h * HEAD_SIZE, HEAD_SIZE), HEAD_SIZE)
        kcols = pl.ds(pl.multiple_of((h // repeat) * HEAD_SIZE, HEAD_SIZE), HEAD_SIZE)
        vcols = pl.ds(pl.multiple_of(kv + (h // repeat) * HEAD_SIZE, HEAD_SIZE), HEAD_SIZE)
        keys = kv_all[:, :, kcols].reshape(n * tok, HEAD_SIZE)
        values = kv_all[:, :, vcols].reshape(n * tok, HEAD_SIZE)
        scores = dot(queries[:, hcols], keys, 1, 1) * scale + bias_scr[...]
        expo = jnp.exp(scores - jnp.max(scores, axis=-1, keepdims=True))
        total = jnp.sum(expo, axis=-1, keepdims=True)
        stage[:, hcols] = (dot(expo.astype(BF16), values) / total).astype(BF16)

    def send_ctx():
        for which in range(2):
            send(ctx_stage, ctx_out, slice(None), c_send, c_recv, which)

    loads[4].wait()
    hops = n - 1 - me
    middle = pieces // 2

    peers = has_left.astype(jnp.int32) + has_right.astype(jnp.int32) + int(paired)

    @pl.when(has_left)
    def _():
        pl.semaphore_wait(barrier, peers)

    @pl.when(jnp.logical_not(has_right))
    def _():
        log_out[...] = own_log
        log_copy().start()

    @pl.when(has_right & has_left)
    def _():
        for copy in kv_left(me):
            copy.start()

    @pl.when(kv_right_on & has_left)
    def _():
        kv_right(me).start()

    prepare(0)

    @pl.when(jnp.logical_not(has_left))
    def _():
        pl.semaphore_wait(barrier, peers)

    def first_step(k, _):
        @pl.when(k > 0)
        def _():
            prepare(k)

        @pl.when((k == units // 2) & (me == n - 1))
        def _():
            relay_left(0)

        for i in range(span):
            @pl.when(me == 0)
            def _(i=i):
                step_a(span * k + i)

            @pl.when(me == n - 1)
            def _(i=i):
                step_b(span * k + i)

        return 0

    between = has_left & has_right
    lax.fori_loop(0, jnp.where(between, units - 2, units), first_step, 0)
    for load in loads[5:7]:
        load.wait()

    @pl.when((me == 0) & kv_right_on)
    def _():
        relay_right(0)

    @pl.when(helped)
    def _():
        q_copy().start()

    def base(distance):
        return (14 * jnp.maximum(distance - 1, 0)) // 3

    lag_a = base(me)
    lag_b = base(hops)
    block_b = 2 * n - 1 - me
    hold_plus = block_b // 2 - 1 > me
    hold_minus = me // 2 + 1 < me
    gap = jnp.where(hops > 1, 6, 2)
    free = jnp.maximum(lag_a + pieces - 1, lag_b + pieces + gap + 1)
    gates = jnp.maximum(lag_a - 2, lag_b + gap) + pieces - units + 3
    gates = gates + jnp.where(2 * me < n, jnp.where(has_left, 3, 0), jnp.where(has_right, 7, 1))
    gates = jnp.maximum(gates, jnp.where(hold_plus, lag_a + pieces + 2, 0))
    gates = jnp.maximum(gates, jnp.where(hold_minus, lag_b + pieces + gap + 2, 0))
    quick = gates >= jnp.maximum(lag_a + pieces + 2, lag_b + pieces + gap + 2)
    ending = has_left & jnp.logical_not(has_right)
    first_out = jnp.where((2 * me < n) | jnp.logical_not(has_right), 1, 0)
    early = lag_b + middle + 1
    fills = has_left & has_right & (2 * me >= n) & (lag_a + 2 * span <= early)
    last = functools.reduce(jnp.maximum, [
        lag_a + pieces + 2, lag_b + pieces + gap + 2, gates + jnp.where(quick, middle // 2, middle),
        6 * n - 10, 2 * units,
    ])

    def greet_pair(pair_sem, peers):
        if paired:
            @pl.when(functools.reduce(jnp.logical_or, [ok for _, ok in peers]))
            def _():
                pl.semaphore_signal(pair_sem, inc=1, device_id={"hd": partner}, device_id_type=mesh_id)

    def release(pair_sem, sem, peers):
        if paired:
            @pl.when(functools.reduce(jnp.logical_or, [ok for _, ok in peers]))
            def _():
                pl.semaphore_wait(pair_sem, 1)

        for peer, ok in peers:
            @pl.when(ok)
            def _(peer=peer):
                pl.semaphore_signal(sem, inc=1, device_id={"ctx": peer}, device_id_type=mesh_id)

    plus_peers = [(p, (p >= 0) & (p < me)) for p in (2 * n - 3 - 2 * me, 2 * n - 4 - 2 * me)]
    minus_peers = [(p, (p > me) & (p < n)) for p in (2 * me - 2, 2 * me - 1)]
    plus_peers = [(p, ok & has_right) for p, ok in plus_peers]
    minus_peers = [(p, ok & has_left) for p, ok in minus_peers]

    def chain_a(t):
        at = t - lag_a

        @pl.when((at >= 0) & (at < pieces) & has_left)
        def _():
            step_a(at)

        @pl.when((at == pieces + 1) & has_left & kv_right_on)
        def _():
            relay_right(me)

        @pl.when((at == pieces - 1) & has_left)
        def _():
            greet_pair(pair_plus, plus_peers)

    def chain_b(t):
        at = t - lag_b

        @pl.when((at == 0) & has_right)
        def _():
            take_log()

        @pl.when((at == middle + gap) & has_right)
        def _():
            relay_left(hops)

        k = jnp.where(at < middle, at, at - gap - 2)

        @pl.when(((at >= 0) & (at < middle) | (at > middle + gap + 1) & (at <= pieces + gap + 1)) & has_right)
        def _():
            step_b(k)

        @pl.when((at == pieces + gap + 1) & has_right)
        def _():
            greet_pair(pair_minus, minus_peers)

    def slot_step(t, _):
        @pl.when(2 * me >= n)
        def _():
            chain_b(t)

        chain_a(t)

        @pl.when(2 * me < n)
        def _():
            chain_b(t)

        @pl.when(t == free)
        def _():
            release(pair_minus, minus_sem, minus_peers)
            release(pair_plus, plus_sem, plus_peers)

        for h in range(1, n - 1):
            @pl.when((t == 4 * h - 4) & (h < me) & jnp.logical_not(helped))
            def _(h=h):
                relay_right(h)

            @pl.when((t == 6 * h - 4) & (h < hops))
            def _(h=h):
                relay_left(h)

        @pl.when(t == 0)
        def _():
            causal_products()

        @pl.when(between & ((t == 1) | (t == 3)))
        def _():
            prepare(units - 2 + t // 2)

        @pl.when((t < 2 * units) & (lax.rem(t, 2) == 0))
        def _():
            within_blocks(t // 2)

        @pl.when((t == gates) & hold_plus)
        def _():
            pl.semaphore_wait(plus_sem, 1)

        @pl.when((t == gates) & hold_minus)
        def _():
            pl.semaphore_wait(minus_sem, 1)

        @pl.when((t == early) & fills)
        def _():
            for i in range(2):
                gate_a(i)
            for i in range(2):
                send_gated(i, 0)

        @pl.when((t == lag_a + middle - 1) & ending)
        def _():
            def gate_early(i, _):
                for j in range(2):
                    gate_a(2 * i + j)
                    gate_b(2 * i + j)
                for j in range(2):
                    send_gated(2 * i + j, 1)
                return 0

            lax.fori_loop(0, units // 4, gate_early, 0)

        at = jnp.where(quick, 2, 1) * (t - gates)
        on = (at >= jnp.where(ending, units // 4 * 2, 0)) & (at < units) & (lax.rem(at, 2) == 0)
        done_a = fills & (at == 0)

        @pl.when(on & jnp.logical_not(done_a))
        def _():
            for i in range(2):
                gate_a(at + i)
                gate_b(at + i)
            for which in range(2):
                @pl.when(first_out == which)
                def _(which=which):
                    for i in range(2):
                        send_gated(at + i, which)

        @pl.when(on & done_a)
        def _():
            for i in range(2):
                gate_b(at + i)

        return 0

    lax.fori_loop(0, last, slot_step, 0)

    for which in range(2):
        @pl.when(first_out != which)
        def _(which=which):
            def send_rest(k, _):
                send_gated(k, which)
                return 0

            lax.fori_loop(0, units, send_rest, 0)

    def attend(who, queries, stage):
        attention_mask(who)

        def two_heads(i, _):
            one_head(2 * i, queries, stage)
            one_head(2 * i + 1, queries, stage)
            return 0

        lax.fori_loop(0, q_heads // 2, two_heads, 0)

    @pl.when(helper & has_left)
    def _():
        kv_right(0).wait_recv()

    @pl.when(jnp.logical_not(helped))
    def _():
        attend(me, q_ref, ctx_stage)
        send_ctx()

    @pl.when(helper)
    def _():
        q_copy().wait_recv()
        attend(n - 1, q_more, ctx_more)
        for which in range(2):
            send(ctx_more, ctx_out, slice(None), m_send, c_recv, which, jnp.int32(n - 1 + which))

    @pl.when(has_right)
    def _():
        remote(out_a, buf_a, a_send, a_recv.at[0], me).wait_send()

    @pl.when(has_left)
    def _():
        remote(out_b, buf_b, b_send, b_recv.at[0], me).wait_send()

    @pl.when(has_left)
    def _():
        log_copy().wait_send()

    for i in range(n):
        @pl.when((me == i) & kv_right_on)
        def _(i=i):
            part = kv_all.at[pl.ds(0, i + 1), first]
            remote(part, part, kv_plus, kv_recv.at[0, 0], me).wait_send()

        @pl.when((me == i) & has_left)
        def _(i=i):
            part = kv_all.at[pl.ds(i, n - i)]
            remote(part, part, kv_minus, kv_recv.at[0, 0], me).wait_send()

    def settle(stage, final, send_sem, recv_sem, away, missing):
        for count in (1, 2):
            rows = pl.ds(0, count * half)
            copy = remote(stage.at[rows], final.at[rows], send_sem, recv_sem, me)

            @pl.when(away == count)
            def _(copy=copy):
                copy.wait_send()

            @pl.when(missing == count)
            def _(copy=copy):
                copy.wait_recv()

    def tally(flags):
        return sum(jnp.where(flag, 1, 0) for flag in flags)

    def source_of(slot):
        block = 2 * me + slot
        return jnp.where(block < n, block, 2 * n - 1 - block)

    away = tally(block_id(which) // 2 != me for which in range(2))
    missing = tally(source_of(slot) != me for slot in range(2))
    served = [jnp.minimum(source_of(slot), n - 2) if n > 1 else source_of(slot) for slot in range(2)]
    served_missing = tally(source != me for source in served)
    more = sum(1 for block in (n - 1, n) if block // 2 != n - 2)

    @pl.when(helped)
    def _():
        q_copy().wait_send()

    settle(ctx_stage, ctx_out, c_send, c_recv, jnp.where(helped, 0, away), served_missing)
    settle(ctx_more, ctx_out, m_send, c_recv, jnp.where(helper, more, 0), 0)
    loads[7].wait()
    settle(gated, arrived, o_send, o_recv, away, missing)


def finish(groups, ctx_ref, gated_ref, gain_ref, ctx_out, mix_out, mixed, sems):
    tok, width = gated_ref.shape
    group_width = width // groups
    half = tok // 2
    copies = [pltpu.make_async_copy(ctx_ref, ctx_out, sems.at[0])]
    copies[0].start()
    for g in range(groups):
        for which in range(2):
            rows, cols = pl.ds(which * half, half), pl.ds(g * group_width, group_width)
            value = gated_ref[rows, cols].astype(F32)
            power = jnp.mean(value * value, axis=-1, keepdims=True)
            mixed[rows, cols] = (value * lax.rsqrt(power + NORM_EPS) * gain_ref[:, cols]).astype(BF16)
            copies.append(
                pltpu.make_async_copy(
                    mixed.at[rows, cols], mix_out.at[rows, cols], sems.at[1 + 2 * g + which]
                )
            )
            copies[-1].start()
    for copy in copies:
        copy.wait()


def body(n, wide_hd, query, keys, values, m_x, m_z, m_b, m_c, dt_raw, dt_bias, a_log, d_skip, norm_gain):
    tok, width = m_x.shape
    half = tok // 2
    heads = dt_raw.shape[1]
    anywhere = pl.BlockSpec(memory_space=INPUT_SPACE)
    groups = m_b.shape[1] // MN
    piece = math.gcd(width // groups, PIECE)
    pieces = width // piece
    unit = math.gcd(width // groups, UNIT)
    units = width // unit
    kv = keys.shape[1]
    q_heads = query.shape[1] // HEAD_SIZE
    dma = pltpu.SemaphoreType.DMA
    vmem = pltpu.VMEM
    state = (pieces, MN, piece)
    spec = pl.BlockSpec(memory_space=pltpu.VMEM)
    spare = 2 * (query.size + m_x.size) + 4 * width + 49152
    context, gated, gain = pl.pallas_call(
        functools.partial(kernel, n, wide_hd),
        out_shape=(
            vmem(query.shape, BF16),
            vmem(m_x.shape, BF16),
            vmem((1, width), F32),
        ),
        in_specs=[anywhere] * 12,
        out_specs=(spec, spec, spec),
        scratch_shapes=[
            vmem(query.shape, BF16),
            vmem(m_x.shape, BF16),
            vmem(m_x.shape, BF16),
            vmem((2,) + m_b.shape, BF16),
            vmem((heads, tok), BF16),
            vmem((3, 1, heads), F32),
            vmem((n, tok, 2 * kv), BF16),
            vmem((tok, n * tok), F32),
            vmem(query.shape, BF16),
            vmem(m_x.shape, BF16),
            vmem((tok, width), F32),
            vmem((tok, width), F32),
            vmem((tok, width), BF16),
            vmem((3 * tok + 16, 3 * heads), BF16),
            vmem((tok, 3 * heads), BF16),
            vmem((groups, tok, unit // MP * (tok // 2)), F32),
            vmem(state, BF16),
            vmem(state, BF16),
            vmem(state, BF16),
            vmem(state, BF16),
            vmem(state, F32),
            vmem(state, F32),
            vmem((pieces, 8, piece), F32),
            vmem((pieces, 8, piece), F32),
            vmem((8, heads), F32),
            vmem((8, heads), F32),
            vmem((8, width), F32),
            dma(()),
            dma(()),
            dma((n, 2)),
            dma(()),
            dma((pieces,)),
            dma(()),
            dma((pieces,)),
            dma(()),
            dma(()),
            dma(()),
            dma(()),
            dma(()),
            dma(()),
            vmem(query.shape, BF16),
            vmem(query.shape, BF16),
            dma(()),
            dma(()),
            dma(()),
            pltpu.SemaphoreType.REGULAR,
            pltpu.SemaphoreType.REGULAR,
            pltpu.SemaphoreType.REGULAR,
            pltpu.SemaphoreType.REGULAR,
            dma((8,)),
        ],
        compiler_params=pltpu.CompilerParams(
            collective_id=0, has_side_effects=True, vmem_limit_bytes=VMEM_BYTES - spare
        ),
    )(
        query, keys, values, m_x, m_z, m_b, m_c, dt_raw.T,
        dt_bias.reshape(1, -1), a_log.reshape(1, -1), d_skip.reshape(1, -1), norm_gain.reshape(1, -1),
    )
    return pl.pallas_call(
        functools.partial(finish, groups),
        out_shape=(
            jax.ShapeDtypeStruct(query.shape, BF16),
            jax.ShapeDtypeStruct(m_x.shape, BF16),
        ),
        in_specs=[spec] * 3,
        out_specs=(anywhere, anywhere),
        scratch_shapes=[vmem(m_x.shape, BF16), dma((1 + 2 * groups,))],
        compiler_params=pltpu.CompilerParams(vmem_limit_bytes=4 << 20),
    )(context, gated, gain)


def solution(mesh):
    rows = P(("grp", "ctx"), "hd")
    in_specs = (rows,) * 8 + (P("hd"),) * 4
    return jax.shard_map(
        functools.partial(body, mesh.shape["ctx"], mesh.shape["hd"]),
        mesh=mesh, in_specs=in_specs, out_specs=(rows, rows), check_vma=False,
    )
```

```python
import functools
import math

import jax
import jax.numpy as jnp
from jax import lax
from jax.experimental import pallas as pl
from jax.experimental.pallas import tpu as pltpu
from jax.sharding import PartitionSpec as P

HEAD_SIZE = 128
MP = 64
MN = 128
NORM_EPS = 1e-05
MASKED = -1e30
HIGHEST = lax.Precision.HIGHEST
F32 = jnp.float32
BF16 = jnp.bfloat16
INPUT_SPACE = pltpu.HBM
PIECE = 128
UNIT = 256
VMEM_BYTES = 67043328


def dot(a, b, ca=1, cb=0, precision=None):
    return lax.dot_general(
        a, b, (((ca,), (cb,)), ((), ())), preferred_element_type=F32, precision=precision
    )


def split(value):
    high = value.astype(BF16)
    rest = value - high.astype(F32)
    mid = rest.astype(BF16)
    return high, mid, (rest - mid.astype(F32)).astype(BF16)


def kernel(
    n, wide_hd, q_in, k_in, v_in, x_in, z_in, b_in, c_in, dt_in, bias_in, alog_in, skip_in,
    gain_in, ctx_out, arrived, gain_ref,
    q_ref, x_ref, z_ref, bc_ref, dt_ref, small_ref,
    kv_all, bias_scr, ctx_stage, gated, base_scr, er_scr, xdt_scr, hs, run_split, gmask,
    buf_a, buf_b, out_a, out_b, sloc_a, sloc_b, tot_a, tot_b, log_in, log_out, wide_t,
    kv_plus, kv_minus, kv_recv, a_send, a_recv, b_send, b_recv, o_send, o_recv, c_send, c_recv,
    log_send, log_recv, q_more, ctx_more, q_send, q_recv, m_send, plus_sem, minus_sem, pair_plus, pair_minus, load_sem,
):
    me = lax.axis_index("ctx")
    tok = q_ref.shape[0]
    half = tok // 2
    heads = dt_ref.shape[0]
    width = x_ref.shape[1]
    groups = bc_ref.shape[2] // MN
    group_width = width // groups
    pieces, _, piece = buf_a.shape
    unit = math.gcd(group_width, UNIT)
    units = width // unit
    per_unit = unit // MP
    per_group = group_width // unit
    span = unit // piece
    q_heads = q_ref.shape[1] // HEAD_SIZE
    kv = kv_all.shape[2] // 2
    repeat = q_ref.shape[1] // kv
    mesh_id = pl.DeviceIdType.MESH
    core = lax.axis_index("hd")
    paired = wide_hd % 2 == 0
    partner = core + 1 - 2 * lax.rem(core, 2)
    has_left = me > 0
    has_right = me < n - 1
    helped = (me == n - 1) & (n > 1)
    helper = (me == n - 2) & (n > 1)
    kv_right_on = me < n - 2

    b_ref, c_ref = bc_ref.at[0], bc_ref.at[1]
    bias_ref, alog_ref, skip_ref = (small_ref.at[i] for i in range(3))
    parts = (
        ((dt_in, dt_ref),),
        ((bias_in, bias_ref), (alog_in, alog_ref), (skip_in, skip_ref)),
        ((k_in, kv_all.at[me, :, pl.ds(0, kv)]), (v_in, kv_all.at[me, :, pl.ds(kv, kv)])),
        ((b_in, b_ref), (c_in, c_ref)), ((x_in, x_ref),), ((z_in, z_ref),), ((q_in, q_ref),),
        ((gain_in, gain_ref),),
    )
    wholes = (dt_ref, small_ref, kv_all.at[me], bc_ref, x_ref, z_ref, q_ref, gain_ref)
    loads = [
        pltpu.make_async_copy(whole, whole, load_sem.at[i]) for i, whole in enumerate(wholes)
    ]

    barrier = pltpu.get_barrier_semaphore()

    def greet(peer):
        pl.semaphore_signal(barrier, inc=1, device_id={"ctx": peer}, device_id_type=mesh_id)

    @pl.when(has_left)
    def _():
        greet(me - 1)

    @pl.when(has_right)
    def _():
        greet(me + 1)

    if paired:
        pl.semaphore_signal(barrier, inc=1, device_id={"hd": partner}, device_id_type=mesh_id)

    for i, pairs in enumerate(parts):
        for src, dst in pairs:
            pltpu.make_async_copy(src, dst, load_sem.at[i]).start()

    def remote(src, dst, send, recv, peer):
        return pltpu.make_async_remote_copy(
            src_ref=src, dst_ref=dst, send_sem=send, recv_sem=recv,
            device_id={"ctx": peer}, device_id_type=mesh_id,
        )

    first = pl.ds(0, half)

    def kv_right(s):
        part = kv_all.at[s, first]
        return remote(part, part, kv_plus, kv_recv.at[s, 0], jnp.minimum(me + 1, n - 1))

    def kv_left(s):
        copies = []
        for i in range(2):
            part = kv_all.at[s, pl.ds(i * half, half)]
            copies.append(
                remote(part, part, kv_minus, kv_recv.at[s, i], jnp.maximum(me - 1, 0))
            )
        return copies

    def log_copy():
        return remote(log_out, log_in, log_send, log_recv, jnp.maximum(me - 1, 0))

    row = lax.broadcasted_iota(jnp.int32, (tok, tok), 0)
    col = lax.broadcasted_iota(jnp.int32, (tok, tok), 1)
    for load in loads[:2]:
        load.wait()
    raw = dot((row == col).astype(BF16), dt_ref[...], 1, 1) + bias_ref[...]
    steps = jnp.maximum(raw, 0.0) + jnp.log1p(jnp.exp(-jnp.abs(raw)))
    decay = -steps * jnp.exp(alog_ref[...])
    lower = (col <= row) & ((row < half) == (col < half))
    tri = lower.astype(BF16)
    high, mid, low = split(decay)
    run = dot(tri, high) + dot(tri, mid) + dot(tri, low)
    ends = jnp.where(
        lax.broadcasted_iota(jnp.int32, (tok, heads), 0) < half, run[half - 1 : half], run[tok - 1 : tok]
    )

    def keep_split(ref, start, value):
        for i, part in enumerate(split(value)):
            ref[start : start + value.shape[0], i * heads : (i + 1) * heads] = part

    keep_split(run_split, 0, run)
    keep_split(hs, 0, jnp.exp(run))
    keep_split(hs, tok, jnp.exp(ends - run) * steps)
    keep_split(hs, 2 * tok, steps)
    keep_split(hs, 3 * tok, jnp.broadcast_to(skip_ref[...], (16, heads)))
    own_log = jnp.broadcast_to(run[half - 1 : half] + run[tok - 1 : tok], (8, heads))

    for load in loads[2:4]:
        load.wait()
    lanes = per_unit * half
    lane = lax.broadcasted_iota(jnp.int32, (half, lanes), 1)
    source = lane - lane // half * half
    target = lax.broadcasted_iota(jnp.int32, (half, lanes), 0)
    causal = source <= target
    diagonal = source == target

    def causal_products():
        for g in range(groups):
            cols = slice(g * MN, (g + 1) * MN)
            for which in range(2):
                rows = slice(which * half, (which + 1) * half)
                repeated = jnp.concatenate([b_ref[rows, cols]] * per_unit, axis=0)
                gmask[g, rows, :] = jnp.where(causal, dot(c_ref[rows, cols], repeated, 1, 1), 0.0)

    @pl.when(me == 0)
    def _():
        buf_a[...] = jnp.zeros_like(buf_a)

    @pl.when(me == n - 1)
    def _():
        buf_b[...] = jnp.zeros_like(buf_b)
        wide_t[...] = jnp.ones_like(wide_t)

    split_head = lax.rem(lax.broadcasted_iota(jnp.int32, (3 * heads, unit), 0), heads)
    lane_head = lax.broadcasted_iota(jnp.int32, (3 * heads, unit), 1) // MP
    wide_head = lax.rem(lax.broadcasted_iota(jnp.int32, (3 * heads, lanes), 0), heads)
    wide_lane = lax.broadcasted_iota(jnp.int32, (3 * heads, lanes), 1) // half
    part_head = lax.broadcasted_iota(jnp.int32, (half, unit), 1) // MP

    def block_id(which):
        return me if which == 0 else 2 * n - 1 - me

    def send(stage, final, cols, send_sem, recv_sem, which, block=None):
        block = block_id(which) if block is None else block
        owner = block // 2
        slot = lax.rem(block, 2)
        rows = pl.ds(which * half, half)
        target = pl.ds(pl.multiple_of(slot * half, half), half)

        @pl.when(owner == me)
        def _():
            final[target, cols] = stage[rows, cols]

        @pl.when(owner != me)
        def _():
            remote(
                stage.at[rows, cols], final.at[target, cols], send_sem, recv_sem, owner
            ).start()

    def silu(value):
        return value / (1.0 + jnp.exp(-value))

    def prepare(k):
        cols = pl.ds(pl.multiple_of(k * unit, unit), unit)
        gcols = pl.ds(pl.multiple_of((k // per_group) * MN, MN), MN)
        spread = dot(hs[...], (split_head == k * per_unit + lane_head).astype(BF16))
        xs = x_ref[:, cols].astype(F32)
        weighted = (xs * spread[tok : 2 * tok]).astype(BF16)
        b_rows = b_ref[:, gcols]
        local_a = dot(b_rows[0:half], weighted[0:half], 0, 0)
        local_b = dot(b_rows[half:], weighted[half:], 0, 0)
        for i in range(span):
            part = slice(i * piece, (i + 1) * piece)
            sloc_a[span * k + i] = local_a[:, part]
            sloc_b[span * k + i] = local_b[:, part]
            tot_a[span * k + i] = jnp.broadcast_to(spread[half - 1 : half, part], (8, piece))
            tot_b[span * k + i] = jnp.broadcast_to(spread[tok - 1 : tok, part], (8, piece))
        er_scr[:, cols] = spread[0:tok]
        xdt_scr[:, cols] = (xs * spread[2 * tok : 3 * tok]).astype(BF16)
        base_scr[:, cols] = spread[3 * tok : 3 * tok + 1] * xs

    def within_blocks(k):
        cols = pl.ds(pl.multiple_of(k * unit, unit), unit)
        wide = dot(run_split[...], (wide_head == k * per_unit + wide_lane).astype(BF16))
        for which in range(2):
            rows = slice(which * half, (which + 1) * half)
            mine = wide[rows]
            gap = mine - jnp.sum(jnp.where(diagonal, mine, 0.0), axis=0, keepdims=True)
            weights = (jnp.exp(jnp.minimum(gap, 0.0)) * gmask[k // per_group, rows, :]).astype(BF16)
            part = xdt_scr[rows, cols]
            none = jnp.zeros_like(part)
            stacked = jnp.concatenate(
                [jnp.where(part_head == h, part, none) for h in range(per_unit)], axis=0
            )
            base_scr[rows, cols] = base_scr[rows, cols] + dot(weights, stacked)

    def a_copy(k):
        return remote(out_a.at[k], buf_a.at[k], a_send, a_recv.at[k], jnp.minimum(me + 1, n - 1))

    def b_copy(k):
        return remote(out_b.at[k], buf_b.at[k], b_send, b_recv.at[k], jnp.maximum(me - 1, 0))

    def step_a(k):
        @pl.when(has_left)
        def _():
            a_copy(k).wait_recv()

        @pl.when(has_right)
        def _():
            out_a[k] = (buf_a[k].astype(F32) * tot_a[k][0:1] + sloc_a[k]).astype(BF16)
            a_copy(k).start()

    def step_b(k):
        cols = pl.ds(pl.multiple_of(k * piece, piece), piece)

        @pl.when(has_right)
        def _():
            b_copy(k).wait_recv()

        @pl.when(has_left)
        def _():
            mine = sloc_a[k] * wide_t[0:1, cols] + buf_b[k].astype(F32)
            out_b[k] = (mine * tot_b[k][0:1] + sloc_b[k]).astype(BF16)
            b_copy(k).start()

    def gate(k, which, state):
        cols = pl.ds(pl.multiple_of(k * unit, unit), unit)
        gcols = pl.ds(pl.multiple_of((k // per_group) * MN, MN), MN)
        rows = slice(which * half, (which + 1) * half)
        carried = dot(c_ref[rows, gcols], state) * er_scr[rows, cols]
        z = z_ref[rows, cols].astype(F32)
        gated[rows, cols] = ((base_scr[rows, cols] + carried) * silu(z)).astype(BF16)

    def send_gated(k, which):
        cols = pl.ds(pl.multiple_of(k * unit, unit), unit)
        send(gated, arrived, cols, o_send, o_recv, which)

    def gate_a(k):
        gate(k, 0, jnp.concatenate([buf_a[span * k + i] for i in range(span)], axis=1))

    def gate_b(k):
        entering = []
        for i in range(span):
            j = span * k + i
            cols = pl.ds(pl.multiple_of(j * piece, piece), piece)
            after = buf_a[j].astype(F32) * tot_a[j][0:1] + sloc_a[j]
            entering.append((after * wide_t[0:1, cols] + buf_b[j].astype(F32)).astype(BF16))
        gate(k, 1, jnp.concatenate(entering, axis=1))

    def take_log():
        @pl.when(has_right)
        def _():
            log_copy().wait_recv()
            later = log_in[...]
            @pl.when(has_left)
            def _():
                log_out[...] = later + own_log
                log_copy().start()

            shape = (heads, width)
            pick = lax.broadcasted_iota(jnp.int32, shape, 0) == lax.broadcasted_iota(jnp.int32, shape, 1) // MP
            high, mid, low = split(jnp.exp(later))
            pick = pick.astype(BF16)
            wide_t[...] = dot(high, pick) + dot(mid, pick) + dot(low, pick)

    def relay_right(h):
        source = jnp.maximum(me - h, 0)

        @pl.when(source != me)
        def _():
            kv_right(source).wait_recv()

        @pl.when(kv_right_on)
        def _():
            kv_right(source).start()

    def q_copy():
        return remote(q_ref, q_more, q_send, q_recv, jnp.maximum(me - 1, 0))

    def relay_left(h):
        source = jnp.minimum(me + h, n - 1)
        for copy in kv_left(source):
            @pl.when(source != me)
            def _(copy=copy):
                copy.wait_recv()

            @pl.when(has_left)
            def _(copy=copy):
                copy.start()

    def attention_mask(who):
        def clear(s, _):
            @pl.when(s < me)
            def _():
                kv_all[s, half:, :] = jnp.zeros((half, 2 * kv), BF16)

            return 0

        lax.fori_loop(0, n, clear, 0)
        key = lax.broadcasted_iota(jnp.int32, (tok, n * tok), 1)
        source = key // tok
        within = key - source * tok
        key_pos = jnp.where(
            within < half, source * half + within, (2 * n - 2 - source) * half + within
        )
        query = lax.broadcasted_iota(jnp.int32, (tok, n * tok), 0)
        query_pos = jnp.where(query < half, who * half + query, (2 * n - 2 - who) * half + query)
        bias_scr[...] = jnp.where(key_pos <= query_pos, 0.0, MASKED)

    scale = 1.0 / math.sqrt(HEAD_SIZE)

    def one_head(h, queries, stage):
        hcols = pl.ds(pl.multiple_of(h * HEAD_SIZE, HEAD_SIZE), HEAD_SIZE)
        kcols = pl.ds(pl.multiple_of((h // repeat) * HEAD_SIZE, HEAD_SIZE), HEAD_SIZE)
        vcols = pl.ds(pl.multiple_of(kv + (h // repeat) * HEAD_SIZE, HEAD_SIZE), HEAD_SIZE)
        keys = kv_all[:, :, kcols].reshape(n * tok, HEAD_SIZE)
        values = kv_all[:, :, vcols].reshape(n * tok, HEAD_SIZE)
        scores = dot(queries[:, hcols], keys, 1, 1) * scale + bias_scr[...]
        expo = jnp.exp(scores - jnp.max(scores, axis=-1, keepdims=True))
        total = jnp.sum(expo, axis=-1, keepdims=True)
        stage[:, hcols] = (dot(expo.astype(BF16), values) / total).astype(BF16)

    def send_ctx():
        for which in range(2):
            send(ctx_stage, ctx_out, slice(None), c_send, c_recv, which)

    loads[4].wait()
    hops = n - 1 - me
    middle = pieces // 2

    peers = has_left.astype(jnp.int32) + has_right.astype(jnp.int32) + int(paired)

    @pl.when(has_left)
    def _():
        pl.semaphore_wait(barrier, peers)

    @pl.when(jnp.logical_not(has_right))
    def _():
        log_out[...] = own_log
        log_copy().start()

    @pl.when(has_right & has_left)
    def _():
        for copy in kv_left(me):
            copy.start()

    @pl.when(kv_right_on & has_left)
    def _():
        kv_right(me).start()

    prepare(0)

    @pl.when(jnp.logical_not(has_left))
    def _():
        pl.semaphore_wait(barrier, peers)

    def first_step(k, _):
        @pl.when(k > 0)
        def _():
            prepare(k)

        @pl.when((k == units // 2) & (me == n - 1))
        def _():
            relay_left(0)

        for i in range(span):
            @pl.when(me == 0)
            def _(i=i):
                step_a(span * k + i)

            @pl.when(me == n - 1)
            def _(i=i):
                step_b(span * k + i)

        return 0

    between = has_left & has_right
    lax.fori_loop(0, jnp.where(between, units - 2, units), first_step, 0)
    for load in loads[5:7]:
        load.wait()

    @pl.when((me == 0) & kv_right_on)
    def _():
        relay_right(0)

    @pl.when(helped)
    def _():
        q_copy().start()

    def base(distance):
        return (14 * jnp.maximum(distance - 1, 0)) // 3

    lag_a = base(me)
    lag_b = base(hops)
    block_b = 2 * n - 1 - me
    hold_plus = block_b // 2 - 1 > me
    hold_minus = me // 2 + 1 < me
    gap = jnp.where(hops > 1, 6, 2)
    free = jnp.maximum(lag_a + pieces - 1, lag_b + pieces + gap + 1)
    gates = jnp.maximum(lag_a - 2, lag_b + gap) + pieces - units + 3
    gates = gates + jnp.where(2 * me < n, jnp.where(has_left, 1, 0), jnp.where(has_right, 7, 1))
    gates = jnp.maximum(gates, jnp.where(hold_plus, lag_a + pieces + 2, 0))
    gates = jnp.maximum(gates, jnp.where(hold_minus, lag_b + pieces + gap + 2, 0))
    quick = gates >= jnp.maximum(lag_a + pieces + 2, lag_b + pieces + gap + 2)
    ending = has_left & jnp.logical_not(has_right)
    first_out = jnp.where((2 * me < n) | jnp.logical_not(has_right), 1, 0)
    early = lag_b + middle + 1
    fills = has_left & has_right & (2 * me >= n) & (lag_a + 2 * span <= early)
    last = functools.reduce(jnp.maximum, [
        lag_a + pieces + 2, lag_b + pieces + gap + 2, gates + jnp.where(quick, middle // 2, middle),
        6 * n - 10, 2 * units,
    ])

    def greet_pair(pair_sem, peers):
        if paired:
            @pl.when(functools.reduce(jnp.logical_or, [ok for _, ok in peers]))
            def _():
                pl.semaphore_signal(pair_sem, inc=1, device_id={"hd": partner}, device_id_type=mesh_id)

    def release(pair_sem, sem, peers):
        if paired:
            @pl.when(functools.reduce(jnp.logical_or, [ok for _, ok in peers]))
            def _():
                pl.semaphore_wait(pair_sem, 1)

        for peer, ok in peers:
            @pl.when(ok)
            def _(peer=peer):
                pl.semaphore_signal(sem, inc=1, device_id={"ctx": peer}, device_id_type=mesh_id)

    plus_peers = [(p, (p >= 0) & (p < me)) for p in (2 * n - 3 - 2 * me, 2 * n - 4 - 2 * me)]
    minus_peers = [(p, (p > me) & (p < n)) for p in (2 * me - 2, 2 * me - 1)]
    plus_peers = [(p, ok & has_right) for p, ok in plus_peers]
    minus_peers = [(p, ok & has_left) for p, ok in minus_peers]

    def chain_a(t):
        at = t - lag_a

        @pl.when((at >= 0) & (at < pieces) & has_left)
        def _():
            step_a(at)

        @pl.when((at == pieces + 1) & has_left & kv_right_on)
        def _():
            relay_right(me)

        @pl.when((at == pieces - 3) & has_left)
        def _():
            greet_pair(pair_plus, plus_peers)

    def chain_b(t):
        at = t - lag_b

        @pl.when((at == 0) & has_right)
        def _():
            take_log()

        @pl.when((at == middle + gap) & has_right)
        def _():
            relay_left(hops)

        k = jnp.where(at < middle, at, at - gap - 2)

        @pl.when(((at >= 0) & (at < middle) | (at > middle + gap + 1) & (at <= pieces + gap + 1)) & has_right)
        def _():
            step_b(k)

        @pl.when((at == pieces + gap + 1) & has_right)
        def _():
            greet_pair(pair_minus, minus_peers)

    def slot_step(t, _):
        @pl.when(2 * me >= n)
        def _():
            chain_b(t)

        chain_a(t)

        @pl.when(2 * me < n)
        def _():
            chain_b(t)

        @pl.when(t == lag_a + pieces - 2)
        def _():
            release(pair_plus, plus_sem, plus_peers)

        @pl.when(t == free)
        def _():
            release(pair_minus, minus_sem, minus_peers)

        for h in range(1, n - 1):
            @pl.when((t == 4 * h - 4) & (h < me) & jnp.logical_not(helped))
            def _(h=h):
                relay_right(h)

            @pl.when((t == 6 * h - 4) & (h < hops))
            def _(h=h):
                relay_left(h)

        @pl.when(t == 0)
        def _():
            causal_products()

        @pl.when(between & ((t == 1) | (t == 3)))
        def _():
            prepare(units - 2 + t // 2)

        @pl.when((t < 2 * units) & (lax.rem(t, 2) == 0))
        def _():
            within_blocks(t // 2)

        @pl.when((t == gates) & hold_plus)
        def _():
            pl.semaphore_wait(plus_sem, 1)

        @pl.when((t == gates) & hold_minus)
        def _():
            pl.semaphore_wait(minus_sem, 1)

        @pl.when((t == early) & fills)
        def _():
            for i in range(2):
                gate_a(i)
            for i in range(2):
                send_gated(i, 0)

        @pl.when((t == lag_a + middle - 1) & ending)
        def _():
            def gate_early(i, _):
                for j in range(2):
                    gate_a(2 * i + j)
                    gate_b(2 * i + j)
                for j in range(2):
                    send_gated(2 * i + j, 1)
                return 0

            lax.fori_loop(0, units // 4, gate_early, 0)

        at = jnp.where(quick, 2, 1) * (t - gates)
        on = (at >= jnp.where(ending, units // 4 * 2, 0)) & (at < units) & (lax.rem(at, 2) == 0)
        done_a = fills & (at == 0)

        @pl.when(on & jnp.logical_not(done_a))
        def _():
            for i in range(2):
                gate_a(at + i)
                gate_b(at + i)
            for which in range(2):
                @pl.when(first_out == which)
                def _(which=which):
                    for i in range(2):
                        send_gated(at + i, which)

        @pl.when(on & done_a)
        def _():
            for i in range(2):
                gate_b(at + i)

        return 0

    lax.fori_loop(0, last, slot_step, 0)

    for which in range(2):
        @pl.when(first_out != which)
        def _(which=which):
            def send_rest(k, _):
                send_gated(k, which)
                return 0

            lax.fori_loop(0, units, send_rest, 0)

    def attend(who, queries, stage):
        attention_mask(who)

        def two_heads(i, _):
            one_head(2 * i, queries, stage)
            one_head(2 * i + 1, queries, stage)
            return 0

        lax.fori_loop(0, q_heads // 2, two_heads, 0)

    @pl.when(helper & has_left)
    def _():
        kv_right(0).wait_recv()

    @pl.when(jnp.logical_not(helped))
    def _():
        attend(me, q_ref, ctx_stage)
        send_ctx()

    @pl.when(helper)
    def _():
        q_copy().wait_recv()
        attend(n - 1, q_more, ctx_more)
        for which in range(2):
            send(ctx_more, ctx_out, slice(None), m_send, c_recv, which, jnp.int32(n - 1 + which))

    @pl.when(has_right)
    def _():
        remote(out_a, buf_a, a_send, a_recv.at[0], me).wait_send()

    @pl.when(has_left)
    def _():
        remote(out_b, buf_b, b_send, b_recv.at[0], me).wait_send()

    @pl.when(has_left)
    def _():
        log_copy().wait_send()

    for i in range(n):
        @pl.when((me == i) & kv_right_on)
        def _(i=i):
            part = kv_all.at[pl.ds(0, i + 1), first]
            remote(part, part, kv_plus, kv_recv.at[0, 0], me).wait_send()

        @pl.when((me == i) & has_left)
        def _(i=i):
            part = kv_all.at[pl.ds(i, n - i)]
            remote(part, part, kv_minus, kv_recv.at[0, 0], me).wait_send()

    def settle(stage, final, send_sem, recv_sem, away, missing):
        for count in (1, 2):
            rows = pl.ds(0, count * half)
            copy = remote(stage.at[rows], final.at[rows], send_sem, recv_sem, me)

            @pl.when(away == count)
            def _(copy=copy):
                copy.wait_send()

            @pl.when(missing == count)
            def _(copy=copy):
                copy.wait_recv()

    def tally(flags):
        return sum(jnp.where(flag, 1, 0) for flag in flags)

    def source_of(slot):
        block = 2 * me + slot
        return jnp.where(block < n, block, 2 * n - 1 - block)

    away = tally(block_id(which) // 2 != me for which in range(2))
    missing = tally(source_of(slot) != me for slot in range(2))
    served = [jnp.minimum(source_of(slot), n - 2) if n > 1 else source_of(slot) for slot in range(2)]
    served_missing = tally(source != me for source in served)
    more = sum(1 for block in (n - 1, n) if block // 2 != n - 2)

    @pl.when(helped)
    def _():
        q_copy().wait_send()

    settle(ctx_stage, ctx_out, c_send, c_recv, jnp.where(helped, 0, away), served_missing)
    settle(ctx_more, ctx_out, m_send, c_recv, jnp.where(helper, more, 0), 0)
    loads[7].wait()
    settle(gated, arrived, o_send, o_recv, away, missing)


def finish(groups, ctx_ref, gated_ref, gain_ref, ctx_out, mix_out, mixed, sems):
    tok, width = gated_ref.shape
    group_width = width // groups
    half = tok // 2
    copies = [pltpu.make_async_copy(ctx_ref, ctx_out, sems.at[0])]
    copies[0].start()
    for g in range(groups):
        for which in range(2):
            rows, cols = pl.ds(which * half, half), pl.ds(g * group_width, group_width)
            value = gated_ref[rows, cols].astype(F32)
            power = jnp.mean(value * value, axis=-1, keepdims=True)
            mixed[rows, cols] = (value * lax.rsqrt(power + NORM_EPS) * gain_ref[:, cols]).astype(BF16)
            copies.append(
                pltpu.make_async_copy(
                    mixed.at[rows, cols], mix_out.at[rows, cols], sems.at[1 + 2 * g + which]
                )
            )
            copies[-1].start()
    for copy in copies:
        copy.wait()


def body(n, wide_hd, query, keys, values, m_x, m_z, m_b, m_c, dt_raw, dt_bias, a_log, d_skip, norm_gain):
    tok, width = m_x.shape
    half = tok // 2
    heads = dt_raw.shape[1]
    anywhere = pl.BlockSpec(memory_space=INPUT_SPACE)
    groups = m_b.shape[1] // MN
    piece = math.gcd(width // groups, PIECE)
    pieces = width // piece
    unit = math.gcd(width // groups, UNIT)
    units = width // unit
    kv = keys.shape[1]
    q_heads = query.shape[1] // HEAD_SIZE
    dma = pltpu.SemaphoreType.DMA
    vmem = pltpu.VMEM
    state = (pieces, MN, piece)
    spec = pl.BlockSpec(memory_space=pltpu.VMEM)
    spare = 2 * (query.size + m_x.size) + 4 * width + 49152
    context, gated, gain = pl.pallas_call(
        functools.partial(kernel, n, wide_hd),
        out_shape=(
            vmem(query.shape, BF16),
            vmem(m_x.shape, BF16),
            vmem((1, width), F32),
        ),
        in_specs=[anywhere] * 12,
        out_specs=(spec, spec, spec),
        scratch_shapes=[
            vmem(query.shape, BF16),
            vmem(m_x.shape, BF16),
            vmem(m_x.shape, BF16),
            vmem((2,) + m_b.shape, BF16),
            vmem((heads, tok), BF16),
            vmem((3, 1, heads), F32),
            vmem((n, tok, 2 * kv), BF16),
            vmem((tok, n * tok), F32),
            vmem(query.shape, BF16),
            vmem(m_x.shape, BF16),
            vmem((tok, width), F32),
            vmem((tok, width), F32),
            vmem((tok, width), BF16),
            vmem((3 * tok + 16, 3 * heads), BF16),
            vmem((tok, 3 * heads), BF16),
            vmem((groups, tok, unit // MP * (tok // 2)), F32),
            vmem(state, BF16),
            vmem(state, BF16),
            vmem(state, BF16),
            vmem(state, BF16),
            vmem(state, F32),
            vmem(state, F32),
            vmem((pieces, 8, piece), F32),
            vmem((pieces, 8, piece), F32),
            vmem((8, heads), F32),
            vmem((8, heads), F32),
            vmem((8, width), F32),
            dma(()),
            dma(()),
            dma((n, 2)),
            dma(()),
            dma((pieces,)),
            dma(()),
            dma((pieces,)),
            dma(()),
            dma(()),
            dma(()),
            dma(()),
            dma(()),
            dma(()),
            vmem(query.shape, BF16),
            vmem(query.shape, BF16),
            dma(()),
            dma(()),
            dma(()),
            pltpu.SemaphoreType.REGULAR,
            pltpu.SemaphoreType.REGULAR,
            pltpu.SemaphoreType.REGULAR,
            pltpu.SemaphoreType.REGULAR,
            dma((8,)),
        ],
        compiler_params=pltpu.CompilerParams(
            collective_id=0, has_side_effects=True, vmem_limit_bytes=VMEM_BYTES - spare
        ),
    )(
        query, keys, values, m_x, m_z, m_b, m_c, dt_raw.T,
        dt_bias.reshape(1, -1), a_log.reshape(1, -1), d_skip.reshape(1, -1), norm_gain.reshape(1, -1),
    )
    return pl.pallas_call(
        functools.partial(finish, groups),
        out_shape=(
            jax.ShapeDtypeStruct(query.shape, BF16),
            jax.ShapeDtypeStruct(m_x.shape, BF16),
        ),
        in_specs=[spec] * 3,
        out_specs=(anywhere, anywhere),
        scratch_shapes=[vmem(m_x.shape, BF16), dma((1 + 2 * groups,))],
        compiler_params=pltpu.CompilerParams(vmem_limit_bytes=4 << 20),
    )(context, gated, gain)


def solution(mesh):
    rows = P(("grp", "ctx"), "hd")
    in_specs = (rows,) * 8 + (P("hd"),) * 4
    return jax.shard_map(
        functools.partial(body, mesh.shape["ctx"], mesh.shape["hd"]),
        mesh=mesh, in_specs=in_specs, out_specs=(rows, rows), check_vma=False,
    )
```

```python
import functools
import math

import jax
import jax.numpy as jnp
from jax import lax
from jax.experimental import pallas as pl
from jax.experimental.pallas import tpu as pltpu
from jax.sharding import PartitionSpec as P

HEAD_SIZE = 128
MP = 64
MN = 128
NORM_EPS = 1e-05
MASKED = -1e30
HIGHEST = lax.Precision.HIGHEST
F32 = jnp.float32
BF16 = jnp.bfloat16
INPUT_SPACE = pltpu.HBM
PIECE = 128
UNIT = 256
VMEM_BYTES = 67043328


def dot(a, b, ca=1, cb=0, precision=None):
    return lax.dot_general(
        a, b, (((ca,), (cb,)), ((), ())), preferred_element_type=F32, precision=precision
    )


def split(value):
    high = value.astype(BF16)
    rest = value - high.astype(F32)
    mid = rest.astype(BF16)
    return high, mid, (rest - mid.astype(F32)).astype(BF16)


def kernel(
    n, wide_hd, q_in, k_in, v_in, x_in, z_in, b_in, c_in, dt_in, bias_in, alog_in, skip_in,
    gain_in, ctx_out, arrived, gain_ref,
    q_ref, x_ref, z_ref, bc_ref, dt_ref, small_ref,
    kv_all, bias_scr, ctx_stage, gated, base_scr, er_scr, xdt_scr, hs, run_split, gmask,
    buf_a, buf_b, out_a, out_b, sloc_a, sloc_b, tot_a, tot_b, log_in, log_out, wide_t,
    kv_plus, kv_minus, kv_recv, a_send, a_recv, b_send, b_recv, o_send, o_recv, c_send, c_recv,
    log_send, log_recv, q_more, ctx_more, q_send, q_recv, m_send, plus_sem, minus_sem, pair_plus, pair_minus, load_sem,
):
    me = lax.axis_index("ctx")
    tok = q_ref.shape[0]
    half = tok // 2
    heads = dt_ref.shape[0]
    width = x_ref.shape[1]
    groups = bc_ref.shape[2] // MN
    group_width = width // groups
    pieces, _, piece = buf_a.shape
    unit = math.gcd(group_width, UNIT)
    units = width // unit
    per_unit = unit // MP
    per_group = group_width // unit
    span = unit // piece
    q_heads = q_ref.shape[1] // HEAD_SIZE
    kv = kv_all.shape[2] // 2
    repeat = q_ref.shape[1] // kv
    mesh_id = pl.DeviceIdType.MESH
    core = lax.axis_index("hd")
    paired = wide_hd % 2 == 0
    partner = core + 1 - 2 * lax.rem(core, 2)
    has_left = me > 0
    has_right = me < n - 1
    helped = (me == n - 1) & (n > 1)
    helper = (me == n - 2) & (n > 1)
    kv_right_on = me < n - 2

    b_ref, c_ref = bc_ref.at[0], bc_ref.at[1]
    bias_ref, alog_ref, skip_ref = (small_ref.at[i] for i in range(3))
    parts = (
        ((dt_in, dt_ref),),
        ((bias_in, bias_ref), (alog_in, alog_ref), (skip_in, skip_ref)),
        ((k_in, kv_all.at[me, :, pl.ds(0, kv)]), (v_in, kv_all.at[me, :, pl.ds(kv, kv)])),
        ((b_in, b_ref), (c_in, c_ref)), ((x_in, x_ref),), ((z_in, z_ref),), ((q_in, q_ref),),
        ((gain_in, gain_ref),),
    )
    wholes = (dt_ref, small_ref, kv_all.at[me], bc_ref, x_ref, z_ref, q_ref, gain_ref)
    loads = [
        pltpu.make_async_copy(whole, whole, load_sem.at[i]) for i, whole in enumerate(wholes)
    ]

    barrier = pltpu.get_barrier_semaphore()

    def greet(peer):
        pl.semaphore_signal(barrier, inc=1, device_id={"ctx": peer}, device_id_type=mesh_id)

    @pl.when(has_left)
    def _():
        greet(me - 1)

    @pl.when(has_right)
    def _():
        greet(me + 1)

    if paired:
        pl.semaphore_signal(barrier, inc=1, device_id={"hd": partner}, device_id_type=mesh_id)

    for i, pairs in enumerate(parts):
        for src, dst in pairs:
            pltpu.make_async_copy(src, dst, load_sem.at[i]).start()

    def remote(src, dst, send, recv, peer):
        return pltpu.make_async_remote_copy(
            src_ref=src, dst_ref=dst, send_sem=send, recv_sem=recv,
            device_id={"ctx": peer}, device_id_type=mesh_id,
        )

    first = pl.ds(0, half)

    def kv_right(s):
        part = kv_all.at[s, first]
        return remote(part, part, kv_plus, kv_recv.at[s, 0], jnp.minimum(me + 1, n - 1))

    def kv_left(s):
        copies = []
        for i in range(2):
            part = kv_all.at[s, pl.ds(i * half, half)]
            copies.append(
                remote(part, part, kv_minus, kv_recv.at[s, i], jnp.maximum(me - 1, 0))
            )
        return copies

    def log_copy():
        return remote(log_out, log_in, log_send, log_recv, jnp.maximum(me - 1, 0))

    row = lax.broadcasted_iota(jnp.int32, (tok, tok), 0)
    col = lax.broadcasted_iota(jnp.int32, (tok, tok), 1)
    for load in loads[:2]:
        load.wait()
    raw = dot((row == col).astype(BF16), dt_ref[...], 1, 1) + bias_ref[...]
    steps = jnp.maximum(raw, 0.0) + jnp.log1p(jnp.exp(-jnp.abs(raw)))
    decay = -steps * jnp.exp(alog_ref[...])
    lower = (col <= row) & ((row < half) == (col < half))
    tri = lower.astype(BF16)
    high, mid, low = split(decay)
    run = dot(tri, high) + dot(tri, mid) + dot(tri, low)
    ends = jnp.where(
        lax.broadcasted_iota(jnp.int32, (tok, heads), 0) < half, run[half - 1 : half], run[tok - 1 : tok]
    )

    def keep_split(ref, start, value):
        for i, part in enumerate(split(value)):
            ref[start : start + value.shape[0], i * heads : (i + 1) * heads] = part

    keep_split(run_split, 0, run)
    keep_split(hs, 0, jnp.exp(run))
    keep_split(hs, tok, jnp.exp(ends - run) * steps)
    keep_split(hs, 2 * tok, steps)
    keep_split(hs, 3 * tok, jnp.broadcast_to(skip_ref[...], (16, heads)))
    own_log = jnp.broadcast_to(run[half - 1 : half] + run[tok - 1 : tok], (8, heads))

    for load in loads[2:4]:
        load.wait()
    lanes = per_unit * half
    lane = lax.broadcasted_iota(jnp.int32, (half, lanes), 1)
    source = lane - lane // half * half
    target = lax.broadcasted_iota(jnp.int32, (half, lanes), 0)
    causal = source <= target
    diagonal = source == target

    def causal_products():
        for g in range(groups):
            cols = slice(g * MN, (g + 1) * MN)
            for which in range(2):
                rows = slice(which * half, (which + 1) * half)
                repeated = jnp.concatenate([b_ref[rows, cols]] * per_unit, axis=0)
                gmask[g, rows, :] = jnp.where(causal, dot(c_ref[rows, cols], repeated, 1, 1), 0.0)

    @pl.when(me == 0)
    def _():
        buf_a[...] = jnp.zeros_like(buf_a)

    @pl.when(me == n - 1)
    def _():
        buf_b[...] = jnp.zeros_like(buf_b)
        wide_t[...] = jnp.ones_like(wide_t)

    split_head = lax.rem(lax.broadcasted_iota(jnp.int32, (3 * heads, unit), 0), heads)
    lane_head = lax.broadcasted_iota(jnp.int32, (3 * heads, unit), 1) // MP
    wide_head = lax.rem(lax.broadcasted_iota(jnp.int32, (3 * heads, lanes), 0), heads)
    wide_lane = lax.broadcasted_iota(jnp.int32, (3 * heads, lanes), 1) // half
    part_head = lax.broadcasted_iota(jnp.int32, (half, unit), 1) // MP

    def block_id(which):
        return me if which == 0 else 2 * n - 1 - me

    def send(stage, final, cols, send_sem, recv_sem, which, block=None):
        block = block_id(which) if block is None else block
        owner = block // 2
        slot = lax.rem(block, 2)
        rows = pl.ds(which * half, half)
        target = pl.ds(pl.multiple_of(slot * half, half), half)

        @pl.when(owner == me)
        def _():
            final[target, cols] = stage[rows, cols]

        @pl.when(owner != me)
        def _():
            remote(
                stage.at[rows, cols], final.at[target, cols], send_sem, recv_sem, owner
            ).start()

    def silu(value):
        return value / (1.0 + jnp.exp(-value))

    def prepare(k):
        cols = pl.ds(pl.multiple_of(k * unit, unit), unit)
        gcols = pl.ds(pl.multiple_of((k // per_group) * MN, MN), MN)
        spread = dot(hs[...], (split_head == k * per_unit + lane_head).astype(BF16))
        xs = x_ref[:, cols].astype(F32)
        weighted = (xs * spread[tok : 2 * tok]).astype(BF16)
        b_rows = b_ref[:, gcols]
        local_a = dot(b_rows[0:half], weighted[0:half], 0, 0)
        local_b = dot(b_rows[half:], weighted[half:], 0, 0)
        for i in range(span):
            part = slice(i * piece, (i + 1) * piece)
            sloc_a[span * k + i] = local_a[:, part]
            sloc_b[span * k + i] = local_b[:, part]
            tot_a[span * k + i] = jnp.broadcast_to(spread[half - 1 : half, part], (8, piece))
            tot_b[span * k + i] = jnp.broadcast_to(spread[tok - 1 : tok, part], (8, piece))
        er_scr[:, cols] = spread[0:tok]
        xdt_scr[:, cols] = (xs * spread[2 * tok : 3 * tok]).astype(BF16)
        base_scr[:, cols] = spread[3 * tok : 3 * tok + 1] * xs

    def within_blocks(k):
        cols = pl.ds(pl.multiple_of(k * unit, unit), unit)
        wide = dot(run_split[...], (wide_head == k * per_unit + wide_lane).astype(BF16))
        for which in range(2):
            rows = slice(which * half, (which + 1) * half)
            mine = wide[rows]
            gap = mine - jnp.sum(jnp.where(diagonal, mine, 0.0), axis=0, keepdims=True)
            weights = (jnp.exp(jnp.minimum(gap, 0.0)) * gmask[k // per_group, rows, :]).astype(BF16)
            part = xdt_scr[rows, cols]
            none = jnp.zeros_like(part)
            stacked = jnp.concatenate(
                [jnp.where(part_head == h, part, none) for h in range(per_unit)], axis=0
            )
            base_scr[rows, cols] = base_scr[rows, cols] + dot(weights, stacked)

    def a_copy(k):
        return remote(out_a.at[k], buf_a.at[k], a_send, a_recv.at[k], jnp.minimum(me + 1, n - 1))

    def b_copy(k):
        return remote(out_b.at[k], buf_b.at[k], b_send, b_recv.at[k], jnp.maximum(me - 1, 0))

    def step_a(k):
        @pl.when(has_left)
        def _():
            a_copy(k).wait_recv()

        @pl.when(has_right)
        def _():
            out_a[k] = (buf_a[k].astype(F32) * tot_a[k][0:1] + sloc_a[k]).astype(BF16)
            a_copy(k).start()

    def step_b(k):
        cols = pl.ds(pl.multiple_of(k * piece, piece), piece)

        @pl.when(has_right)
        def _():
            b_copy(k).wait_recv()

        @pl.when(has_left)
        def _():
            mine = sloc_a[k] * wide_t[0:1, cols] + buf_b[k].astype(F32)
            out_b[k] = (mine * tot_b[k][0:1] + sloc_b[k]).astype(BF16)
            b_copy(k).start()

    def gate(k, which, state):
        cols = pl.ds(pl.multiple_of(k * unit, unit), unit)
        gcols = pl.ds(pl.multiple_of((k // per_group) * MN, MN), MN)
        rows = slice(which * half, (which + 1) * half)
        carried = dot(c_ref[rows, gcols], state) * er_scr[rows, cols]
        z = z_ref[rows, cols].astype(F32)
        gated[rows, cols] = ((base_scr[rows, cols] + carried) * silu(z)).astype(BF16)

    def send_gated(k, which):
        cols = pl.ds(pl.multiple_of(k * unit, unit), unit)
        send(gated, arrived, cols, o_send, o_recv, which)

    def gate_a(k):
        gate(k, 0, jnp.concatenate([buf_a[span * k + i] for i in range(span)], axis=1))

    def gate_b(k):
        entering = []
        for i in range(span):
            j = span * k + i
            cols = pl.ds(pl.multiple_of(j * piece, piece), piece)
            after = buf_a[j].astype(F32) * tot_a[j][0:1] + sloc_a[j]
            entering.append((after * wide_t[0:1, cols] + buf_b[j].astype(F32)).astype(BF16))
        gate(k, 1, jnp.concatenate(entering, axis=1))

    def take_log():
        @pl.when(has_right)
        def _():
            log_copy().wait_recv()
            later = log_in[...]
            @pl.when(has_left)
            def _():
                log_out[...] = later + own_log
                log_copy().start()

            shape = (heads, width)
            pick = lax.broadcasted_iota(jnp.int32, shape, 0) == lax.broadcasted_iota(jnp.int32, shape, 1) // MP
            high, mid, low = split(jnp.exp(later))
            pick = pick.astype(BF16)
            wide_t[...] = dot(high, pick) + dot(mid, pick) + dot(low, pick)

    def relay_right(h):
        source = jnp.maximum(me - h, 0)

        @pl.when(source != me)
        def _():
            kv_right(source).wait_recv()

        @pl.when(kv_right_on)
        def _():
            kv_right(source).start()

    def q_copy():
        return remote(q_ref, q_more, q_send, q_recv, jnp.maximum(me - 1, 0))

    def relay_left(h):
        source = jnp.minimum(me + h, n - 1)
        for copy in kv_left(source):
            @pl.when(source != me)
            def _(copy=copy):
                copy.wait_recv()

            @pl.when(has_left)
            def _(copy=copy):
                copy.start()

    def attention_mask(who):
        def clear(s, _):
            @pl.when(s < me)
            def _():
                kv_all[s, half:, :] = jnp.zeros((half, 2 * kv), BF16)

            return 0

        lax.fori_loop(0, n, clear, 0)
        key = lax.broadcasted_iota(jnp.int32, (tok, n * tok), 1)
        source = key // tok
        within = key - source * tok
        key_pos = jnp.where(
            within < half, source * half + within, (2 * n - 2 - source) * half + within
        )
        query = lax.broadcasted_iota(jnp.int32, (tok, n * tok), 0)
        query_pos = jnp.where(query < half, who * half + query, (2 * n - 2 - who) * half + query)
        bias_scr[...] = jnp.where(key_pos <= query_pos, 0.0, MASKED)

    scale = 1.0 / math.sqrt(HEAD_SIZE)

    def one_head(h, queries, stage):
        hcols = pl.ds(pl.multiple_of(h * HEAD_SIZE, HEAD_SIZE), HEAD_SIZE)
        kcols = pl.ds(pl.multiple_of((h // repeat) * HEAD_SIZE, HEAD_SIZE), HEAD_SIZE)
        vcols = pl.ds(pl.multiple_of(kv + (h // repeat) * HEAD_SIZE, HEAD_SIZE), HEAD_SIZE)
        keys = kv_all[:, :, kcols].reshape(n * tok, HEAD_SIZE)
        values = kv_all[:, :, vcols].reshape(n * tok, HEAD_SIZE)
        scores = dot(queries[:, hcols], keys, 1, 1) * scale + bias_scr[...]
        expo = jnp.exp(scores - jnp.max(scores, axis=-1, keepdims=True))
        total = jnp.sum(expo, axis=-1, keepdims=True)
        stage[:, hcols] = (dot(expo.astype(BF16), values) / total).astype(BF16)

    def send_ctx():
        for which in range(2):
            send(ctx_stage, ctx_out, slice(None), c_send, c_recv, which)

    loads[4].wait()
    hops = n - 1 - me
    middle = pieces // 2

    peers = has_left.astype(jnp.int32) + has_right.astype(jnp.int32) + int(paired)

    @pl.when(has_left)
    def _():
        pl.semaphore_wait(barrier, peers)

    @pl.when(jnp.logical_not(has_right))
    def _():
        log_out[...] = own_log
        log_copy().start()

    @pl.when(has_right & has_left)
    def _():
        for copy in kv_left(me):
            copy.start()

    @pl.when(kv_right_on & has_left)
    def _():
        kv_right(me).start()

    prepare(0)

    @pl.when(jnp.logical_not(has_left))
    def _():
        pl.semaphore_wait(barrier, peers)

    def first_step(k, _):
        @pl.when(k > 0)
        def _():
            prepare(k)

        @pl.when((k == units // 2) & (me == n - 1))
        def _():
            relay_left(0)

        for i in range(span):
            @pl.when(me == 0)
            def _(i=i):
                step_a(span * k + i)

            @pl.when(me == n - 1)
            def _(i=i):
                step_b(span * k + i)

        return 0

    between = has_left & has_right
    lax.fori_loop(0, jnp.where(between, units - 2, units), first_step, 0)
    for load in loads[5:7]:
        load.wait()

    @pl.when((me == 0) & kv_right_on)
    def _():
        relay_right(0)

    @pl.when(helped)
    def _():
        q_copy().start()

    def base(distance):
        return (14 * jnp.maximum(distance - 1, 0)) // 3

    lag_a = base(me)
    lag_b = base(hops)
    block_b = 2 * n - 1 - me
    hold_plus = block_b // 2 - 1 > me
    hold_minus = me // 2 + 1 < me
    gap = jnp.where(hops > 1, 6, 2)
    free = jnp.maximum(lag_a + pieces - 1, lag_b + pieces + gap + 1)
    gates = jnp.maximum(lag_a - 2, lag_b + gap) + pieces - units + 3
    gates = gates + jnp.where(2 * me < n, jnp.where(has_left, 1, 0), jnp.where(has_right, 7, 1))
    gates = jnp.maximum(gates, jnp.where(hold_plus, lag_a + pieces + 2, 0))
    gates = jnp.maximum(gates, jnp.where(hold_minus, lag_b + pieces + gap + 2, 0))
    quick = gates >= jnp.maximum(lag_a + pieces + 2, lag_b + pieces + gap + 2)
    ending = has_left & jnp.logical_not(has_right)
    first_out = jnp.where((2 * me < n) | jnp.logical_not(has_right), 1, 0)
    early = lag_b + middle
    fills = has_left & has_right & (2 * me >= n) & (lag_a + 2 * span <= early)
    last = functools.reduce(jnp.maximum, [
        lag_a + pieces + 2, lag_b + pieces + gap + 2, gates + jnp.where(quick, middle // 2, middle),
        6 * n - 10, 2 * units,
    ])

    def greet_pair(pair_sem, peers):
        if paired:
            @pl.when(functools.reduce(jnp.logical_or, [ok for _, ok in peers]))
            def _():
                pl.semaphore_signal(pair_sem, inc=1, device_id={"hd": partner}, device_id_type=mesh_id)

    def release(pair_sem, sem, peers):
        if paired:
            @pl.when(functools.reduce(jnp.logical_or, [ok for _, ok in peers]))
            def _():
                pl.semaphore_wait(pair_sem, 1)

        for peer, ok in peers:
            @pl.when(ok)
            def _(peer=peer):
                pl.semaphore_signal(sem, inc=1, device_id={"ctx": peer}, device_id_type=mesh_id)

    plus_peers = [(p, (p >= 0) & (p < me)) for p in (2 * n - 3 - 2 * me, 2 * n - 4 - 2 * me)]
    minus_peers = [(p, (p > me) & (p < n)) for p in (2 * me - 2, 2 * me - 1)]
    plus_peers = [(p, ok & has_right) for p, ok in plus_peers]
    minus_peers = [(p, ok & has_left) for p, ok in minus_peers]

    def chain_a(t):
        at = t - lag_a

        @pl.when((at >= 0) & (at < pieces) & has_left)
        def _():
            step_a(at)

        @pl.when((at == pieces + 1) & has_left & kv_right_on)
        def _():
            relay_right(me)

        @pl.when((at == pieces - 3) & has_left)
        def _():
            greet_pair(pair_plus, plus_peers)

    def chain_b(t):
        at = t - lag_b

        @pl.when((at == 0) & has_right)
        def _():
            take_log()

        @pl.when((at == middle + gap) & has_right)
        def _():
            relay_left(hops)

        k = jnp.where(at < middle, at, at - gap - 2)

        @pl.when(((at >= 0) & (at < middle) | (at > middle + gap + 1) & (at <= pieces + gap + 1)) & has_right)
        def _():
            step_b(k)

        @pl.when((at == pieces + gap + 1) & has_right)
        def _():
            greet_pair(pair_minus, minus_peers)

    def slot_step(t, _):
        @pl.when(2 * me >= n)
        def _():
            chain_b(t)

        chain_a(t)

        @pl.when(2 * me < n)
        def _():
            chain_b(t)

        @pl.when(t == lag_a + pieces - 2)
        def _():
            release(pair_plus, plus_sem, plus_peers)

        @pl.when(t == free)
        def _():
            release(pair_minus, minus_sem, minus_peers)

        for h in range(1, n - 1):
            @pl.when((t == 4 * h - 4) & (h < me) & jnp.logical_not(helped))
            def _(h=h):
                relay_right(h)

            @pl.when((t == 6 * h - 4) & (h < hops))
            def _(h=h):
                relay_left(h)

        @pl.when(t == 0)
        def _():
            causal_products()

        @pl.when(between & ((t == 1) | (t == 3)))
        def _():
            prepare(units - 2 + t // 2)

        @pl.when((t < 2 * units) & (lax.rem(t, 2) == 0))
        def _():
            within_blocks(t // 2)

        @pl.when((t == gates) & hold_plus)
        def _():
            pl.semaphore_wait(plus_sem, 1)

        @pl.when((t == gates) & hold_minus)
        def _():
            pl.semaphore_wait(minus_sem, 1)

        @pl.when((t == early) & fills)
        def _():
            for i in range(2):
                gate_a(i)
            for i in range(2):
                send_gated(i, 0)

        @pl.when((t == lag_a + middle - 1) & ending)
        def _():
            def gate_early(i, _):
                for j in range(2):
                    gate_a(2 * i + j)
                    gate_b(2 * i + j)
                for j in range(2):
                    send_gated(2 * i + j, 1)
                return 0

            lax.fori_loop(0, units // 4, gate_early, 0)

        at = jnp.where(quick, 2, 1) * (t - gates)
        on = (at >= jnp.where(ending, units // 4 * 2, 0)) & (at < units) & (lax.rem(at, 2) == 0)
        done_a = fills & (at == 0)

        @pl.when(on & jnp.logical_not(done_a))
        def _():
            for i in range(2):
                gate_a(at + i)
                gate_b(at + i)
            for which in range(2):
                @pl.when(first_out == which)
                def _(which=which):
                    for i in range(2):
                        send_gated(at + i, which)

        @pl.when(on & done_a)
        def _():
            for i in range(2):
                gate_b(at + i)

        return 0

    lax.fori_loop(0, last, slot_step, 0)

    for which in range(2):
        @pl.when(first_out != which)
        def _(which=which):
            def send_rest(k, _):
                send_gated(k, which)
                return 0

            lax.fori_loop(0, units, send_rest, 0)

    def attend(who, queries, stage):
        attention_mask(who)

        def two_heads(i, _):
            one_head(2 * i, queries, stage)
            one_head(2 * i + 1, queries, stage)
            return 0

        lax.fori_loop(0, q_heads // 2, two_heads, 0)

    @pl.when(helper & has_left)
    def _():
        kv_right(0).wait_recv()

    @pl.when(jnp.logical_not(helped))
    def _():
        attend(me, q_ref, ctx_stage)
        send_ctx()

    @pl.when(helper)
    def _():
        q_copy().wait_recv()
        attend(n - 1, q_more, ctx_more)
        for which in range(2):
            send(ctx_more, ctx_out, slice(None), m_send, c_recv, which, jnp.int32(n - 1 + which))

    @pl.when(has_right)
    def _():
        remote(out_a, buf_a, a_send, a_recv.at[0], me).wait_send()

    @pl.when(has_left)
    def _():
        remote(out_b, buf_b, b_send, b_recv.at[0], me).wait_send()

    @pl.when(has_left)
    def _():
        log_copy().wait_send()

    for i in range(n):
        @pl.when((me == i) & kv_right_on)
        def _(i=i):
            part = kv_all.at[pl.ds(0, i + 1), first]
            remote(part, part, kv_plus, kv_recv.at[0, 0], me).wait_send()

        @pl.when((me == i) & has_left)
        def _(i=i):
            part = kv_all.at[pl.ds(i, n - i)]
            remote(part, part, kv_minus, kv_recv.at[0, 0], me).wait_send()

    def settle(stage, final, send_sem, recv_sem, away, missing):
        for count in (1, 2):
            rows = pl.ds(0, count * half)
            copy = remote(stage.at[rows], final.at[rows], send_sem, recv_sem, me)

            @pl.when(away == count)
            def _(copy=copy):
                copy.wait_send()

            @pl.when(missing == count)
            def _(copy=copy):
                copy.wait_recv()

    def tally(flags):
        return sum(jnp.where(flag, 1, 0) for flag in flags)

    def source_of(slot):
        block = 2 * me + slot
        return jnp.where(block < n, block, 2 * n - 1 - block)

    away = tally(block_id(which) // 2 != me for which in range(2))
    missing = tally(source_of(slot) != me for slot in range(2))
    served = [jnp.minimum(source_of(slot), n - 2) if n > 1 else source_of(slot) for slot in range(2)]
    served_missing = tally(source != me for source in served)
    more = sum(1 for block in (n - 1, n) if block // 2 != n - 2)

    @pl.when(helped)
    def _():
        q_copy().wait_send()

    settle(ctx_stage, ctx_out, c_send, c_recv, jnp.where(helped, 0, away), served_missing)
    settle(ctx_more, ctx_out, m_send, c_recv, jnp.where(helper, more, 0), 0)
    loads[7].wait()
    settle(gated, arrived, o_send, o_recv, away, missing)


def finish(groups, ctx_ref, gated_ref, gain_ref, ctx_out, mix_out, mixed, sems):
    tok, width = gated_ref.shape
    group_width = width // groups
    half = tok // 2
    copies = [pltpu.make_async_copy(ctx_ref, ctx_out, sems.at[0])]
    copies[0].start()
    for g in range(groups):
        for which in range(2):
            rows, cols = pl.ds(which * half, half), pl.ds(g * group_width, group_width)
            value = gated_ref[rows, cols].astype(F32)
            power = jnp.mean(value * value, axis=-1, keepdims=True)
            mixed[rows, cols] = (value * lax.rsqrt(power + NORM_EPS) * gain_ref[:, cols]).astype(BF16)
            copies.append(
                pltpu.make_async_copy(
                    mixed.at[rows, cols], mix_out.at[rows, cols], sems.at[1 + 2 * g + which]
                )
            )
            copies[-1].start()
    for copy in copies:
        copy.wait()


def body(n, wide_hd, query, keys, values, m_x, m_z, m_b, m_c, dt_raw, dt_bias, a_log, d_skip, norm_gain):
    tok, width = m_x.shape
    half = tok // 2
    heads = dt_raw.shape[1]
    anywhere = pl.BlockSpec(memory_space=INPUT_SPACE)
    groups = m_b.shape[1] // MN
    piece = math.gcd(width // groups, PIECE)
    pieces = width // piece
    unit = math.gcd(width // groups, UNIT)
    units = width // unit
    kv = keys.shape[1]
    q_heads = query.shape[1] // HEAD_SIZE
    dma = pltpu.SemaphoreType.DMA
    vmem = pltpu.VMEM
    state = (pieces, MN, piece)
    spec = pl.BlockSpec(memory_space=pltpu.VMEM)
    spare = 2 * (query.size + m_x.size) + 4 * width + 49152
    context, gated, gain = pl.pallas_call(
        functools.partial(kernel, n, wide_hd),
        out_shape=(
            vmem(query.shape, BF16),
            vmem(m_x.shape, BF16),
            vmem((1, width), F32),
        ),
        in_specs=[anywhere] * 12,
        out_specs=(spec, spec, spec),
        scratch_shapes=[
            vmem(query.shape, BF16),
            vmem(m_x.shape, BF16),
            vmem(m_x.shape, BF16),
            vmem((2,) + m_b.shape, BF16),
            vmem((heads, tok), BF16),
            vmem((3, 1, heads), F32),
            vmem((n, tok, 2 * kv), BF16),
            vmem((tok, n * tok), F32),
            vmem(query.shape, BF16),
            vmem(m_x.shape, BF16),
            vmem((tok, width), F32),
            vmem((tok, width), F32),
            vmem((tok, width), BF16),
            vmem((3 * tok + 16, 3 * heads), BF16),
            vmem((tok, 3 * heads), BF16),
            vmem((groups, tok, unit // MP * (tok // 2)), F32),
            vmem(state, BF16),
            vmem(state, BF16),
            vmem(state, BF16),
            vmem(state, BF16),
            vmem(state, F32),
            vmem(state, F32),
            vmem((pieces, 8, piece), F32),
            vmem((pieces, 8, piece), F32),
            vmem((8, heads), F32),
            vmem((8, heads), F32),
            vmem((8, width), F32),
            dma(()),
            dma(()),
            dma((n, 2)),
            dma(()),
            dma((pieces,)),
            dma(()),
            dma((pieces,)),
            dma(()),
            dma(()),
            dma(()),
            dma(()),
            dma(()),
            dma(()),
            vmem(query.shape, BF16),
            vmem(query.shape, BF16),
            dma(()),
            dma(()),
            dma(()),
            pltpu.SemaphoreType.REGULAR,
            pltpu.SemaphoreType.REGULAR,
            pltpu.SemaphoreType.REGULAR,
            pltpu.SemaphoreType.REGULAR,
            dma((8,)),
        ],
        compiler_params=pltpu.CompilerParams(
            collective_id=0, has_side_effects=True, vmem_limit_bytes=VMEM_BYTES - spare
        ),
    )(
        query, keys, values, m_x, m_z, m_b, m_c, dt_raw.T,
        dt_bias.reshape(1, -1), a_log.reshape(1, -1), d_skip.reshape(1, -1), norm_gain.reshape(1, -1),
    )
    return pl.pallas_call(
        functools.partial(finish, groups),
        out_shape=(
            jax.ShapeDtypeStruct(query.shape, BF16),
            jax.ShapeDtypeStruct(m_x.shape, BF16),
        ),
        in_specs=[spec] * 3,
        out_specs=(anywhere, anywhere),
        scratch_shapes=[vmem(m_x.shape, BF16), dma((1 + 2 * groups,))],
        compiler_params=pltpu.CompilerParams(vmem_limit_bytes=4 << 20),
    )(context, gated, gain)


def solution(mesh):
    rows = P(("grp", "ctx"), "hd")
    in_specs = (rows,) * 8 + (P("hd"),) * 4
    return jax.shard_map(
        functools.partial(body, mesh.shape["ctx"], mesh.shape["hd"]),
        mesh=mesh, in_specs=in_specs, out_specs=(rows, rows), check_vma=False,
    )
```

```python
import functools
import math

import jax
import jax.numpy as jnp
from jax import lax
from jax.experimental import pallas as pl
from jax.experimental.pallas import tpu as pltpu
from jax.sharding import PartitionSpec as P

HEAD_SIZE = 128
MP = 64
MN = 128
NORM_EPS = 1e-05
MASKED = -1e30
HIGHEST = lax.Precision.HIGHEST
F32 = jnp.float32
BF16 = jnp.bfloat16
INPUT_SPACE = pltpu.HBM
PIECE = 128
UNIT = 256
VMEM_BYTES = 67043328


def dot(a, b, ca=1, cb=0, precision=None):
    return lax.dot_general(
        a, b, (((ca,), (cb,)), ((), ())), preferred_element_type=F32, precision=precision
    )


def split(value):
    high = value.astype(BF16)
    rest = value - high.astype(F32)
    mid = rest.astype(BF16)
    return high, mid, (rest - mid.astype(F32)).astype(BF16)


def kernel(
    n, wide_hd, q_in, k_in, v_in, x_in, z_in, b_in, c_in, dt_in, bias_in, alog_in, skip_in,
    gain_in, ctx_out, arrived, gain_ref,
    q_ref, x_ref, z_ref, bc_ref, dt_ref, small_ref,
    kv_all, bias_scr, ctx_stage, gated, base_scr, er_scr, xdt_scr, hs, run_split, gmask,
    buf_a, buf_b, out_a, out_b, sloc_a, sloc_b, tot_a, tot_b, log_in, log_out, wide_t,
    kv_plus, kv_minus, kv_recv, a_send, a_recv, b_send, b_recv, o_send, o_recv, c_send, c_recv,
    log_send, log_recv, q_more, ctx_more, q_send, q_recv, m_send, plus_sem, minus_sem, pair_plus, pair_minus, load_sem,
):
    me = lax.axis_index("ctx")
    tok = q_ref.shape[0]
    half = tok // 2
    heads = dt_ref.shape[0]
    width = x_ref.shape[1]
    groups = bc_ref.shape[2] // MN
    group_width = width // groups
    pieces, _, piece = buf_a.shape
    unit = math.gcd(group_width, UNIT)
    units = width // unit
    per_unit = unit // MP
    per_group = group_width // unit
    span = unit // piece
    q_heads = q_ref.shape[1] // HEAD_SIZE
    kv = kv_all.shape[2] // 2
    repeat = q_ref.shape[1] // kv
    mesh_id = pl.DeviceIdType.MESH
    core = lax.axis_index("hd")
    paired = wide_hd % 2 == 0
    partner = core + 1 - 2 * lax.rem(core, 2)
    has_left = me > 0
    has_right = me < n - 1
    helped = (me == n - 1) & (n > 1)
    helper = (me == n - 2) & (n > 1)
    kv_right_on = me < n - 2

    b_ref, c_ref = bc_ref.at[0], bc_ref.at[1]
    bias_ref, alog_ref, skip_ref = (small_ref.at[i] for i in range(3))
    parts = (
        ((dt_in, dt_ref),),
        ((bias_in, bias_ref), (alog_in, alog_ref), (skip_in, skip_ref)),
        ((k_in, kv_all.at[me, :, pl.ds(0, kv)]), (v_in, kv_all.at[me, :, pl.ds(kv, kv)])),
        ((b_in, b_ref), (c_in, c_ref)), ((x_in, x_ref),), ((z_in, z_ref),), ((q_in, q_ref),),
        ((gain_in, gain_ref),),
    )
    wholes = (dt_ref, small_ref, kv_all.at[me], bc_ref, x_ref, z_ref, q_ref, gain_ref)
    loads = [
        pltpu.make_async_copy(whole, whole, load_sem.at[i]) for i, whole in enumerate(wholes)
    ]

    barrier = pltpu.get_barrier_semaphore()

    def greet(peer):
        pl.semaphore_signal(barrier, inc=1, device_id={"ctx": peer}, device_id_type=mesh_id)

    @pl.when(has_left)
    def _():
        greet(me - 1)

    @pl.when(has_right)
    def _():
        greet(me + 1)

    if paired:
        pl.semaphore_signal(barrier, inc=1, device_id={"hd": partner}, device_id_type=mesh_id)

    for i, pairs in enumerate(parts):
        for src, dst in pairs:
            pltpu.make_async_copy(src, dst, load_sem.at[i]).start()

    def remote(src, dst, send, recv, peer):
        return pltpu.make_async_remote_copy(
            src_ref=src, dst_ref=dst, send_sem=send, recv_sem=recv,
            device_id={"ctx": peer}, device_id_type=mesh_id,
        )

    first = pl.ds(0, half)

    def kv_right(s):
        part = kv_all.at[s, first]
        return remote(part, part, kv_plus, kv_recv.at[s, 0], jnp.minimum(me + 1, n - 1))

    def kv_left(s):
        copies = []
        for i in range(2):
            part = kv_all.at[s, pl.ds(i * half, half)]
            copies.append(
                remote(part, part, kv_minus, kv_recv.at[s, i], jnp.maximum(me - 1, 0))
            )
        return copies

    def log_copy():
        return remote(log_out, log_in, log_send, log_recv, jnp.maximum(me - 1, 0))

    row = lax.broadcasted_iota(jnp.int32, (tok, tok), 0)
    col = lax.broadcasted_iota(jnp.int32, (tok, tok), 1)
    for load in loads[:2]:
        load.wait()
    raw = dot((row == col).astype(BF16), dt_ref[...], 1, 1) + bias_ref[...]
    steps = jnp.maximum(raw, 0.0) + jnp.log1p(jnp.exp(-jnp.abs(raw)))
    decay = -steps * jnp.exp(alog_ref[...])
    lower = (col <= row) & ((row < half) == (col < half))
    tri = lower.astype(BF16)
    high, mid, low = split(decay)
    run = dot(tri, high) + dot(tri, mid) + dot(tri, low)
    ends = jnp.where(
        lax.broadcasted_iota(jnp.int32, (tok, heads), 0) < half, run[half - 1 : half], run[tok - 1 : tok]
    )

    def keep_split(ref, start, value):
        for i, part in enumerate(split(value)):
            ref[start : start + value.shape[0], i * heads : (i + 1) * heads] = part

    keep_split(run_split, 0, run)
    keep_split(hs, 0, jnp.exp(run))
    keep_split(hs, tok, jnp.exp(ends - run) * steps)
    keep_split(hs, 2 * tok, steps)
    keep_split(hs, 3 * tok, jnp.broadcast_to(skip_ref[...], (16, heads)))
    own_log = jnp.broadcast_to(run[half - 1 : half] + run[tok - 1 : tok], (8, heads))

    for load in loads[2:4]:
        load.wait()
    lanes = per_unit * half
    lane = lax.broadcasted_iota(jnp.int32, (half, lanes), 1)
    source = lane - lane // half * half
    target = lax.broadcasted_iota(jnp.int32, (half, lanes), 0)
    causal = source <= target
    diagonal = source == target

    def causal_products():
        for g in range(groups):
            cols = slice(g * MN, (g + 1) * MN)
            for which in range(2):
                rows = slice(which * half, (which + 1) * half)
                repeated = jnp.concatenate([b_ref[rows, cols]] * per_unit, axis=0)
                gmask[g, rows, :] = jnp.where(causal, dot(c_ref[rows, cols], repeated, 1, 1), 0.0)

    @pl.when(me == 0)
    def _():
        buf_a[...] = jnp.zeros_like(buf_a)

    @pl.when(me == n - 1)
    def _():
        buf_b[...] = jnp.zeros_like(buf_b)
        wide_t[...] = jnp.ones_like(wide_t)

    split_head = lax.rem(lax.broadcasted_iota(jnp.int32, (3 * heads, unit), 0), heads)
    lane_head = lax.broadcasted_iota(jnp.int32, (3 * heads, unit), 1) // MP
    wide_head = lax.rem(lax.broadcasted_iota(jnp.int32, (3 * heads, lanes), 0), heads)
    wide_lane = lax.broadcasted_iota(jnp.int32, (3 * heads, lanes), 1) // half
    part_head = lax.broadcasted_iota(jnp.int32, (half, unit), 1) // MP

    def block_id(which):
        return me if which == 0 else 2 * n - 1 - me

    def send(stage, final, cols, send_sem, recv_sem, which, block=None):
        block = block_id(which) if block is None else block
        owner = block // 2
        slot = lax.rem(block, 2)
        rows = pl.ds(which * half, half)
        target = pl.ds(pl.multiple_of(slot * half, half), half)

        @pl.when(owner == me)
        def _():
            final[target, cols] = stage[rows, cols]

        @pl.when(owner != me)
        def _():
            remote(
                stage.at[rows, cols], final.at[target, cols], send_sem, recv_sem, owner
            ).start()

    def silu(value):
        return value / (1.0 + jnp.exp(-value))

    def prepare(k):
        cols = pl.ds(pl.multiple_of(k * unit, unit), unit)
        gcols = pl.ds(pl.multiple_of((k // per_group) * MN, MN), MN)
        spread = dot(hs[...], (split_head == k * per_unit + lane_head).astype(BF16))
        xs = x_ref[:, cols].astype(F32)
        weighted = (xs * spread[tok : 2 * tok]).astype(BF16)
        b_rows = b_ref[:, gcols]
        local_a = dot(b_rows[0:half], weighted[0:half], 0, 0)
        local_b = dot(b_rows[half:], weighted[half:], 0, 0)
        for i in range(span):
            part = slice(i * piece, (i + 1) * piece)
            sloc_a[span * k + i] = local_a[:, part]
            sloc_b[span * k + i] = local_b[:, part]
            tot_a[span * k + i] = jnp.broadcast_to(spread[half - 1 : half, part], (8, piece))
            tot_b[span * k + i] = jnp.broadcast_to(spread[tok - 1 : tok, part], (8, piece))
        er_scr[:, cols] = spread[0:tok]
        xdt_scr[:, cols] = (xs * spread[2 * tok : 3 * tok]).astype(BF16)
        base_scr[:, cols] = spread[3 * tok : 3 * tok + 1] * xs

    def within_blocks(k):
        cols = pl.ds(pl.multiple_of(k * unit, unit), unit)
        wide = dot(run_split[...], (wide_head == k * per_unit + wide_lane).astype(BF16))
        for which in range(2):
            rows = slice(which * half, (which + 1) * half)
            mine = wide[rows]
            gap = mine - jnp.sum(jnp.where(diagonal, mine, 0.0), axis=0, keepdims=True)
            weights = (jnp.exp(jnp.minimum(gap, 0.0)) * gmask[k // per_group, rows, :]).astype(BF16)
            part = xdt_scr[rows, cols]
            none = jnp.zeros_like(part)
            stacked = jnp.concatenate(
                [jnp.where(part_head == h, part, none) for h in range(per_unit)], axis=0
            )
            base_scr[rows, cols] = base_scr[rows, cols] + dot(weights, stacked)

    def a_copy(k):
        return remote(out_a.at[k], buf_a.at[k], a_send, a_recv.at[k], jnp.minimum(me + 1, n - 1))

    def b_copy(k):
        return remote(out_b.at[k], buf_b.at[k], b_send, b_recv.at[k], jnp.maximum(me - 1, 0))

    def step_a(k):
        @pl.when(has_left)
        def _():
            a_copy(k).wait_recv()

        @pl.when(has_right)
        def _():
            out_a[k] = (buf_a[k].astype(F32) * tot_a[k][0:1] + sloc_a[k]).astype(BF16)
            a_copy(k).start()

    def step_b(k):
        cols = pl.ds(pl.multiple_of(k * piece, piece), piece)

        @pl.when(has_right)
        def _():
            b_copy(k).wait_recv()

        @pl.when(has_left)
        def _():
            mine = sloc_a[k] * wide_t[0:1, cols] + buf_b[k].astype(F32)
            out_b[k] = (mine * tot_b[k][0:1] + sloc_b[k]).astype(BF16)
            b_copy(k).start()

    def gate(k, which, state):
        cols = pl.ds(pl.multiple_of(k * unit, unit), unit)
        gcols = pl.ds(pl.multiple_of((k // per_group) * MN, MN), MN)
        rows = slice(which * half, (which + 1) * half)
        carried = dot(c_ref[rows, gcols], state) * er_scr[rows, cols]
        z = z_ref[rows, cols].astype(F32)
        gated[rows, cols] = ((base_scr[rows, cols] + carried) * silu(z)).astype(BF16)

    def send_gated(k, which):
        cols = pl.ds(pl.multiple_of(k * unit, unit), unit)
        send(gated, arrived, cols, o_send, o_recv, which)

    def gate_a(k):
        gate(k, 0, jnp.concatenate([buf_a[span * k + i] for i in range(span)], axis=1))

    def gate_b(k):
        entering = []
        for i in range(span):
            j = span * k + i
            cols = pl.ds(pl.multiple_of(j * piece, piece), piece)
            after = buf_a[j].astype(F32) * tot_a[j][0:1] + sloc_a[j]
            entering.append((after * wide_t[0:1, cols] + buf_b[j].astype(F32)).astype(BF16))
        gate(k, 1, jnp.concatenate(entering, axis=1))

    def take_log():
        @pl.when(has_right)
        def _():
            log_copy().wait_recv()
            later = log_in[...]
            @pl.when(has_left)
            def _():
                log_out[...] = later + own_log
                log_copy().start()

            shape = (heads, width)
            pick = lax.broadcasted_iota(jnp.int32, shape, 0) == lax.broadcasted_iota(jnp.int32, shape, 1) // MP
            high, mid, low = split(jnp.exp(later))
            pick = pick.astype(BF16)
            wide_t[...] = dot(high, pick) + dot(mid, pick) + dot(low, pick)

    def relay_right(h):
        source = jnp.maximum(me - h, 0)

        @pl.when(source != me)
        def _():
            kv_right(source).wait_recv()

        @pl.when(kv_right_on)
        def _():
            kv_right(source).start()

    def q_copy():
        return remote(q_ref, q_more, q_send, q_recv, jnp.maximum(me - 1, 0))

    def relay_left(h):
        source = jnp.minimum(me + h, n - 1)
        for copy in kv_left(source):
            @pl.when(source != me)
            def _(copy=copy):
                copy.wait_recv()

            @pl.when(has_left)
            def _(copy=copy):
                copy.start()

    def attention_mask(who):
        def clear(s, _):
            @pl.when(s < me)
            def _():
                kv_all[s, half:, :] = jnp.zeros((half, 2 * kv), BF16)

            return 0

        lax.fori_loop(0, n, clear, 0)
        key = lax.broadcasted_iota(jnp.int32, (tok, n * tok), 1)
        source = key // tok
        within = key - source * tok
        key_pos = jnp.where(
            within < half, source * half + within, (2 * n - 2 - source) * half + within
        )
        query = lax.broadcasted_iota(jnp.int32, (tok, n * tok), 0)
        query_pos = jnp.where(query < half, who * half + query, (2 * n - 2 - who) * half + query)
        bias_scr[...] = jnp.where(key_pos <= query_pos, 0.0, MASKED)

    scale = 1.0 / math.sqrt(HEAD_SIZE)

    def one_head(h, queries, stage):
        hcols = pl.ds(pl.multiple_of(h * HEAD_SIZE, HEAD_SIZE), HEAD_SIZE)
        kcols = pl.ds(pl.multiple_of((h // repeat) * HEAD_SIZE, HEAD_SIZE), HEAD_SIZE)
        vcols = pl.ds(pl.multiple_of(kv + (h // repeat) * HEAD_SIZE, HEAD_SIZE), HEAD_SIZE)
        keys = kv_all[:, :, kcols].reshape(n * tok, HEAD_SIZE)
        values = kv_all[:, :, vcols].reshape(n * tok, HEAD_SIZE)
        scores = dot(queries[:, hcols], keys, 1, 1) * scale + bias_scr[...]
        expo = jnp.exp(scores - jnp.max(scores, axis=-1, keepdims=True))
        total = jnp.sum(expo, axis=-1, keepdims=True)
        stage[:, hcols] = (dot(expo.astype(BF16), values) / total).astype(BF16)

    def send_ctx():
        for which in range(2):
            send(ctx_stage, ctx_out, slice(None), c_send, c_recv, which)

    loads[4].wait()
    hops = n - 1 - me
    middle = pieces // 2

    peers = has_left.astype(jnp.int32) + has_right.astype(jnp.int32) + int(paired)

    @pl.when(has_left)
    def _():
        pl.semaphore_wait(barrier, peers)

    @pl.when(jnp.logical_not(has_right))
    def _():
        log_out[...] = own_log
        log_copy().start()

    @pl.when(has_right & has_left)
    def _():
        for copy in kv_left(me):
            copy.start()

    @pl.when(kv_right_on & has_left)
    def _():
        kv_right(me).start()

    prepare(0)

    @pl.when(jnp.logical_not(has_left))
    def _():
        pl.semaphore_wait(barrier, peers)

    def first_step(k, _):
        @pl.when(k > 0)
        def _():
            prepare(k)

        @pl.when((k == units // 2) & (me == n - 1))
        def _():
            relay_left(0)

        for i in range(span):
            @pl.when(me == 0)
            def _(i=i):
                step_a(span * k + i)

            @pl.when(me == n - 1)
            def _(i=i):
                step_b(span * k + i)

        return 0

    between = has_left & has_right
    lax.fori_loop(0, jnp.where(between, units - 2, units), first_step, 0)
    for load in loads[5:7]:
        load.wait()

    @pl.when((me == 0) & kv_right_on)
    def _():
        relay_right(0)

    @pl.when(helped)
    def _():
        q_copy().start()

    def base(distance):
        return (14 * jnp.maximum(distance - 1, 0)) // 3

    lag_a = base(me)
    lag_b = base(hops)
    block_b = 2 * n - 1 - me
    hold_plus = block_b // 2 - 1 > me
    hold_minus = me // 2 + 1 < me
    gap = jnp.where(hops > 1, 6, 2)
    free = jnp.maximum(lag_a + pieces - 1, lag_b + pieces + gap + 1)
    gates = jnp.maximum(lag_a - 2, lag_b + gap) + pieces - units + 3
    gates = gates + jnp.where(2 * me < n, jnp.where(has_left, 1, 0), jnp.where(has_right, 7, 1))
    gates = jnp.maximum(gates, jnp.where(hold_plus, lag_a + pieces + 2, 0))
    gates = jnp.maximum(gates, jnp.where(hold_minus, lag_b + pieces + gap + 2, 0))
    quick = gates >= jnp.maximum(lag_a + pieces, lag_b + pieces + gap + 2)
    ending = has_left & jnp.logical_not(has_right)
    first_out = jnp.where((2 * me < n) | jnp.logical_not(has_right), 1, 0)
    early = lag_b + middle
    fills = has_left & has_right & (2 * me >= n) & (lag_a + 2 * span <= early)
    last = functools.reduce(jnp.maximum, [
        lag_a + pieces + 2, lag_b + pieces + gap + 2, gates + jnp.where(quick, middle // 2, middle),
        6 * n - 10, 2 * units,
    ])

    def greet_pair(pair_sem, peers):
        if paired:
            @pl.when(functools.reduce(jnp.logical_or, [ok for _, ok in peers]))
            def _():
                pl.semaphore_signal(pair_sem, inc=1, device_id={"hd": partner}, device_id_type=mesh_id)

    def release(pair_sem, sem, peers):
        if paired:
            @pl.when(functools.reduce(jnp.logical_or, [ok for _, ok in peers]))
            def _():
                pl.semaphore_wait(pair_sem, 1)

        for peer, ok in peers:
            @pl.when(ok)
            def _(peer=peer):
                pl.semaphore_signal(sem, inc=1, device_id={"ctx": peer}, device_id_type=mesh_id)

    plus_peers = [(p, (p >= 0) & (p < me)) for p in (2 * n - 3 - 2 * me, 2 * n - 4 - 2 * me)]
    minus_peers = [(p, (p > me) & (p < n)) for p in (2 * me - 2, 2 * me - 1)]
    plus_peers = [(p, ok & has_right) for p, ok in plus_peers]
    minus_peers = [(p, ok & has_left) for p, ok in minus_peers]

    def chain_a(t):
        at = t - lag_a

        @pl.when((at >= 0) & (at < pieces) & has_left)
        def _():
            step_a(at)

        @pl.when((at == pieces + 1) & has_left & kv_right_on)
        def _():
            relay_right(me)

        @pl.when((at == pieces - 3) & has_left)
        def _():
            greet_pair(pair_plus, plus_peers)

    def chain_b(t):
        at = t - lag_b

        @pl.when((at == 0) & has_right)
        def _():
            take_log()

        @pl.when((at == middle + gap) & has_right)
        def _():
            relay_left(hops)

        k = jnp.where(at < middle, at, at - gap - 2)

        @pl.when(((at >= 0) & (at < middle) | (at > middle + gap + 1) & (at <= pieces + gap + 1)) & has_right)
        def _():
            step_b(k)

        @pl.when((at == pieces + gap + 1) & has_right)
        def _():
            greet_pair(pair_minus, minus_peers)

    def slot_step(t, _):
        @pl.when(2 * me >= n)
        def _():
            chain_b(t)

        chain_a(t)

        @pl.when(2 * me < n)
        def _():
            chain_b(t)

        @pl.when(t == lag_a + pieces - 2)
        def _():
            release(pair_plus, plus_sem, plus_peers)

        @pl.when(t == free)
        def _():
            release(pair_minus, minus_sem, minus_peers)

        for h in range(1, n - 1):
            @pl.when((t == 4 * h - 4) & (h < me) & jnp.logical_not(helped))
            def _(h=h):
                relay_right(h)

            @pl.when((t == 6 * h - 4) & (h < hops))
            def _(h=h):
                relay_left(h)

        @pl.when(t == 0)
        def _():
            causal_products()

        @pl.when(between & ((t == 1) | (t == 3)))
        def _():
            prepare(units - 2 + t // 2)

        @pl.when((t < 2 * units) & (lax.rem(t, 2) == 0))
        def _():
            within_blocks(t // 2)

        @pl.when((t == gates) & hold_plus)
        def _():
            pl.semaphore_wait(plus_sem, 1)

        @pl.when((t == gates) & hold_minus)
        def _():
            pl.semaphore_wait(minus_sem, 1)

        @pl.when((t == early) & fills)
        def _():
            for i in range(2):
                gate_a(i)
            for i in range(2):
                send_gated(i, 0)

        @pl.when((t == lag_a + middle - 1) & ending)
        def _():
            def gate_early(i, _):
                for j in range(2):
                    gate_a(2 * i + j)
                    gate_b(2 * i + j)
                for j in range(2):
                    send_gated(2 * i + j, 1)
                return 0

            lax.fori_loop(0, units // 4, gate_early, 0)

        at = jnp.where(quick, 2, 1) * (t - gates)
        on = (at >= jnp.where(ending, units // 4 * 2, 0)) & (at < units) & (lax.rem(at, 2) == 0)
        done_a = fills & (at == 0)

        @pl.when(on & jnp.logical_not(done_a))
        def _():
            for i in range(2):
                gate_a(at + i)
                gate_b(at + i)
            for which in range(2):
                @pl.when(first_out == which)
                def _(which=which):
                    for i in range(2):
                        send_gated(at + i, which)

        @pl.when(on & done_a)
        def _():
            for i in range(2):
                gate_b(at + i)

        return 0

    lax.fori_loop(0, last, slot_step, 0)

    for which in range(2):
        @pl.when(first_out != which)
        def _(which=which):
            def send_rest(k, _):
                send_gated(k, which)
                return 0

            lax.fori_loop(0, units, send_rest, 0)

    def attend(who, queries, stage):
        attention_mask(who)

        def two_heads(i, _):
            one_head(2 * i, queries, stage)
            one_head(2 * i + 1, queries, stage)
            return 0

        lax.fori_loop(0, q_heads // 2, two_heads, 0)

    @pl.when(helper & has_left)
    def _():
        kv_right(0).wait_recv()

    @pl.when(jnp.logical_not(helped))
    def _():
        attend(me, q_ref, ctx_stage)
        send_ctx()

    @pl.when(helper)
    def _():
        q_copy().wait_recv()
        attend(n - 1, q_more, ctx_more)
        for which in range(2):
            send(ctx_more, ctx_out, slice(None), m_send, c_recv, which, jnp.int32(n - 1 + which))

    @pl.when(has_right)
    def _():
        remote(out_a, buf_a, a_send, a_recv.at[0], me).wait_send()

    @pl.when(has_left)
    def _():
        remote(out_b, buf_b, b_send, b_recv.at[0], me).wait_send()

    @pl.when(has_left)
    def _():
        log_copy().wait_send()

    for i in range(n):
        @pl.when((me == i) & kv_right_on)
        def _(i=i):
            part = kv_all.at[pl.ds(0, i + 1), first]
            remote(part, part, kv_plus, kv_recv.at[0, 0], me).wait_send()

        @pl.when((me == i) & has_left)
        def _(i=i):
            part = kv_all.at[pl.ds(i, n - i)]
            remote(part, part, kv_minus, kv_recv.at[0, 0], me).wait_send()

    def settle(stage, final, send_sem, recv_sem, away, missing):
        for count in (1, 2):
            rows = pl.ds(0, count * half)
            copy = remote(stage.at[rows], final.at[rows], send_sem, recv_sem, me)

            @pl.when(away == count)
            def _(copy=copy):
                copy.wait_send()

            @pl.when(missing == count)
            def _(copy=copy):
                copy.wait_recv()

    def tally(flags):
        return sum(jnp.where(flag, 1, 0) for flag in flags)

    def source_of(slot):
        block = 2 * me + slot
        return jnp.where(block < n, block, 2 * n - 1 - block)

    away = tally(block_id(which) // 2 != me for which in range(2))
    missing = tally(source_of(slot) != me for slot in range(2))
    served = [jnp.minimum(source_of(slot), n - 2) if n > 1 else source_of(slot) for slot in range(2)]
    served_missing = tally(source != me for source in served)
    more = sum(1 for block in (n - 1, n) if block // 2 != n - 2)

    @pl.when(helped)
    def _():
        q_copy().wait_send()

    settle(ctx_stage, ctx_out, c_send, c_recv, jnp.where(helped, 0, away), served_missing)
    settle(ctx_more, ctx_out, m_send, c_recv, jnp.where(helper, more, 0), 0)
    loads[7].wait()
    settle(gated, arrived, o_send, o_recv, away, missing)


def finish(groups, ctx_ref, gated_ref, gain_ref, ctx_out, mix_out, mixed, sems):
    tok, width = gated_ref.shape
    group_width = width // groups
    half = tok // 2
    copies = [pltpu.make_async_copy(ctx_ref, ctx_out, sems.at[0])]
    copies[0].start()
    for g in range(groups):
        for which in range(2):
            rows, cols = pl.ds(which * half, half), pl.ds(g * group_width, group_width)
            value = gated_ref[rows, cols].astype(F32)
            power = jnp.mean(value * value, axis=-1, keepdims=True)
            mixed[rows, cols] = (value * lax.rsqrt(power + NORM_EPS) * gain_ref[:, cols]).astype(BF16)
            copies.append(
                pltpu.make_async_copy(
                    mixed.at[rows, cols], mix_out.at[rows, cols], sems.at[1 + 2 * g + which]
                )
            )
            copies[-1].start()
    for copy in copies:
        copy.wait()


def body(n, wide_hd, query, keys, values, m_x, m_z, m_b, m_c, dt_raw, dt_bias, a_log, d_skip, norm_gain):
    tok, width = m_x.shape
    half = tok // 2
    heads = dt_raw.shape[1]
    anywhere = pl.BlockSpec(memory_space=INPUT_SPACE)
    groups = m_b.shape[1] // MN
    piece = math.gcd(width // groups, PIECE)
    pieces = width // piece
    unit = math.gcd(width // groups, UNIT)
    units = width // unit
    kv = keys.shape[1]
    q_heads = query.shape[1] // HEAD_SIZE
    dma = pltpu.SemaphoreType.DMA
    vmem = pltpu.VMEM
    state = (pieces, MN, piece)
    spec = pl.BlockSpec(memory_space=pltpu.VMEM)
    spare = 2 * (query.size + m_x.size) + 4 * width + 49152
    context, gated, gain = pl.pallas_call(
        functools.partial(kernel, n, wide_hd),
        out_shape=(
            vmem(query.shape, BF16),
            vmem(m_x.shape, BF16),
            vmem((1, width), F32),
        ),
        in_specs=[anywhere] * 12,
        out_specs=(spec, spec, spec),
        scratch_shapes=[
            vmem(query.shape, BF16),
            vmem(m_x.shape, BF16),
            vmem(m_x.shape, BF16),
            vmem((2,) + m_b.shape, BF16),
            vmem((heads, tok), BF16),
            vmem((3, 1, heads), F32),
            vmem((n, tok, 2 * kv), BF16),
            vmem((tok, n * tok), F32),
            vmem(query.shape, BF16),
            vmem(m_x.shape, BF16),
            vmem((tok, width), F32),
            vmem((tok, width), F32),
            vmem((tok, width), BF16),
            vmem((3 * tok + 16, 3 * heads), BF16),
            vmem((tok, 3 * heads), BF16),
            vmem((groups, tok, unit // MP * (tok // 2)), F32),
            vmem(state, BF16),
            vmem(state, BF16),
            vmem(state, BF16),
            vmem(state, BF16),
            vmem(state, F32),
            vmem(state, F32),
            vmem((pieces, 8, piece), F32),
            vmem((pieces, 8, piece), F32),
            vmem((8, heads), F32),
            vmem((8, heads), F32),
            vmem((8, width), F32),
            dma(()),
            dma(()),
            dma((n, 2)),
            dma(()),
            dma((pieces,)),
            dma(()),
            dma((pieces,)),
            dma(()),
            dma(()),
            dma(()),
            dma(()),
            dma(()),
            dma(()),
            vmem(query.shape, BF16),
            vmem(query.shape, BF16),
            dma(()),
            dma(()),
            dma(()),
            pltpu.SemaphoreType.REGULAR,
            pltpu.SemaphoreType.REGULAR,
            pltpu.SemaphoreType.REGULAR,
            pltpu.SemaphoreType.REGULAR,
            dma((8,)),
        ],
        compiler_params=pltpu.CompilerParams(
            collective_id=0, has_side_effects=True, vmem_limit_bytes=VMEM_BYTES - spare
        ),
    )(
        query, keys, values, m_x, m_z, m_b, m_c, dt_raw.T,
        dt_bias.reshape(1, -1), a_log.reshape(1, -1), d_skip.reshape(1, -1), norm_gain.reshape(1, -1),
    )
    return pl.pallas_call(
        functools.partial(finish, groups),
        out_shape=(
            jax.ShapeDtypeStruct(query.shape, BF16),
            jax.ShapeDtypeStruct(m_x.shape, BF16),
        ),
        in_specs=[spec] * 3,
        out_specs=(anywhere, anywhere),
        scratch_shapes=[vmem(m_x.shape, BF16), dma((1 + 2 * groups,))],
        compiler_params=pltpu.CompilerParams(vmem_limit_bytes=4 << 20),
    )(context, gated, gain)


def solution(mesh):
    rows = P(("grp", "ctx"), "hd")
    in_specs = (rows,) * 8 + (P("hd"),) * 4
    return jax.shard_map(
        functools.partial(body, mesh.shape["ctx"], mesh.shape["hd"]),
        mesh=mesh, in_specs=in_specs, out_specs=(rows, rows), check_vma=False,
    )
```
